16 devices in a mesh: ep: 16 (over z, y, x, core).
Axes of the slice: x: 2, y: 2, z: 2, core: 2. Of those that a mesh axis runs over, the one named last changes fastest.
Arguments:
- tokens: bfloat16 [256, 256, 768], P('ep')
- pad_mask: int32 [256, 256], P('ep')
- second_draw: float32 [256, 256], P('ep')
- choices: int32 [256, 256, 2], P('ep')
- norm_attn: float32 [768], replicated
- w_query: bfloat16 [768, 12, 64], replicated
- w_key: bfloat16 [768, 12, 64], replicated
- w_value: bfloat16 [768, 12, 64], replicated
- w_attn_out: bfloat16 [12, 64, 768], replicated
- norm_moe: float32 [768], replicated
- w_gate: float32 [768, 128], replicated
- w_in: bfloat16 [128, 768, 3072], P('ep')
- w_out: bfloat16 [128, 3072, 768], P('ep')
Outputs:
- output 1: bfloat16 [256, 256, 768], P('ep')
- output 2: float32 [], replicated
All inputs are finite; a program needn't handle non-finite values.
Results may differ from the reference program's by a relative error of at most 0.0175475.
Values are sent between devices in bfloat16 or wider.
A program may use at most 1 GiB of HBM per device.

```python
import math
import jax
import jax.numpy as jnp
from jax import lax

D_MODEL = 768
NUM_HEADS = 12
HEAD_DIM = 64
FF_DIM = 3072
EXPERTS = 128
GROUPS = 256
SEQ_LEN = 256

CAPACITY = (2 * SEQ_LEN + EXPERTS - 1) // EXPERTS
NORM_EPS = 1e-6


def rms_norm(values, scale_vec):
    values_f = values.astype(jnp.float32)
    inv_rms = lax.rsqrt(jnp.mean(values_f * values_f, axis=-1, keepdims=True) + NORM_EPS)
    return (values_f * inv_rms * scale_vec).astype(jnp.bfloat16)


def draw_routing(base_key):
    key_list = jax.random.split(base_key, 7)
    lengths = jax.random.randint(key_list[0], (GROUPS,), SEQ_LEN // 2, SEQ_LEN + 1)
    lengths = lengths.at[0].set(SEQ_LEN).at[1].set(SEQ_LEN // 2)
    pad_mask = (jnp.arange(SEQ_LEN)[None, :] < lengths[:, None]).astype(jnp.int32)
    second_draw = jax.random.uniform(key_list[1], (GROUPS, SEQ_LEN), jnp.float32)
    hot_expert = jax.random.randint(key_list[2], (GROUPS, 1), 0, EXPERTS)
    hot_share = jax.random.randint(key_list[3], (GROUPS, 1), 0, 5)
    coin_draw = jax.random.randint(key_list[4], (GROUPS, SEQ_LEN), 0, 16)
    any_first = jax.random.randint(key_list[5], (GROUPS, SEQ_LEN), 0, EXPERTS)
    first_pick = jnp.where(coin_draw < hot_share, hot_expert, any_first)
    offset = jax.random.randint(key_list[6], (GROUPS, SEQ_LEN), 1, EXPERTS)
    second_pick = (first_pick + offset) % EXPERTS
    choices = jnp.stack([first_pick, second_pick], axis=-1).astype(jnp.int32)
    return pad_mask, second_draw, choices


def setup_inputs(seed: int = 0) -> dict:
    key_list = jax.random.split(jax.random.key(seed), 11)
    head_width = NUM_HEADS * HEAD_DIM
    att_gain = math.sqrt(math.log(SEQ_LEN) / 2.0)
    out_gain = 0.5 * SEQ_LEN ** 0.25
    pad_mask, second_draw, choices = draw_routing(key_list[0])

    def normal_draw(index, shape, scale_val):
        return jax.random.normal(key_list[index], shape, jnp.float32) * scale_val

    return {
        "tokens": normal_draw(1, (GROUPS, SEQ_LEN, D_MODEL), 1.0).astype(jnp.bfloat16),
        "pad_mask": pad_mask,
        "second_draw": second_draw,
        "choices": choices,
        "norm_attn": 1.0 + normal_draw(2, (D_MODEL,), 0.3),
        "w_query": normal_draw(3, (D_MODEL, NUM_HEADS, HEAD_DIM), att_gain / math.sqrt(D_MODEL)).astype(jnp.bfloat16),
        "w_key": normal_draw(4, (D_MODEL, NUM_HEADS, HEAD_DIM), 1.0 / math.sqrt(D_MODEL)).astype(jnp.bfloat16),
        "w_value": normal_draw(5, (D_MODEL, NUM_HEADS, HEAD_DIM), 1.0 / math.sqrt(D_MODEL)).astype(jnp.bfloat16),
        "w_attn_out": normal_draw(6, (NUM_HEADS, HEAD_DIM, D_MODEL), out_gain / math.sqrt(head_width)).astype(jnp.bfloat16),
        "norm_moe": 1.0 + normal_draw(7, (D_MODEL,), 0.3),
        "w_gate": normal_draw(8, (D_MODEL, EXPERTS), 1.0 / math.sqrt(D_MODEL)),
        "w_in": normal_draw(9, (EXPERTS, D_MODEL, FF_DIM), 1.0 / math.sqrt(D_MODEL)).astype(jnp.bfloat16),
        "w_out": normal_draw(10, (EXPERTS, FF_DIM, D_MODEL), 2.0 / math.sqrt(FF_DIM)).astype(jnp.bfloat16),
    }


def reference(tokens, pad_mask, second_draw, choices, norm_attn, w_query, w_key, w_value, w_attn_out, norm_moe, w_gate, w_in, w_out):
    head_width = NUM_HEADS * HEAD_DIM
    wq_flat = w_query.reshape(D_MODEL, head_width)
    wk_flat = w_key.reshape(D_MODEL, head_width)
    wv_flat = w_value.reshape(D_MODEL, head_width)
    wo_flat = w_attn_out.reshape(head_width, D_MODEL)
    w_in_f = w_in.astype(jnp.float32)
    w_out_f = w_out.astype(jnp.float32)
    expert_ids = jnp.arange(EXPERTS)
    slot_ids = jnp.arange(CAPACITY)

    def one_group(group_args):
        x_grp, mask_grp, draw_grp, pick_grp = group_args
        normed = rms_norm(x_grp, norm_attn)
        q_heads = jnp.dot(normed, wq_flat, preferred_element_type=jnp.float32).astype(jnp.bfloat16).reshape(SEQ_LEN, NUM_HEADS, HEAD_DIM)
        k_heads = jnp.dot(normed, wk_flat, preferred_element_type=jnp.float32).astype(jnp.bfloat16).reshape(SEQ_LEN, NUM_HEADS, HEAD_DIM)
        v_heads = jnp.dot(normed, wv_flat, preferred_element_type=jnp.float32).astype(jnp.bfloat16).reshape(SEQ_LEN, NUM_HEADS, HEAD_DIM)
        scores = jnp.einsum("qhc,khc->hqk", q_heads.astype(jnp.float32), k_heads.astype(jnp.float32)) * (HEAD_DIM ** -0.5)
        scores = jnp.where(mask_grp[None, None, :] == 1, scores, -1e30)
        attn_probs = jax.nn.softmax(scores, axis=-1).astype(jnp.bfloat16)
        context = jnp.einsum("hqk,khc->qhc", attn_probs.astype(jnp.float32), v_heads.astype(jnp.float32)).astype(jnp.bfloat16)
        attn_out = jnp.dot(context.reshape(SEQ_LEN, head_width), wo_flat, preferred_element_type=jnp.float32)
        hidden = (x_grp.astype(jnp.float32) + attn_out).astype(jnp.bfloat16)
        moe_in = rms_norm(hidden, norm_moe)
        logits = jnp.dot(moe_in.astype(jnp.float32), w_gate)
        gate_probs = jax.nn.softmax(logits, axis=-1)
        is_valid = mask_grp == 1
        first_hot = pick_grp[:, 0:1] == expert_ids
        second_hot = pick_grp[:, 1:2] == expert_ids
        p_first = jnp.sum(jnp.where(first_hot, gate_probs, 0.0), axis=-1)
        p_second = jnp.sum(jnp.where(second_hot, gate_probs, 0.0), axis=-1)
        gate_first = p_first / (p_first + p_second)
        gate_second = p_second / (p_first + p_second)
        want_second = is_valid & (draw_grp < 2.0 * gate_second)
        first_take = (first_hot & is_valid[:, None]).astype(jnp.int32)
        first_pos = jnp.sum((jnp.cumsum(first_take, axis=0) - 1) * first_take, axis=-1)
        first_count = jnp.sum(first_take, axis=0)
        keep_first = is_valid & (first_pos < CAPACITY)
        second_take = (second_hot & want_second[:, None]).astype(jnp.int32)
        second_pos = jnp.sum((jnp.cumsum(second_take, axis=0) - 1 + jnp.minimum(first_count, CAPACITY)[None, :]) * second_take, axis=-1)
        keep_second = want_second & (second_pos < CAPACITY)
        first_slot = (first_pos[:, None] == slot_ids) & keep_first[:, None]
        second_slot = (second_pos[:, None] == slot_ids) & keep_second[:, None]
        first_mask = first_hot[:, :, None] & first_slot[:, None, :]
        second_mask = second_hot[:, :, None] & second_slot[:, None, :]
        dispatch = (first_mask | second_mask).astype(jnp.float32)
        combine = (jnp.where(first_mask, gate_first[:, None, None], 0.0) + jnp.where(second_mask, gate_second[:, None, None], 0.0)).astype(jnp.bfloat16)
        send_buf = jnp.einsum("sec,sd->ecd", dispatch, moe_in.astype(jnp.float32)).astype(jnp.bfloat16)
        inner_act = jnp.maximum(jnp.einsum("ecd,edf->ecf", send_buf.astype(jnp.float32), w_in_f), 0.0).astype(jnp.bfloat16)
        expert_out = jnp.einsum("ecf,efd->ecd", inner_act.astype(jnp.float32), w_out_f).astype(jnp.bfloat16)
        moe_out = jnp.einsum("sec,ecd->sd", combine.astype(jnp.float32), expert_out.astype(jnp.float32))
        out_grp = (hidden.astype(jnp.float32) + moe_out).astype(jnp.bfloat16)
        density = jnp.sum(jnp.where(is_valid[:, None], gate_probs, 0.0), axis=0) / SEQ_LEN
        aux_grp = jnp.sum(first_count.astype(jnp.float32) / SEQ_LEN * density)
        return out_grp, aux_grp

    out_tokens, aux_groups = lax.map(one_group, (tokens, pad_mask, second_draw, choices))
    aux_loss = EXPERTS * jnp.sum(aux_groups) / GROUPS
    return out_tokens, aux_loss
```

```python
import functools
import jax
import jax.numpy as jnp
from jax import lax
from jax.experimental import pallas as pl
from jax.experimental.pallas import tpu as pltpu
from jax.sharding import PartitionSpec as P

NORM_EPS = 1e-6
N_DEV = 16
MESH = pl.DeviceIdType.MESH
F32 = jnp.float32
BF16 = jnp.bfloat16
ORDER = (0, 9, 2, 11, 4, 13, 6, 15, 8, 1, 10, 3, 12, 5, 14, 7)
VMEM_LIMIT = 62 * 1024 * 1024


def partner(me, mask):
    out = 0
    for bit in range(4):
        val = lax.rem(me // (1 << bit), 2)
        out = out + (1 << bit) * ((1 - val) if (mask >> bit) & 1 else val)
    return out


def greet(me):
    barrier = pltpu.get_barrier_semaphore()
    for mask in range(1, N_DEV):
        pl.semaphore_signal(barrier, inc=1, device_id=(partner(me, mask),), device_id_type=MESH)


def rms_norm(values_f, scale_vec):
    inv_rms = lax.rsqrt(jnp.mean(values_f * values_f, axis=-1, keepdims=True) + NORM_EPS)
    return (values_f * inv_rms * scale_vec).astype(BF16)


def dot(a, b):
    return jnp.dot(a, b, preferred_element_type=F32)


def front_kernel(
    tokens_ref, keymask_ref, cols_ref, norm_attn_ref, wqkv_ref, wo_ref, norm_moe_ref, wgate_ref,
    hidden_ref, meta_ref, recv_ref, auxr_ref,
    qkv_s, ctx_s, wg_s, aux_s, send_s, send_sem, recv_sem, local_sem, aux_send_sem, aux_recv_sem,
    *, heads, head_dim, capacity,
):
    step = pl.program_id(0)
    steps = pl.num_programs(0)
    me = lax.axis_index("ep")
    seq = tokens_ref.shape[1]
    d_model = tokens_ref.shape[2]
    experts = wgate_ref.shape[1]
    e_loc = experts // N_DEV
    half = e_loc // 2
    slots = experts * capacity
    rows = 2 * capacity
    per_src = steps * rows

    def send_pair(pair):
        for place, mask in enumerate(ORDER):
            dev = partner(me, mask)
            src = send_s.at[pair, dev]
            dst = recv_ref.at[:, pl.ds(pl.multiple_of(place * per_src + pair * rows, rows), rows), :]
            if mask == 0:
                pltpu.make_async_copy(src, dst, local_sem.at[0]).start()
            else:
                pltpu.make_async_remote_copy(
                    src_ref=src, dst_ref=dst, send_sem=send_sem, recv_sem=recv_sem,
                    device_id=(dev,), device_id_type=MESH).start()

    @pl.when(step == 0)
    def _():
        greet(me)
        aux_s[...] = jnp.zeros_like(aux_s)
        wg = wgate_ref[...]
        hi = wg.astype(BF16)
        rest = wg - hi.astype(F32)
        mid = rest.astype(BF16)
        low = (rest - mid.astype(F32)).astype(BF16)
        wg_s[:, 0:experts] = hi
        wg_s[:, experts:2 * experts] = mid
        wg_s[:, 2 * experts:3 * experts] = low

    @pl.when(step == 1)
    def _():
        pl.semaphore_wait(pltpu.get_barrier_semaphore(), N_DEV - 1)

    @pl.when(step > 0)
    def _():
        send_pair(step - 1)

    x = tokens_ref[...].reshape(2 * seq, d_model)
    a = rms_norm(x.astype(F32), norm_attn_ref[...])
    qkv_s[...] = dot(a, wqkv_ref[...]).astype(BF16)

    width = 2 * head_dim
    lane = lax.broadcasted_iota(jnp.int32, (1, width), 1)
    ones = [(lane < head_dim).astype(F32).astype(BF16), (lane >= head_dim).astype(F32).astype(BF16)]
    scaled = [m * jnp.asarray(head_dim ** -0.5, BF16) for m in ones]
    hw = heads * head_dim
    for grp in range(2):
        tok = pl.ds(grp * seq, seq)
        keep_key = keymask_ref[grp] == 1
        for pair_idx in range(heads // 2):
            off = pair_idx * width
            q = qkv_s[tok, pl.ds(off, width)]
            k = qkv_s[tok, pl.ds(hw + off, width)]
            v = qkv_s[tok, pl.ds(2 * hw + off, width)]
            ctx = None
            for side in range(2):
                s = lax.dot_general(q * scaled[side], k, (((1,), (1,)), ((), ())), preferred_element_type=F32)
                s = jnp.where(keep_key, s, -1e30)
                ex = jnp.exp(s - jnp.max(s, axis=-1, keepdims=True))
                prob = (ex * (1.0 / jnp.sum(ex, axis=-1, keepdims=True))).astype(BF16)
                part = dot(prob, v * ones[side])
                ctx = part if ctx is None else ctx + part
            ctx_s[tok, pl.ds(off, width)] = ctx.astype(BF16)

    hidden = (x.astype(F32) + dot(ctx_s[...], wo_ref[...])).astype(BF16)
    hidden_ref[...] = hidden.reshape(2, seq, d_model)
    b = rms_norm(hidden.astype(F32), norm_moe_ref[...])
    lg = dot(b, wg_s[...])
    logits = (lg[:, 2 * experts:] + lg[:, experts:2 * experts]) + lg[:, :experts]
    ex = jnp.exp(logits - jnp.max(logits, axis=-1, keepdims=True))
    gate_probs = ex / jnp.sum(ex, axis=-1, keepdims=True)

    eid = lax.broadcasted_iota(jnp.int32, (seq, experts), 1)
    tri = (lax.broadcasted_iota(jnp.int32, (seq, seq), 0) >= lax.broadcasted_iota(jnp.int32, (seq, seq), 1)).astype(F32).astype(BF16)
    slot_id = lax.broadcasted_iota(jnp.int32, (seq, slots), 1)
    meta_lane = lax.broadcasted_iota(jnp.int32, (seq, experts), 1)
    picked = []
    for grp in range(2):
        p = gate_probs[grp * seq:(grp + 1) * seq]
        cols = cols_ref[grp]
        valid = cols[:, 0:1] == 1.0
        draw = cols[:, 1:2]
        e1 = cols[:, 2:3].astype(jnp.int32)
        e2 = cols[:, 3:4].astype(jnp.int32)
        hot1 = eid == e1
        hot2 = eid == e2
        p1 = jnp.sum(jnp.where(hot1, p, 0.0), axis=-1, keepdims=True)
        p2 = jnp.sum(jnp.where(hot2, p, 0.0), axis=-1, keepdims=True)
        g1 = p1 / (p1 + p2)
        g2 = p2 / (p1 + p2)
        want2 = valid & (draw < 2.0 * g2)
        take1 = jnp.where(hot1 & valid, 1.0, 0.0)
        take2 = jnp.where(hot2 & want2, 1.0, 0.0)
        cum = dot(tri, jnp.concatenate([take1, take2], axis=1).astype(BF16))
        cum1 = cum[:, :experts]
        cum2 = cum[:, experts:]
        count1 = cum1[seq - 1:seq, :]
        pos1 = jnp.sum((cum1 - 1.0) * take1, axis=-1, keepdims=True).astype(jnp.int32)
        pos2 = jnp.sum((cum2 - 1.0 + jnp.minimum(count1, float(capacity))) * take2, axis=-1, keepdims=True).astype(jnp.int32)
        keep1 = valid & (pos1 < capacity)
        keep2 = want2 & (pos2 < capacity)

        density = jnp.sum(jnp.where(valid, p, 0.0), axis=0, keepdims=True) / seq
        aux_s[0:1, :] += count1 / seq * density

        def places(e, pos, keep):
            dev = e // e_loc
            r = e - dev * e_loc
            upper = r // half
            i = r - upper * half
            side = upper if grp == 0 else 1 - upper
            disp = ((dev * half + i) * 2 + side) * capacity + pos
            comb = (e * 2 + side) * capacity + pos
            return jnp.where(keep, disp, -1), jnp.where(keep, comb, -1)

        d1, c1 = places(e1, pos1, keep1)
        d2, c2 = places(e2, pos2, keep2)
        meta = jnp.where(meta_lane == 0, c1.astype(F32), 0.0)
        meta = jnp.where(meta_lane == 1, c2.astype(F32), meta)
        meta = jnp.where(meta_lane == 2, g1, meta)
        meta = jnp.where(meta_lane == 3, g2, meta)
        meta_ref[grp] = meta
        disp_mat = jnp.where((slot_id == d1) | (slot_id == d2), 1.0, 0.0).astype(BF16)
        got = lax.dot_general(disp_mat, b[grp * seq:(grp + 1) * seq], (((0,), (0,)), ((), ())), preferred_element_type=F32)
        picked.append(got.reshape(N_DEV * half, rows, d_model))

    top = lax.broadcasted_iota(jnp.int32, (1, rows, 1), 1) < capacity
    lower = jnp.where(top, picked[0], picked[1]).astype(BF16)
    upper = jnp.where(top, picked[1], picked[0]).astype(BF16)
    send_s[step, :, 0:half] = lower.reshape(N_DEV, half, rows, d_model)
    send_s[step, :, half:e_loc] = upper.reshape(N_DEV, half, rows, d_model)

    @pl.when(step == steps - 1)
    def _():
        send_pair(steps - 1)
        for mask in range(1, N_DEV):
            pltpu.make_async_remote_copy(
                src_ref=aux_s, dst_ref=auxr_ref.at[mask], send_sem=aux_send_sem, recv_sem=aux_recv_sem,
                device_id=(partner(me, mask),), device_id_type=MESH).start()
        own = pltpu.make_async_copy(aux_s, auxr_ref.at[0], local_sem.at[1])
        own.start()
        own.wait()
        others = pl.ds(0, N_DEV - 1)
        pltpu.make_async_copy(send_s.at[:, others], send_s.at[:, others], send_sem).wait()
        pltpu.make_async_copy(send_s.at[:, 0], send_s.at[:, 0], local_sem.at[0]).wait()
        pltpu.make_async_copy(auxr_ref.at[others], auxr_ref.at[others], aux_send_sem).wait()
        pltpu.make_async_copy(auxr_ref.at[others], auxr_ref.at[others], aux_recv_sem).wait()
        arrived = recv_ref.at[:, pl.ds(0, (N_DEV - 1) * per_src), :]
        pltpu.make_async_copy(arrived, arrived, recv_sem).wait()


def expert_kernel(recv_ref, w_in_ref, w_out_ref, ret_ref, act_s, z_s, send_sem, recv_sem, local_sem, *, tile):
    e = pl.program_id(0)
    n_exp = pl.num_programs(0)
    me = lax.axis_index("ep")
    rows = recv_ref.shape[1]
    ff = w_in_ref.shape[2]
    per_src = rows // N_DEV
    n_tiles = rows // tile
    chunk = 1024

    @pl.when(e == 0)
    def _():
        greet(me)

    for t in range(n_tiles):
        x = recv_ref[0, pl.ds(t * tile, tile), :]
        for f in range(ff // chunk):
            act = dot(x, w_in_ref[0, :, pl.ds(f * chunk, chunk)])
            act_s[:, pl.ds(f * chunk, chunk)] = jnp.maximum(act, 0.0).astype(BF16)
        z_s[e, pl.ds(t * tile, tile), :] = dot(act_s[...], w_out_ref[0]).astype(BF16)

        if t == 0:
            @pl.when(e == 0)
            def _():
                pl.semaphore_wait(pltpu.get_barrier_semaphore(), N_DEV - 1)

        for place in range(t * tile // per_src, (t + 1) * tile // per_src):
            mask = ORDER[place]
            dev = partner(me, mask)
            src = z_s.at[e, pl.ds(place * per_src, per_src), :]
            dst = ret_ref.at[me * n_exp + e]
            if mask == 0:
                pltpu.make_async_copy(src, dst, local_sem).start()
            else:
                pltpu.make_async_remote_copy(
                    src_ref=src, dst_ref=dst, send_sem=send_sem, recv_sem=recv_sem,
                    device_id=(dev,), device_id_type=MESH).start()

    @pl.when(e == n_exp - 1)
    def _():
        sent = z_s.at[:, pl.ds(0, (N_DEV - 1) * per_src), :]
        pltpu.make_async_copy(sent, sent, send_sem).wait()
        own = z_s.at[:, pl.ds(0, per_src), :]
        pltpu.make_async_copy(own, own, local_sem).wait()
        arrived = ret_ref.at[pl.ds(0, (N_DEV - 1) * n_exp)]
        pltpu.make_async_copy(arrived, arrived, recv_sem).wait()


def back_kernel(ret_ref, hidden_ref, meta_ref, auxr_ref, out_ref, aux_ref, *, n_groups):
    experts, rows, d_model = ret_ref.shape
    seq = hidden_ref.shape[1]
    z = ret_ref[...].reshape(experts * rows, d_model)
    slot_id = lax.broadcasted_iota(jnp.int32, (seq, experts * rows), 1)
    for grp in range(2):
        meta = meta_ref[grp]
        c1 = meta[:, 0:1].astype(jnp.int32)
        c2 = meta[:, 1:2].astype(jnp.int32)
        comb = jnp.where(slot_id == c1, meta[:, 2:3], 0.0) + jnp.where(slot_id == c2, meta[:, 3:4], 0.0)
        moe = dot(comb.astype(BF16), z)
        out_ref[grp] = (hidden_ref[grp].astype(F32) + moe).astype(BF16)

    @pl.when(pl.program_id(0) == 0)
    def _():
        total = jnp.sum(auxr_ref[...], axis=0)
        total = jnp.sum(jnp.sum(total, axis=1, keepdims=True), axis=0, keepdims=True)
        aux_ref[...] = jnp.broadcast_to(total * (experts / n_groups), aux_ref.shape)


def solution(mesh):
    def local_step(tokens, pad_mask, second_draw, choices, norm_attn, w_query, w_key, w_value, w_attn_out, norm_moe, w_gate, w_in, w_out):
        groups, seq, d_model = tokens.shape
        _, heads, head_dim = w_query.shape
        experts = w_gate.shape[1]
        ff = w_in.shape[2]
        e_loc = experts // N_DEV
        capacity = (2 * seq + experts - 1) // experts
        hw = heads * head_dim
        rows = 2 * capacity
        steps = groups // 2
        all_rows = N_DEV * steps * rows

        wqkv = jnp.concatenate([w.reshape(d_model, hw) for w in (w_query, w_key, w_value)], axis=1)
        wo = w_attn_out.reshape(hw, d_model)
        cols = jnp.concatenate([
            pad_mask.astype(F32)[:, :, None], second_draw[:, :, None], choices.astype(F32)], axis=-1)
        keymask = pad_mask.reshape(groups, 1, seq)

        def whole(shape):
            return pl.BlockSpec(shape, lambda i: (0,) * len(shape), pipeline_mode=pl.Buffered(1))

        anywhere = pl.BlockSpec(memory_space=pl.ANY)
        hidden, meta, recv, auxr = pl.pallas_call(
            functools.partial(front_kernel, heads=heads, head_dim=head_dim, capacity=capacity),
            name="front",
            grid=(steps,),
            in_specs=[
                pl.BlockSpec((2, seq, d_model), lambda i: (i, 0, 0)),
                pl.BlockSpec((2, 1, seq), lambda i: (i, 0, 0)),
                pl.BlockSpec((2, seq, 4), lambda i: (i, 0, 0)),
                whole((1, d_model)), whole((d_model, 3 * hw)), whole((hw, d_model)),
                whole((1, d_model)), whole((d_model, experts)),
            ],
            out_specs=[
                pl.BlockSpec((2, seq, d_model), lambda i: (i, 0, 0)),
                pl.BlockSpec((2, seq, experts), lambda i: (i, 0, 0)),
                anywhere, anywhere,
            ],
            out_shape=[
                jax.ShapeDtypeStruct((groups, seq, d_model), BF16),
                jax.ShapeDtypeStruct((groups, seq, experts), F32),
                jax.ShapeDtypeStruct((e_loc, all_rows, d_model), BF16),
                jax.ShapeDtypeStruct((N_DEV, 8, experts), F32),
            ],
            scratch_shapes=[
                pltpu.VMEM((2 * seq, 3 * hw), BF16),
                pltpu.VMEM((2 * seq, hw), BF16),
                pltpu.VMEM((d_model, 3 * experts), BF16),
                pltpu.VMEM((8, experts), F32),
                pltpu.VMEM((steps, N_DEV, e_loc, rows, d_model), BF16),
                pltpu.SemaphoreType.DMA,
                pltpu.SemaphoreType.DMA,
                pltpu.SemaphoreType.DMA((2,)),
                pltpu.SemaphoreType.DMA,
                pltpu.SemaphoreType.DMA,
            ],
            compiler_params=pltpu.CompilerParams(
                dimension_semantics=("arbitrary",), collective_id=0, has_side_effects=True, vmem_limit_bytes=VMEM_LIMIT),
        )(tokens, keymask, cols, norm_attn.reshape(1, d_model), wqkv, wo, norm_moe.reshape(1, d_model), w_gate)

        tile = all_rows // 2
        ret = pl.pallas_call(
            functools.partial(expert_kernel, tile=tile),
            name="experts",
            grid=(e_loc,),
            in_specs=[
                pl.BlockSpec((1, all_rows, d_model), lambda i: (i, 0, 0)),
                pl.BlockSpec((1, d_model, ff), lambda i: (i, 0, 0)),
                pl.BlockSpec((1, ff, d_model), lambda i: (i, 0, 0)),
            ],
            out_specs=anywhere,
            out_shape=jax.ShapeDtypeStruct((experts, steps * rows, d_model), BF16),
            scratch_shapes=[
                pltpu.VMEM((tile, ff), BF16),
                pltpu.VMEM((e_loc, all_rows, d_model), BF16),
                pltpu.SemaphoreType.DMA,
                pltpu.SemaphoreType.DMA,
                pltpu.SemaphoreType.DMA,
            ],
            compiler_params=pltpu.CompilerParams(
                dimension_semantics=("arbitrary",), collective_id=1, has_side_effects=True, vmem_limit_bytes=VMEM_LIMIT),
        )(recv, w_in, w_out)

        out, aux = pl.pallas_call(
            functools.partial(back_kernel, n_groups=groups * N_DEV),
            name="back",
            grid=(steps,),
            in_specs=[
                pl.BlockSpec((experts, rows, d_model), lambda i: (0, i, 0)),
                pl.BlockSpec((2, seq, d_model), lambda i: (i, 0, 0)),
                pl.BlockSpec((2, seq, experts), lambda i: (i, 0, 0)),
                pl.BlockSpec((N_DEV, 8, experts), lambda i: (0, 0, 0)),
            ],
            out_specs=[
                pl.BlockSpec((2, seq, d_model), lambda i: (i, 0, 0)),
                pl.BlockSpec((8, experts), lambda i: (0, 0)),
            ],
            out_shape=[
                jax.ShapeDtypeStruct((groups, seq, d_model), BF16),
                jax.ShapeDtypeStruct((8, experts), F32),
            ],
            compiler_params=pltpu.CompilerParams(dimension_semantics=("arbitrary",), vmem_limit_bytes=VMEM_LIMIT),
        )(ret, hidden, meta, auxr)
        return out, aux[0, 0]

    by_group = P("ep")
    replicated = P()
    in_specs = (by_group, by_group, by_group, by_group, replicated, replicated, replicated, replicated, replicated, replicated, replicated, by_group, by_group)
    return jax.shard_map(local_step, mesh=mesh, in_specs=in_specs, out_specs=(by_group, replicated), check_vma=False)
```

```python
import functools
import jax
import jax.numpy as jnp
from jax import lax
from jax.experimental import pallas as pl
from jax.experimental.pallas import tpu as pltpu
from jax.sharding import PartitionSpec as P

NORM_EPS = 1e-6
N_DEV = 16
MESH = pl.DeviceIdType.MESH
F32 = jnp.float32
BF16 = jnp.bfloat16
ORDER = (0, 9, 2, 11, 4, 13, 6, 15, 8, 1, 10, 3, 12, 5, 14, 7)
VMEM_LIMIT = 62 * 1024 * 1024


def partner(me, mask):
    out = 0
    for bit in range(4):
        val = lax.rem(me // (1 << bit), 2)
        out = out + (1 << bit) * ((1 - val) if (mask >> bit) & 1 else val)
    return out


def greet(me):
    barrier = pltpu.get_barrier_semaphore()
    for mask in range(1, N_DEV):
        pl.semaphore_signal(barrier, inc=1, device_id=(partner(me, mask),), device_id_type=MESH)


def rms_norm(values_f, scale_vec):
    inv_rms = lax.rsqrt(jnp.mean(values_f * values_f, axis=-1, keepdims=True) + NORM_EPS)
    return (values_f * inv_rms * scale_vec).astype(BF16)


def dot(a, b):
    return jnp.dot(a, b, preferred_element_type=F32)


def dot_nt(a, b):
    return lax.dot_general(a, b, (((1,), (1,)), ((), ())), preferred_element_type=F32)


def front_kernel(
    tokens_ref, pad_ref, draw_ref, choices_ref, norm_attn_ref, wq_ref, wk_ref, wv_ref, wo_ref, norm_moe_ref, wgate_ref,
    hidden_ref, meta_ref, recv_ref, auxr_ref,
    q_s, k_s, v_s, ctx_s, s_s, p_s, wg_s, aux_s, send_s, send_sem, recv_sem, local_sem, aux_send_sem, aux_recv_sem,
    *, heads, head_dim, capacity,
):
    step = pl.program_id(0)
    steps = pl.num_programs(0)
    me = lax.axis_index("ep")
    seq = tokens_ref.shape[1]
    d_model = tokens_ref.shape[2]
    experts = wgate_ref.shape[1]
    e_loc = experts // N_DEV
    half = e_loc // 2
    slots = experts * capacity
    rows = 2 * capacity
    per_src = steps * rows

    def send_pair(pair):
        for place, mask in enumerate(ORDER):
            dev = partner(me, mask)
            src = send_s.at[pair, dev]
            dst = recv_ref.at[:, pl.ds(pl.multiple_of(place * per_src + pair * rows, rows), rows), :]
            if mask == 0:
                pltpu.make_async_copy(src, dst, local_sem.at[0]).start()
            else:
                pltpu.make_async_remote_copy(
                    src_ref=src, dst_ref=dst, send_sem=send_sem, recv_sem=recv_sem,
                    device_id=(dev,), device_id_type=MESH).start()

    @pl.when(step == 0)
    def _():
        greet(me)
        aux_s[...] = jnp.zeros_like(aux_s)
        wg = wgate_ref[...].T
        hi = wg.astype(BF16)
        rest = wg - hi.astype(F32)
        mid = rest.astype(BF16)
        low = (rest - mid.astype(F32)).astype(BF16)
        wg_s[0:experts] = hi
        wg_s[experts:2 * experts] = mid
        wg_s[2 * experts:3 * experts] = low

    @pl.when(step == 1)
    def _():
        pl.semaphore_wait(pltpu.get_barrier_semaphore(), N_DEV - 1)

    @pl.when(step > 0)
    def _():
        send_pair(step - 1)

    x = tokens_ref[...].reshape(2 * seq, d_model)
    a = rms_norm(x.astype(F32), norm_attn_ref[...][None, :])
    q_s[...] = dot_nt(wq_ref[...], a).astype(BF16)
    k_s[...] = dot_nt(a, wk_ref[...]).astype(BF16)
    v_s[...] = dot_nt(wv_ref[...], a).astype(BF16)

    width = 2 * head_dim
    lane = lax.broadcasted_iota(jnp.int32, (1, width), 1)
    scale = head_dim ** -0.5
    sides = [jnp.where(lane < head_dim, scale, 0.0).astype(BF16), jnp.where(lane < head_dim, 0.0, scale).astype(BF16)]
    cut = seq // 2
    late_key = lax.broadcasted_iota(jnp.int32, (seq - cut, 128), 0) + cut
    batch = s_s.shape[1]
    lanes = 128
    buf = 0
    for grp in range(2):
        tok = pl.ds(grp * seq, seq)
        length = jnp.sum(pad_ref[pl.ds(2 * step + grp, 1), :], axis=1, keepdims=True)
        keep_late = late_key < length
        for first in range(0, heads, batch):
            for i in range(batch):
                off = (first + i) // 2 * width
                k = k_s[tok, pl.ds(off, width)] * sides[(first + i) % 2]
                s_s[buf, i] = dot(k, q_s[pl.ds(off, width), tok])
            for i in range(batch):
                for col in range(0, seq, lanes):
                    cols = pl.ds(col, lanes)
                    early = s_s[buf, i, pl.ds(0, cut), cols]
                    late = jnp.where(keep_late, s_s[buf, i, pl.ds(cut, seq - cut), cols], -1e30)
                    top = jnp.maximum(jnp.max(early, axis=0, keepdims=True), jnp.max(late, axis=0, keepdims=True))
                    early = jnp.exp(early - top)
                    late = jnp.exp(late - top)
                    inv = 1.0 / (jnp.sum(early, axis=0, keepdims=True) + jnp.sum(late, axis=0, keepdims=True))
                    p_s[buf, i, pl.ds(0, cut), cols] = (early * inv).astype(BF16)
                    p_s[buf, i, pl.ds(cut, seq - cut), cols] = (late * inv).astype(BF16)
            for i in range(batch):
                head = pl.ds((first + i) * head_dim, head_dim)
                ctx_s[head, tok] = dot(v_s[head, tok], p_s[buf, i]).astype(BF16)
            buf = 1 - buf

    attn = lax.dot_general(ctx_s[...], wo_ref[...], (((0,), (0,)), ((), ())), preferred_element_type=F32)
    hidden = (x.astype(F32) + attn).astype(BF16)
    hidden_ref[...] = hidden.reshape(2, seq, d_model)
    b = rms_norm(hidden.astype(F32), norm_moe_ref[...][None, :])
    lg = dot_nt(wg_s[...], b)
    logits = (lg[2 * experts:] + lg[experts:2 * experts]) + lg[:experts]
    ex = jnp.exp(logits - jnp.max(logits, axis=0, keepdims=True))
    gate_probs = ex / jnp.sum(ex, axis=0, keepdims=True)

    eid = lax.broadcasted_iota(jnp.int32, (experts, seq), 0)
    tri = jnp.where(lax.broadcasted_iota(jnp.int32, (seq, seq), 0) <= lax.broadcasted_iota(jnp.int32, (seq, seq), 1), 1.0, 0.0).astype(BF16)
    slot_id = lax.broadcasted_iota(jnp.int32, (slots, seq), 0)
    meta_row = lax.broadcasted_iota(jnp.int32, (8, seq), 0)
    picked = []
    for grp in range(2):
        p = gate_probs[:, grp * seq:(grp + 1) * seq]
        valid = pad_ref[pl.ds(2 * step + grp, 1), :] == 1
        draw = draw_ref[pl.ds(2 * step + grp, 1), :]
        e1 = choices_ref[grp, 0:1, :]
        e2 = choices_ref[grp, 1:2, :]
        hot1 = eid == e1
        hot2 = eid == e2
        p1 = jnp.sum(jnp.where(hot1, p, 0.0), axis=0, keepdims=True)
        p2 = jnp.sum(jnp.where(hot2, p, 0.0), axis=0, keepdims=True)
        g1 = p1 / (p1 + p2)
        g2 = p2 / (p1 + p2)
        want2 = valid & (draw < 2.0 * g2)
        take1 = jnp.where(hot1 & valid, 1.0, 0.0)
        take2 = jnp.where(hot2 & want2, 1.0, 0.0)
        cum = dot(jnp.concatenate([take1, take2], axis=0).astype(BF16), tri)
        cum1 = cum[:experts]
        cum2 = cum[experts:]
        count1 = cum1[:, seq - 1:seq]
        pos1 = jnp.sum((cum1 - 1.0) * take1, axis=0, keepdims=True).astype(jnp.int32)
        pos2 = jnp.sum((cum2 - 1.0 + jnp.minimum(count1, float(capacity))) * take2, axis=0, keepdims=True).astype(jnp.int32)
        keep1 = valid & (pos1 < capacity)
        keep2 = want2 & (pos2 < capacity)

        share = jnp.where(valid, p, 0.0) * (count1 * (1.0 / (seq * seq)))
        share = jnp.sum(share.reshape(experts // 8, 8, seq), axis=0)
        for col in range(seq // 128):
            aux_s[...] += share[:, col * 128:(col + 1) * 128]

        def places(e, pos, keep):
            dev = e // e_loc
            r = e - dev * e_loc
            upper = r // half
            i = r - upper * half
            side = upper if grp == 0 else 1 - upper
            disp = ((dev * half + i) * 2 + side) * capacity + pos
            comb = (e * 2 + side) * capacity + pos
            return jnp.where(keep, disp, -1), jnp.where(keep, comb, -1)

        d1, c1 = places(e1, pos1, keep1)
        d2, c2 = places(e2, pos2, keep2)
        meta = jnp.where(meta_row == 0, c1.astype(F32), 0.0)
        meta = jnp.where(meta_row == 1, c2.astype(F32), meta)
        meta = jnp.where(meta_row == 2, g1, meta)
        meta = jnp.where(meta_row == 3, g2, meta)
        meta_ref[grp] = meta
        disp_mat = jnp.where((slot_id == d1) | (slot_id == d2), 1.0, 0.0).astype(BF16)
        got = dot(disp_mat, b[grp * seq:(grp + 1) * seq])
        picked.append(got.reshape(N_DEV * half, rows, d_model))

    top = lax.broadcasted_iota(jnp.int32, (1, rows, 1), 1) < capacity
    lower = jnp.where(top, picked[0], picked[1]).astype(BF16)
    upper = jnp.where(top, picked[1], picked[0]).astype(BF16)
    send_s[step, :, 0:half] = lower.reshape(N_DEV, half, rows, d_model)
    send_s[step, :, half:e_loc] = upper.reshape(N_DEV, half, rows, d_model)

    @pl.when(step == steps - 1)
    def _():
        send_pair(steps - 1)
        for mask in range(1, N_DEV):
            pltpu.make_async_remote_copy(
                src_ref=aux_s, dst_ref=auxr_ref.at[mask], send_sem=aux_send_sem, recv_sem=aux_recv_sem,
                device_id=(partner(me, mask),), device_id_type=MESH).start()
        own = pltpu.make_async_copy(aux_s, auxr_ref.at[0], local_sem.at[1])
        own.start()
        own.wait()
        others = pl.ds(0, N_DEV - 1)
        pltpu.make_async_copy(send_s.at[:, others], send_s.at[:, others], send_sem).wait()
        pltpu.make_async_copy(send_s.at[:, 0], send_s.at[:, 0], local_sem.at[0]).wait()
        pltpu.make_async_copy(auxr_ref.at[others], auxr_ref.at[others], aux_send_sem).wait()
        pltpu.make_async_copy(auxr_ref.at[others], auxr_ref.at[others], aux_recv_sem).wait()
        arrived = recv_ref.at[:, pl.ds(0, (N_DEV - 1) * per_src), :]
        pltpu.make_async_copy(arrived, arrived, recv_sem).wait()


def expert_kernel(recv_ref, w_in_ref, w_out_ref, ret_ref, act_s, z_s, send_sem, recv_sem, local_sem, *, tile):
    e = pl.program_id(0)
    n_exp = pl.num_programs(0)
    me = lax.axis_index("ep")
    rows = recv_ref.shape[1]
    ff = w_in_ref.shape[2]
    per_src = rows // N_DEV
    n_tiles = rows // tile
    chunk = 1024

    @pl.when(e == 0)
    def _():
        greet(me)

    for t in range(n_tiles):
        x = recv_ref[0, pl.ds(t * tile, tile), :]
        for f in range(ff // chunk):
            act = dot(x, w_in_ref[0, :, pl.ds(f * chunk, chunk)])
            act_s[:, pl.ds(f * chunk, chunk)] = jnp.maximum(act, 0.0).astype(BF16)
        z_s[e, pl.ds(t * tile, tile), :] = dot(act_s[...], w_out_ref[0]).astype(BF16)

        if t == 0:
            @pl.when(e == 0)
            def _():
                pl.semaphore_wait(pltpu.get_barrier_semaphore(), N_DEV - 1)

        for place in range(t * tile // per_src, (t + 1) * tile // per_src):
            mask = ORDER[place]
            dev = partner(me, mask)
            src = z_s.at[e, pl.ds(place * per_src, per_src), :]
            dst = ret_ref.at[me * n_exp + e]
            if mask == 0:
                pltpu.make_async_copy(src, dst, local_sem).start()
            else:
                pltpu.make_async_remote_copy(
                    src_ref=src, dst_ref=dst, send_sem=send_sem, recv_sem=recv_sem,
                    device_id=(dev,), device_id_type=MESH).start()

    @pl.when(e == n_exp - 1)
    def _():
        sent = z_s.at[:, pl.ds(0, (N_DEV - 1) * per_src), :]
        pltpu.make_async_copy(sent, sent, send_sem).wait()
        own = z_s.at[:, pl.ds(0, per_src), :]
        pltpu.make_async_copy(own, own, local_sem).wait()
        arrived = ret_ref.at[pl.ds(0, (N_DEV - 1) * n_exp)]
        pltpu.make_async_copy(arrived, arrived, recv_sem).wait()


def back_kernel(ret_ref, hidden_ref, meta_ref, auxr_ref, out_ref, aux_ref, *, n_groups):
    experts, rows, d_model = ret_ref.shape
    seq = hidden_ref.shape[1]
    z = ret_ref[...].reshape(experts * rows, d_model)
    slot_id = lax.broadcasted_iota(jnp.int32, (seq, experts * rows), 1)
    for grp in range(2):
        meta = meta_ref[grp].T
        c1 = meta[:, 0:1].astype(jnp.int32)
        c2 = meta[:, 1:2].astype(jnp.int32)
        comb = jnp.where(slot_id == c1, meta[:, 2:3], 0.0) + jnp.where(slot_id == c2, meta[:, 3:4], 0.0)
        moe = dot(comb.astype(BF16), z)
        out_ref[grp] = (hidden_ref[grp].astype(F32) + moe).astype(BF16)

    @pl.when(pl.program_id(0) == 0)
    def _():
        total = jnp.sum(auxr_ref[...], axis=0)
        total = jnp.sum(jnp.sum(total, axis=1, keepdims=True), axis=0, keepdims=True)
        aux_ref[...] = jnp.broadcast_to(total * (experts / n_groups), aux_ref.shape)


def solution(mesh):
    def local_step(tokens, pad_mask, second_draw, choices, norm_attn, w_query, w_key, w_value, w_attn_out, norm_moe, w_gate, w_in, w_out):
        groups, seq, d_model = tokens.shape
        _, heads, head_dim = w_query.shape
        experts = w_gate.shape[1]
        ff = w_in.shape[2]
        e_loc = experts // N_DEV
        capacity = (2 * seq + experts - 1) // experts
        hw = heads * head_dim
        rows = 2 * capacity
        steps = groups // 2
        all_rows = N_DEV * steps * rows

        wq, wk, wv = (w.transpose(1, 2, 0).reshape(hw, d_model) for w in (w_query, w_key, w_value))
        wo = w_attn_out.reshape(hw, d_model)

        def whole(shape):
            return pl.BlockSpec(shape, lambda i: (0,) * len(shape), pipeline_mode=pl.Buffered(1))

        anywhere = pl.BlockSpec(memory_space=pl.ANY)
        hidden, meta, recv, auxr = pl.pallas_call(
            functools.partial(front_kernel, heads=heads, head_dim=head_dim, capacity=capacity),
            name="front",
            grid=(steps,),
            in_specs=[
                pl.BlockSpec((2, seq, d_model), lambda i: (i, 0, 0)),
                whole((groups, seq)), whole((groups, seq)),
                pl.BlockSpec((2, 2, seq), lambda i: (i, 0, 0)),
                whole((d_model,)), whole((hw, d_model)), whole((hw, d_model)), whole((hw, d_model)), whole((hw, d_model)),
                whole((d_model,)), whole((d_model, experts)),
            ],
            out_specs=[
                pl.BlockSpec((2, seq, d_model), lambda i: (i, 0, 0)),
                pl.BlockSpec((2, 8, seq), lambda i: (i, 0, 0)),
                anywhere, anywhere,
            ],
            out_shape=[
                jax.ShapeDtypeStruct((groups, seq, d_model), BF16),
                jax.ShapeDtypeStruct((groups, 8, seq), F32),
                jax.ShapeDtypeStruct((e_loc, all_rows, d_model), BF16),
                jax.ShapeDtypeStruct((N_DEV, 8, 128), F32),
            ],
            scratch_shapes=[
                pltpu.VMEM((hw, 2 * seq), BF16),
                pltpu.VMEM((2 * seq, hw), BF16),
                pltpu.VMEM((hw, 2 * seq), BF16),
                pltpu.VMEM((hw, 2 * seq), BF16),
                pltpu.VMEM((2, 4, seq, seq), F32),
                pltpu.VMEM((2, 4, seq, seq), BF16),
                pltpu.VMEM((3 * experts, d_model), BF16),
                pltpu.VMEM((8, 128), F32),
                pltpu.VMEM((steps, N_DEV, e_loc, rows, d_model), BF16),
                pltpu.SemaphoreType.DMA,
                pltpu.SemaphoreType.DMA,
                pltpu.SemaphoreType.DMA((2,)),
                pltpu.SemaphoreType.DMA,
                pltpu.SemaphoreType.DMA,
            ],
            compiler_params=pltpu.CompilerParams(
                dimension_semantics=("arbitrary",), collective_id=0, has_side_effects=True, vmem_limit_bytes=VMEM_LIMIT),
        )(tokens, pad_mask, second_draw, choices.transpose(0, 2, 1), norm_attn, wq, wk, wv, wo, norm_moe, w_gate)

        tile = all_rows // 2
        ret = pl.pallas_call(
            functools.partial(expert_kernel, tile=tile),
            name="experts",
            grid=(e_loc,),
            in_specs=[
                pl.BlockSpec((1, all_rows, d_model), lambda i: (i, 0, 0)),
                pl.BlockSpec((1, d_model, ff), lambda i: (i, 0, 0)),
                pl.BlockSpec((1, ff, d_model), lambda i: (i, 0, 0)),
            ],
            out_specs=anywhere,
            out_shape=jax.ShapeDtypeStruct((experts, steps * rows, d_model), BF16),
            scratch_shapes=[
                pltpu.VMEM((tile, ff), BF16),
                pltpu.VMEM((e_loc, all_rows, d_model), BF16),
                pltpu.SemaphoreType.DMA,
                pltpu.SemaphoreType.DMA,
                pltpu.SemaphoreType.DMA,
            ],
            compiler_params=pltpu.CompilerParams(
                dimension_semantics=("arbitrary",), collective_id=1, has_side_effects=True, vmem_limit_bytes=VMEM_LIMIT),
        )(recv, w_in, w_out)

        out, aux = pl.pallas_call(
            functools.partial(back_kernel, n_groups=groups * N_DEV),
            name="back",
            grid=(steps,),
            in_specs=[
                pl.BlockSpec((experts, rows, d_model), lambda i: (0, i, 0)),
                pl.BlockSpec((2, seq, d_model), lambda i: (i, 0, 0)),
                pl.BlockSpec((2, 8, seq), lambda i: (i, 0, 0)),
                pl.BlockSpec((N_DEV, 8, 128), lambda i: (0, 0, 0)),
            ],
            out_specs=[
                pl.BlockSpec((2, seq, d_model), lambda i: (i, 0, 0)),
                pl.BlockSpec((8, 128), lambda i: (0, 0)),
            ],
            out_shape=[
                jax.ShapeDtypeStruct((groups, seq, d_model), BF16),
                jax.ShapeDtypeStruct((8, 128), F32),
            ],
            compiler_params=pltpu.CompilerParams(dimension_semantics=("arbitrary",), vmem_limit_bytes=VMEM_LIMIT),
        )(ret, hidden, meta, auxr)
        return out, aux[0, 0]

    by_group = P("ep")
    replicated = P()
    in_specs = (by_group, by_group, by_group, by_group, replicated, replicated, replicated, replicated, replicated, replicated, replicated, by_group, by_group)
    return jax.shard_map(local_step, mesh=mesh, in_specs=in_specs, out_specs=(by_group, replicated), check_vma=False)
```

```python
import functools
import jax
import jax.numpy as jnp
from jax import lax
from jax.experimental import pallas as pl
from jax.experimental.pallas import tpu as pltpu
from jax.sharding import PartitionSpec as P

NORM_EPS = 1e-6
N_DEV = 16
MESH = pl.DeviceIdType.MESH
F32 = jnp.float32
BF16 = jnp.bfloat16
ORDER = (0, 9, 2, 11, 4, 13, 6, 15, 8, 1, 10, 3, 12, 5, 14, 7)
VMEM_LIMIT = 62 * 1024 * 1024


def partner(me, mask):
    out = 0
    for bit in range(4):
        val = lax.rem(me // (1 << bit), 2)
        out = out + (1 << bit) * ((1 - val) if (mask >> bit) & 1 else val)
    return out


def greet(me):
    barrier = pltpu.get_barrier_semaphore()
    for mask in range(1, N_DEV):
        pl.semaphore_signal(barrier, inc=1, device_id=(partner(me, mask),), device_id_type=MESH)


def rms_norm(values_f, scale_vec):
    inv_rms = lax.rsqrt(jnp.mean(values_f * values_f, axis=-1, keepdims=True) + NORM_EPS)
    return (values_f * inv_rms * scale_vec).astype(BF16)


def dot(a, b):
    return jnp.dot(a, b, preferred_element_type=F32)


def dot_nt(a, b):
    return lax.dot_general(a, b, (((1,), (1,)), ((), ())), preferred_element_type=F32)


def split_gate(wgate_ref, wg_s):
    experts = wgate_ref.shape[1]
    wg = wgate_ref[...].T
    hi = wg.astype(BF16)
    rest = wg - hi.astype(F32)
    mid = rest.astype(BF16)
    low = (rest - mid.astype(F32)).astype(BF16)
    wg_s[0:experts] = hi
    wg_s[experts:2 * experts] = mid
    wg_s[2 * experts:3 * experts] = low


def attend(
    step, tokens_ref, pad_ref, norm_attn_ref, wq_ref, wk_ref, wv_ref, wo_ref, norm_moe_ref, hidden_ref,
    q_s, k_s, v_s, ctx_s, s_s, p_s, wg_s, heads, head_dim, experts,
):
    seq = tokens_ref.shape[1]
    d_model = tokens_ref.shape[2]
    x = tokens_ref[...].reshape(2 * seq, d_model)
    a = rms_norm(x.astype(F32), norm_attn_ref[...][None, :])
    q_s[...] = dot_nt(wq_ref[...], a).astype(BF16)
    k_s[...] = dot_nt(a, wk_ref[...]).astype(BF16)
    v_s[...] = dot_nt(wv_ref[...], a).astype(BF16)

    width = 2 * head_dim
    lane = lax.broadcasted_iota(jnp.int32, (1, width), 1)
    scale = head_dim ** -0.5
    sides = [jnp.where(lane < head_dim, scale, 0.0).astype(BF16), jnp.where(lane < head_dim, 0.0, scale).astype(BF16)]
    cut = seq // 2
    late_key = lax.broadcasted_iota(jnp.int32, (seq - cut, 128), 0) + cut
    batch = s_s.shape[1]
    lanes = 128
    buf = 0
    for grp in range(2):
        tok = pl.ds(grp * seq, seq)
        length = jnp.sum(pad_ref[pl.ds(2 * step + grp, 1), :], axis=1, keepdims=True)
        keep_late = late_key < length
        for first in range(0, heads, batch):
            for i in range(batch):
                off = (first + i) // 2 * width
                k = k_s[tok, pl.ds(off, width)] * sides[(first + i) % 2]
                s_s[buf, i] = dot(k, q_s[pl.ds(off, width), tok])
            for i in range(batch):
                for col in range(0, seq, lanes):
                    cols = pl.ds(col, lanes)
                    early = s_s[buf, i, pl.ds(0, cut), cols]
                    late = jnp.where(keep_late, s_s[buf, i, pl.ds(cut, seq - cut), cols], -1e30)
                    top = jnp.maximum(jnp.max(early, axis=0, keepdims=True), jnp.max(late, axis=0, keepdims=True))
                    early = jnp.exp(early - top)
                    late = jnp.exp(late - top)
                    inv = 1.0 / (jnp.sum(early, axis=0, keepdims=True) + jnp.sum(late, axis=0, keepdims=True))
                    p_s[buf, i, pl.ds(0, cut), cols] = (early * inv).astype(BF16)
                    p_s[buf, i, pl.ds(cut, seq - cut), cols] = (late * inv).astype(BF16)
            for i in range(batch):
                head = pl.ds((first + i) * head_dim, head_dim)
                ctx_s[head, tok] = dot(v_s[head, tok], p_s[buf, i]).astype(BF16)
            buf = 1 - buf

    attn = lax.dot_general(ctx_s[...], wo_ref[...], (((0,), (0,)), ((), ())), preferred_element_type=F32)
    hidden = (x.astype(F32) + attn).astype(BF16)
    hidden_ref[...] = hidden.reshape(2, seq, d_model)
    b = rms_norm(hidden.astype(F32), norm_moe_ref[...][None, :])
    lg = dot_nt(wg_s[...], b)
    logits = (lg[2 * experts:] + lg[experts:2 * experts]) + lg[:experts]
    ex = jnp.exp(logits - jnp.max(logits, axis=0, keepdims=True))
    return b, ex / jnp.sum(ex, axis=0, keepdims=True)


def front_kernel(
    tokens_ref, pad_ref, draw_ref, choices_ref, norm_attn_ref, wq_ref, wk_ref, wv_ref, wo_ref, norm_moe_ref, wgate_ref,
    hidden_ref, meta_ref, recv_ref, auxr_ref,
    q_s, k_s, v_s, ctx_s, s_s, p_s, wg_s, aux_s, send_s, send_sem, recv_sem, local_sem, aux_send_sem, aux_recv_sem,
    *, heads, head_dim, capacity,
):
    step = pl.program_id(0)
    steps = pl.num_programs(0)
    me = lax.axis_index("ep")
    seq = tokens_ref.shape[1]
    d_model = tokens_ref.shape[2]
    experts = wgate_ref.shape[1]
    e_loc = experts // N_DEV
    half = e_loc // 2
    slots = experts * capacity
    rows = 2 * capacity
    per_src = steps * rows

    def send_pair(pair):
        for place, mask in enumerate(ORDER):
            dev = partner(me, mask)
            src = send_s.at[pair, dev]
            dst = recv_ref.at[:, pl.ds(pl.multiple_of(place * per_src + pair * rows, rows), rows), :]
            if mask == 0:
                pltpu.make_async_copy(src, dst, local_sem.at[0]).start()
            else:
                pltpu.make_async_remote_copy(
                    src_ref=src, dst_ref=dst, send_sem=send_sem, recv_sem=recv_sem,
                    device_id=(dev,), device_id_type=MESH).start()

    @pl.when(step == 0)
    def _():
        greet(me)
        aux_s[...] = jnp.zeros_like(aux_s)
        split_gate(wgate_ref, wg_s)

    @pl.when(step == 1)
    def _():
        pl.semaphore_wait(pltpu.get_barrier_semaphore(), N_DEV - 1)

    @pl.when(step > 0)
    def _():
        send_pair(step - 1)

    b, gate_probs = attend(
        step, tokens_ref, pad_ref, norm_attn_ref, wq_ref, wk_ref, wv_ref, wo_ref, norm_moe_ref, hidden_ref,
        q_s, k_s, v_s, ctx_s, s_s, p_s, wg_s, heads, head_dim, experts)

    eid = lax.broadcasted_iota(jnp.int32, (experts, seq), 0)
    tri = jnp.where(lax.broadcasted_iota(jnp.int32, (seq, seq), 0) <= lax.broadcasted_iota(jnp.int32, (seq, seq), 1), 1.0, 0.0).astype(BF16)
    slot_id = lax.broadcasted_iota(jnp.int32, (slots, seq), 0)
    meta_row = lax.broadcasted_iota(jnp.int32, (8, seq), 0)
    picked = []
    for grp in range(2):
        p = gate_probs[:, grp * seq:(grp + 1) * seq]
        valid = pad_ref[pl.ds(2 * step + grp, 1), :] == 1
        draw = draw_ref[pl.ds(2 * step + grp, 1), :]
        e1 = choices_ref[grp, 0:1, :]
        e2 = choices_ref[grp, 1:2, :]
        hot1 = eid == e1
        hot2 = eid == e2
        p1 = jnp.sum(jnp.where(hot1, p, 0.0), axis=0, keepdims=True)
        p2 = jnp.sum(jnp.where(hot2, p, 0.0), axis=0, keepdims=True)
        g1 = p1 / (p1 + p2)
        g2 = p2 / (p1 + p2)
        want2 = valid & (draw < 2.0 * g2)
        take1 = jnp.where(hot1 & valid, 1.0, 0.0)
        take2 = jnp.where(hot2 & want2, 1.0, 0.0)
        cum = dot(jnp.concatenate([take1, take2], axis=0).astype(BF16), tri)
        cum1 = cum[:experts]
        cum2 = cum[experts:]
        count1 = cum1[:, seq - 1:seq]
        pos1 = jnp.sum((cum1 - 1.0) * take1, axis=0, keepdims=True).astype(jnp.int32)
        pos2 = jnp.sum((cum2 - 1.0 + jnp.minimum(count1, float(capacity))) * take2, axis=0, keepdims=True).astype(jnp.int32)
        keep1 = valid & (pos1 < capacity)
        keep2 = want2 & (pos2 < capacity)

        share = jnp.where(valid, p, 0.0) * (count1 * (1.0 / (seq * seq)))
        share = jnp.sum(share.reshape(experts // 8, 8, seq), axis=0)
        for col in range(seq // 128):
            aux_s[...] += share[:, col * 128:(col + 1) * 128]

        def places(e, pos, keep):
            dev = e // e_loc
            r = e - dev * e_loc
            upper = r // half
            i = r - upper * half
            side = upper if grp == 0 else 1 - upper
            disp = ((dev * half + i) * 2 + side) * capacity + pos
            comb = (e * 2 + side) * capacity + pos
            return jnp.where(keep, disp, -1), jnp.where(keep, comb, -1)

        d1, c1 = places(e1, pos1, keep1)
        d2, c2 = places(e2, pos2, keep2)
        meta = jnp.where(meta_row == 0, c1.astype(F32), 0.0)
        meta = jnp.where(meta_row == 1, c2.astype(F32), meta)
        meta = jnp.where(meta_row == 2, g1, meta)
        meta = jnp.where(meta_row == 3, g2, meta)
        meta_ref[grp] = meta
        disp_mat = jnp.where((slot_id == d1) | (slot_id == d2), 1.0, 0.0).astype(BF16)
        got = dot(disp_mat, b[grp * seq:(grp + 1) * seq])
        picked.append(got.reshape(N_DEV * half, rows, d_model))

    top = lax.broadcasted_iota(jnp.int32, (1, rows, 1), 1) < capacity
    lower = jnp.where(top, picked[0], picked[1]).astype(BF16)
    upper = jnp.where(top, picked[1], picked[0]).astype(BF16)
    send_s[step, :, 0:half] = lower.reshape(N_DEV, half, rows, d_model)
    send_s[step, :, half:e_loc] = upper.reshape(N_DEV, half, rows, d_model)

    @pl.when(step == steps - 1)
    def _():
        send_pair(steps - 1)
        for mask in range(1, N_DEV):
            pltpu.make_async_remote_copy(
                src_ref=aux_s, dst_ref=auxr_ref.at[mask], send_sem=aux_send_sem, recv_sem=aux_recv_sem,
                device_id=(partner(me, mask),), device_id_type=MESH).start()
        own = pltpu.make_async_copy(aux_s, auxr_ref.at[0], local_sem.at[1])
        own.start()
        own.wait()
        others = pl.ds(0, N_DEV - 1)
        pltpu.make_async_copy(send_s.at[:, others], send_s.at[:, others], send_sem).wait()
        pltpu.make_async_copy(send_s.at[:, 0], send_s.at[:, 0], local_sem.at[0]).wait()
        pltpu.make_async_copy(auxr_ref.at[others], auxr_ref.at[others], aux_send_sem).wait()
        pltpu.make_async_copy(auxr_ref.at[others], auxr_ref.at[others], aux_recv_sem).wait()
        arrived = recv_ref.at[:, pl.ds(0, (N_DEV - 1) * per_src), :]
        pltpu.make_async_copy(arrived, arrived, recv_sem).wait()


def expert_kernel(recv_ref, w_in_ref, w_out_ref, ret_ref, act_s, z_s, send_sem, recv_sem, local_sem, *, tile):
    e = pl.program_id(0)
    n_exp = pl.num_programs(0)
    me = lax.axis_index("ep")
    rows = recv_ref.shape[1]
    ff = w_in_ref.shape[2]
    per_src = rows // N_DEV
    n_tiles = rows // tile
    chunk = 1024

    @pl.when(e == 0)
    def _():
        greet(me)

    for t in range(n_tiles):
        x = recv_ref[0, pl.ds(t * tile, tile), :]
        for f in range(ff // chunk):
            act = dot(x, w_in_ref[0, :, pl.ds(f * chunk, chunk)])
            act_s[:, pl.ds(f * chunk, chunk)] = jnp.maximum(act, 0.0).astype(BF16)
        z_s[e, pl.ds(t * tile, tile), :] = dot(act_s[...], w_out_ref[0]).astype(BF16)

        if t == 0:
            @pl.when(e == 0)
            def _():
                pl.semaphore_wait(pltpu.get_barrier_semaphore(), N_DEV - 1)

        for place in range(t * tile // per_src, (t + 1) * tile // per_src):
            mask = ORDER[place]
            dev = partner(me, mask)
            src = z_s.at[e, pl.ds(place * per_src, per_src), :]
            dst = ret_ref.at[me * n_exp + e]
            if mask == 0:
                pltpu.make_async_copy(src, dst, local_sem).start()
            else:
                pltpu.make_async_remote_copy(
                    src_ref=src, dst_ref=dst, send_sem=send_sem, recv_sem=recv_sem,
                    device_id=(dev,), device_id_type=MESH).start()

    @pl.when(e == n_exp - 1)
    def _():
        sent = z_s.at[:, pl.ds(0, (N_DEV - 1) * per_src), :]
        pltpu.make_async_copy(sent, sent, send_sem).wait()
        own = z_s.at[:, pl.ds(0, per_src), :]
        pltpu.make_async_copy(own, own, local_sem).wait()
        arrived = ret_ref.at[pl.ds(0, (N_DEV - 1) * n_exp)]
        pltpu.make_async_copy(arrived, arrived, recv_sem).wait()


def back_kernel(ret_ref, hidden_ref, meta_ref, auxr_ref, out_ref, aux_ref, *, n_groups):
    experts, rows, d_model = ret_ref.shape
    seq = hidden_ref.shape[1]
    z = ret_ref[...].reshape(experts * rows, d_model)
    slot_id = lax.broadcasted_iota(jnp.int32, (seq, experts * rows), 1)
    for grp in range(2):
        meta = meta_ref[grp].T
        c1 = meta[:, 0:1].astype(jnp.int32)
        c2 = meta[:, 1:2].astype(jnp.int32)
        comb = jnp.where(slot_id == c1, meta[:, 2:3], 0.0) + jnp.where(slot_id == c2, meta[:, 3:4], 0.0)
        moe = dot(comb.astype(BF16), z)
        out_ref[grp] = (hidden_ref[grp].astype(F32) + moe).astype(BF16)

    @pl.when(pl.program_id(0) == 0)
    def _():
        total = jnp.sum(auxr_ref[...], axis=0)
        total = jnp.sum(jnp.sum(total, axis=1, keepdims=True), axis=0, keepdims=True)
        aux_ref[...] = jnp.broadcast_to(total * (experts / n_groups), aux_ref.shape)


FIX = 8
LOCAL = 48
PACK = 112
EXTRA = 32


def twice(value):
    return jnp.concatenate([value, value], axis=1)


def packed_front_kernel(
    tokens_ref, pad_ref, draw_ref, choices_ref, norm_attn_ref, wq_ref, wk_ref, wv_ref, wo_ref, norm_moe_ref, wgate_ref,
    hidden_ref, meta_ref, fix_ref, pack_ref, msg_ref,
    q_s, k_s, v_s, ctx_s, s_s, p_s, wg_s, b_s, slot_s, count_s, aux_s, flag_s, code_s, goal_s,
    local_s, fix_s, pack_s, msg_s, fix_send, fix_recv, pack_send, pack_recv, msg_send, msg_recv, own_sem,
    *, heads, head_dim, capacity,
):
    step = pl.program_id(0)
    steps = pl.num_programs(0)
    quad = step // 2
    quads = steps // 2
    me = lax.axis_index("ep")
    seq = tokens_ref.shape[1]
    d_model = tokens_ref.shape[2]
    experts = wgate_ref.shape[1]
    e_loc = experts // N_DEV

    def remote(src, dst, send_sem, recv_sem, dev, mask, own):
        if mask == 0:
            pltpu.make_async_copy(src, dst, own_sem.at[own]).start()
        else:
            pltpu.make_async_remote_copy(
                src_ref=src, dst_ref=dst, send_sem=send_sem, recv_sem=recv_sem,
                device_id=(dev,), device_id_type=MESH).start()

    def send_quad(which):
        for place, mask in enumerate(ORDER):
            dev = partner(me, mask)
            row = pl.multiple_of(place * quads * FIX + which * FIX, FIX)
            remote(fix_s.at[which, dev], fix_ref.at[:, pl.ds(row, FIX), :], fix_send, fix_recv, dev, mask, 0)

    @pl.when(step == 0)
    def _():
        greet(me)
        split_gate(wgate_ref, wg_s)
        aux_s[...] = jnp.zeros_like(aux_s)
        flag_s[...] = jnp.zeros_like(flag_s)
        code_s[...] = jnp.zeros_like(code_s)
        goal_s[...] = jnp.zeros_like(goal_s)
        count_s[...] = jnp.zeros_like(count_s)

    @pl.when(step == 2)
    def _():
        pl.semaphore_wait(pltpu.get_barrier_semaphore(), N_DEV - 1)

    @pl.when((step > 0) & (lax.rem(step, 2) == 0))
    def _():
        send_quad(quad - 1)

    b, gate_probs = attend(
        step, tokens_ref, pad_ref, norm_attn_ref, wq_ref, wk_ref, wv_ref, wo_ref, norm_moe_ref, hidden_ref,
        q_s, k_s, v_s, ctx_s, s_s, p_s, wg_s, heads, head_dim, experts)
    side = lax.rem(step, 2)
    b_s[pl.ds(pl.multiple_of(side * 2 * seq, 2 * seq), 2 * seq), :] = b

    eid = lax.broadcasted_iota(jnp.int32, (experts, seq), 0)
    tri = jnp.where(lax.broadcasted_iota(jnp.int32, (seq, seq), 0) <= lax.broadcasted_iota(jnp.int32, (seq, seq), 1), 1.0, 0.0)
    tri = jnp.concatenate([tri, jnp.ones((seq, 128), F32)], axis=1).astype(BF16)
    row_e = lax.broadcasted_iota(jnp.int32, (experts, experts), 0)
    col_e = lax.broadcasted_iota(jnp.int32, (experts, experts), 1)
    same = row_e // e_loc == col_e // e_loc
    mix = jnp.concatenate([jnp.where(same & (col_e < row_e), 1.0, 0.0), jnp.where(same, 1.0, 0.0)], axis=0).astype(BF16)
    spot = lax.broadcasted_iota(jnp.int32, (experts, 128), 1).astype(F32)
    code0 = (lax.rem(lax.broadcasted_iota(jnp.int32, (experts, 128), 0), e_loc) * EXTRA + 1).astype(F32)
    meta_row = lax.broadcasted_iota(jnp.int32, (8, seq), 0)
    for grp in range(2):
        p = gate_probs[:, grp * seq:(grp + 1) * seq]
        valid = pad_ref[pl.ds(2 * step + grp, 1), :] == 1
        draw = draw_ref[pl.ds(2 * step + grp, 1), :]
        e1 = choices_ref[grp, 0:1, :]
        e2 = choices_ref[grp, 1:2, :]
        hot1 = eid == e1
        hot2 = eid == e2
        p1 = jnp.sum(jnp.where(hot1, p, 0.0), axis=0, keepdims=True)
        p2 = jnp.sum(jnp.where(hot2, p, 0.0), axis=0, keepdims=True)
        g1 = p1 / (p1 + p2)
        g2 = p2 / (p1 + p2)
        want2 = valid & (draw < 2.0 * g2)
        take1 = jnp.where(hot1 & valid, 1.0, 0.0)
        take2 = jnp.where(hot2 & want2, 1.0, 0.0)
        cum = dot(jnp.concatenate([take1, take2], axis=0).astype(BF16), tri)
        cum1 = cum[:experts, :seq]
        cum2 = cum[experts:, :seq]
        count1 = cum[:experts, seq:]
        count2 = cum[experts:, seq:]
        first = jnp.minimum(count1, float(capacity))
        pos1 = jnp.sum((cum1 - 1.0) * take1, axis=0, keepdims=True)
        pos2 = jnp.sum((cum2 - 1.0 + twice(first)) * take2, axis=0, keepdims=True)
        keep1 = valid & (pos1 < capacity)
        keep2 = want2 & (pos2 < capacity)

        share = jnp.where(valid, p, 0.0) * twice(count1 * (1.0 / (seq * seq)))
        share = jnp.sum(share.reshape(experts // 8, 8, seq), axis=0)
        for col in range(seq // 128):
            aux_s[...] += share[:, col * 128:(col + 1) * 128]

        before = count_s[0]
        after = before + jnp.minimum(first + count2, float(capacity))
        new = jnp.maximum(after - FIX, 0.0) - jnp.maximum(before - FIX, 0.0)
        sums = dot(mix, new.astype(BF16))
        packed = count_s[1]
        begin = packed + sums[:experts]
        shift = begin - jnp.maximum(before, float(FIX)) + before
        local = shift - count_s[3]
        inside = (spot >= begin) & (spot < begin + new)
        code = jnp.where(inside, code0 + count_s[2] + spot - begin, 0.0)
        code_s[...] += jnp.sum(code.reshape(N_DEV, e_loc, 128), axis=1)
        count_s[0] = after
        count_s[1] = packed + sums[experts:]
        count_s[2] += new

        def places(e, take, pos, keep):
            index = pos + jnp.sum(twice(before) * take, axis=0, keepdims=True)
            in_pack = pos + jnp.sum(twice(shift) * take, axis=0, keepdims=True)
            in_local = pos + jnp.sum(twice(local) * take, axis=0, keepdims=True)
            e = e.astype(F32)
            dev = jnp.floor(e * (1.0 / e_loc))
            fixed = keep & (index < FIX)
            loose = keep & (index >= FIX)
            at_fix = jnp.where(fixed, e * FIX + index, -1.0)
            at_local = jnp.where(loose, dev * LOCAL + in_local, -1.0)
            at_back = jnp.where(loose, experts * FIX + dev * PACK + in_pack, at_fix)
            return at_fix, at_local, at_back

        f1, l1, c1 = places(e1, take1, pos1, keep1)
        f2, l2, c2 = places(e2, take2, pos2, keep2)
        meta = jnp.where(meta_row == 0, c1, 0.0)
        meta = jnp.where(meta_row == 1, c2, meta)
        meta = jnp.where(meta_row == 2, g1, meta)
        meta = jnp.where(meta_row == 3, g2, meta)
        meta_ref[grp] = meta
        tok = pl.ds(pl.multiple_of(side * 2 * seq + grp * seq, seq), seq)
        slot_s[:, tok] = jnp.where(meta_row == 0, f1, jnp.where(meta_row == 1, f2, jnp.where(meta_row == 2, l1, l2))).astype(jnp.int32)

    @pl.when(side == 1)
    def _():
        def gather(first_row, base, count):
            ids = lax.broadcasted_iota(jnp.int32, (count, 4 * seq), 0) + base
            hit = (ids == slot_s[first_row:first_row + 1, :]) | (ids == slot_s[first_row + 1:first_row + 2, :])
            return dot(jnp.where(hit, 1.0, 0.0).astype(BF16), b_s[...]).astype(BF16)

        per_dev = e_loc * FIX
        for base in range(0, N_DEV, 4):
            rows = gather(0, base * per_dev, 4 * per_dev)
            fix_s[quad, base:base + 4] = rows.reshape(4, e_loc, FIX, d_model)
        for base in range(0, N_DEV, 4):
            rows = gather(2, base * LOCAL, 4 * LOCAL)
            local_s[base:base + 4, pl.ds(pl.multiple_of(quad * LOCAL, LOCAL), LOCAL), :] = rows.reshape(4, LOCAL, d_model)

        def per_device(value):
            return value.reshape(N_DEV, e_loc, 128)[:, 0, :]

        start = per_device(count_s[3])
        filled = per_device(count_s[1]) - start
        at = lax.broadcasted_iota(jnp.int32, (N_DEV, 256), 1).astype(F32) - (quad * LOCAL).astype(F32)
        live = (at >= 0.0) & (at < float(LOCAL)) & (at < twice(filled))
        goal_s[...] = jnp.where(live, twice(start) + at + 1.0, goal_s[...])
        flag_s[...] = jnp.maximum(flag_s[...], jnp.where(filled > LOCAL, 1.0, 0.0))
        count_s[0] = jnp.zeros_like(count_s[0])
        count_s[3] = count_s[1]

    @pl.when(step == steps - 1)
    def _():
        send_quad(quads - 1)
        width = goal_s.shape[1] * 3 // 4
        rows = lax.broadcasted_iota(jnp.int32, (PACK, width), 0).astype(F32) + 1.0
        for dev in range(N_DEV):
            hit = jnp.where(rows == goal_s[dev:dev + 1, 0:width], 1.0, 0.0).astype(BF16)
            pack_s[dev] = dot(hit, local_s[dev]).astype(BF16)
        over = jnp.where((count_s[1] > PACK) | (count_s[2] > EXTRA), 1.0, 0.0)
        over = jnp.max(jnp.max(over.reshape(N_DEV, e_loc, 128), axis=1), axis=0, keepdims=True)
        over = jnp.maximum(over, jnp.max(flag_s[...], axis=0, keepdims=True))
        for dev in range(N_DEV):
            msg_s[dev, 0:8] = aux_s[...]
            lower = lax.broadcasted_iota(jnp.int32, (8, 128), 0)
            msg_s[dev, 8:16] = jnp.where(lower == 0, code_s[dev:dev + 1, :], jnp.where(lower == 1, over, 0.0))
        for place, mask in enumerate(ORDER):
            dev = partner(me, mask)
            remote(pack_s.at[dev], pack_ref.at[place], pack_send, pack_recv, dev, mask, 1)
        for place, mask in enumerate(ORDER):
            dev = partner(me, mask)
            remote(msg_s.at[dev], msg_ref.at[place], msg_send, msg_recv, dev, mask, 2)

        def settle(ref, sem):
            pltpu.make_async_copy(ref, ref, sem).wait()

        others = pl.ds(0, N_DEV - 1)
        settle(fix_s.at[:, 0], own_sem.at[0])
        settle(pack_s.at[0], own_sem.at[1])
        settle(msg_s.at[0], own_sem.at[2])
        settle(fix_s.at[:, others], fix_send)
        settle(pack_s.at[others], pack_send)
        settle(msg_s.at[others], msg_send)
        settle(fix_ref.at[:, pl.ds(0, (N_DEV - 1) * quads * FIX), :], fix_recv)
        settle(pack_ref.at[others], pack_recv)
        settle(msg_ref.at[others], msg_recv)


def packed_expert_kernel(
    fix_ref, pack_ref, msg_ref, w_in_ref, w_out_ref, back_ref, back_pack_ref,
    act_s, x_s, z_s, zx_s, pack_s, fix_send, fix_recv, pack_send, pack_recv, own_sem,
):
    e = pl.program_id(0)
    n_exp = pl.num_programs(0)
    me = lax.axis_index("ep")
    rows = fix_ref.shape[1]
    d_model = fix_ref.shape[2]
    ff = w_in_ref.shape[2]
    per_src = rows // N_DEV
    chunk = 1024

    def mlp(x):
        for f in range(ff // chunk):
            act = dot(x, w_in_ref[0, :, pl.ds(f * chunk, chunk)])
            act_s[:, pl.ds(f * chunk, chunk)] = jnp.maximum(act, 0.0).astype(BF16)
        return dot(act_s[...], w_out_ref[0]).astype(BF16)

    def spread(place):
        ids = lax.broadcasted_iota(jnp.int32, (n_exp * EXTRA, PACK), 0).astype(F32) + 1.0
        return jnp.where(ids == msg_ref[place, 8:9, 0:PACK], 1.0, 0.0).astype(BF16)

    def remote(src, dst, send_sem, recv_sem, mask, own):
        if mask == 0:
            pltpu.make_async_copy(src, dst, own_sem.at[own]).start()
        else:
            pltpu.make_async_remote_copy(
                src_ref=src, dst_ref=dst, send_sem=send_sem, recv_sem=recv_sem,
                device_id=(partner(me, mask),), device_id_type=MESH).start()

    @pl.when(e == 0)
    def _():
        greet(me)

    z_s[e] = mlp(fix_ref[0])

    @pl.when(e == 0)
    def _():
        pl.semaphore_wait(pltpu.get_barrier_semaphore(), N_DEV - 1)

    for place, mask in enumerate(ORDER):
        remote(z_s.at[e, pl.ds(place * per_src, per_src), :], back_ref.at[me * n_exp + e], fix_send, fix_recv, mask, 0)

    @pl.when(e == 0)
    def _():
        for place in range(N_DEV):
            x = dot(spread(place), pack_ref[place]).astype(BF16)
            x_s[:, pl.ds(place * EXTRA, EXTRA), :] = x.reshape(n_exp, EXTRA, d_model)

    zx_s[e] = mlp(x_s[e])

    @pl.when(e == n_exp - 1)
    def _():
        for place, mask in enumerate(ORDER):
            z = zx_s[:, pl.ds(place * EXTRA, EXTRA), :].reshape(n_exp * EXTRA, d_model)
            pack_s[place] = lax.dot_general(
                spread(place), z, (((0,), (0,)), ((), ())), preferred_element_type=F32).astype(BF16)
            if place > 0:
                remote(pack_s.at[place - 1], back_pack_ref.at[me], pack_send, pack_recv, ORDER[place - 1], 1)
        remote(pack_s.at[N_DEV - 1], back_pack_ref.at[me], pack_send, pack_recv, ORDER[N_DEV - 1], 1)

        def settle(ref, sem):
            pltpu.make_async_copy(ref, ref, sem).wait()

        others = pl.ds(0, N_DEV - 1)
        settle(z_s.at[:, pl.ds(0, per_src), :], own_sem.at[0])
        settle(pack_s.at[0], own_sem.at[1])
        settle(z_s.at[:, pl.ds(0, (N_DEV - 1) * per_src), :], fix_send)
        settle(pack_s.at[others], pack_send)
        settle(back_ref.at[pl.ds(0, (N_DEV - 1) * n_exp)], fix_recv)
        settle(back_pack_ref.at[others], pack_recv)


def packed_back_kernel(fix_ref, pack_ref, hidden_ref, meta_ref, msg_ref, out_ref, aux_ref, *, n_groups):
    experts, rows, d_model = fix_ref.shape
    seq = hidden_ref.shape[1]
    z = fix_ref[...].reshape(experts * rows, d_model)
    zx = pack_ref[...].reshape(N_DEV * PACK, d_model)
    fix_id = lax.broadcasted_iota(jnp.int32, (seq, experts * rows), 1)
    pack_id = lax.broadcasted_iota(jnp.int32, (seq, N_DEV * PACK), 1) + experts * rows
    for grp in range(2):
        meta = meta_ref[grp].T
        c1 = meta[:, 0:1].astype(jnp.int32)
        c2 = meta[:, 1:2].astype(jnp.int32)
        g1 = meta[:, 2:3]
        g2 = meta[:, 3:4]

        def gates(ids):
            return jnp.where(ids == c1, g1, jnp.where(ids == c2, g2, 0.0)).astype(BF16)

        moe = dot(gates(fix_id), z) + dot(gates(pack_id), zx)
        out_ref[grp] = (hidden_ref[grp].astype(F32) + moe).astype(BF16)

    @pl.when(pl.program_id(0) == 0)
    def _():
        total = jnp.sum(msg_ref[:, 0:8, :], axis=0)
        total = jnp.sum(jnp.sum(total, axis=1, keepdims=True), axis=0, keepdims=True)
        aux_ref[...] = jnp.broadcast_to(total * (experts / n_groups), aux_ref.shape)


def solution(mesh):
    def local_step(tokens, pad_mask, second_draw, choices, norm_attn, w_query, w_key, w_value, w_attn_out, norm_moe, w_gate, w_in, w_out):
        groups, seq, d_model = tokens.shape
        _, heads, head_dim = w_query.shape
        experts = w_gate.shape[1]
        ff = w_in.shape[2]
        e_loc = experts // N_DEV
        capacity = (2 * seq + experts - 1) // experts
        hw = heads * head_dim
        rows = 2 * capacity
        steps = groups // 2
        all_rows = N_DEV * steps * rows

        wq, wk, wv = (w.transpose(1, 2, 0).reshape(hw, d_model) for w in (w_query, w_key, w_value))
        wo = w_attn_out.reshape(hw, d_model)

        def whole(shape):
            return pl.BlockSpec(shape, lambda i: (0,) * len(shape), pipeline_mode=pl.Buffered(1))

        anywhere = pl.BlockSpec(memory_space=pl.ANY)
        def full_path():
            hidden, meta, recv, auxr = pl.pallas_call(
                functools.partial(front_kernel, heads=heads, head_dim=head_dim, capacity=capacity),
                name="front",
                grid=(steps,),
                in_specs=[
                    pl.BlockSpec((2, seq, d_model), lambda i: (i, 0, 0)),
                    whole((groups, seq)), whole((groups, seq)),
                    pl.BlockSpec((2, 2, seq), lambda i: (i, 0, 0)),
                    whole((d_model,)), whole((hw, d_model)), whole((hw, d_model)), whole((hw, d_model)), whole((hw, d_model)),
                    whole((d_model,)), whole((d_model, experts)),
                ],
                out_specs=[
                    pl.BlockSpec((2, seq, d_model), lambda i: (i, 0, 0)),
                    pl.BlockSpec((2, 8, seq), lambda i: (i, 0, 0)),
                    anywhere, anywhere,
                ],
                out_shape=[
                    jax.ShapeDtypeStruct((groups, seq, d_model), BF16),
                    jax.ShapeDtypeStruct((groups, 8, seq), F32),
                    jax.ShapeDtypeStruct((e_loc, all_rows, d_model), BF16),
                    jax.ShapeDtypeStruct((N_DEV, 8, 128), F32),
                ],
                scratch_shapes=[
                    pltpu.VMEM((hw, 2 * seq), BF16),
                    pltpu.VMEM((2 * seq, hw), BF16),
                    pltpu.VMEM((hw, 2 * seq), BF16),
                    pltpu.VMEM((hw, 2 * seq), BF16),
                    pltpu.VMEM((2, 4, seq, seq), F32),
                    pltpu.VMEM((2, 4, seq, seq), BF16),
                    pltpu.VMEM((3 * experts, d_model), BF16),
                    pltpu.VMEM((8, 128), F32),
                    pltpu.VMEM((steps, N_DEV, e_loc, rows, d_model), BF16),
                    pltpu.SemaphoreType.DMA,
                    pltpu.SemaphoreType.DMA,
                    pltpu.SemaphoreType.DMA((2,)),
                    pltpu.SemaphoreType.DMA,
                    pltpu.SemaphoreType.DMA,
                ],
                compiler_params=pltpu.CompilerParams(
                    dimension_semantics=("arbitrary",), collective_id=2, has_side_effects=True, vmem_limit_bytes=VMEM_LIMIT),
            )(tokens, pad_mask, second_draw, choices.transpose(0, 2, 1), norm_attn, wq, wk, wv, wo, norm_moe, w_gate)

            tile = all_rows // 2
            ret = pl.pallas_call(
                functools.partial(expert_kernel, tile=tile),
                name="experts",
                grid=(e_loc,),
                in_specs=[
                    pl.BlockSpec((1, all_rows, d_model), lambda i: (i, 0, 0)),
                    pl.BlockSpec((1, d_model, ff), lambda i: (i, 0, 0)),
                    pl.BlockSpec((1, ff, d_model), lambda i: (i, 0, 0)),
                ],
                out_specs=anywhere,
                out_shape=jax.ShapeDtypeStruct((experts, steps * rows, d_model), BF16),
                scratch_shapes=[
                    pltpu.VMEM((tile, ff), BF16),
                    pltpu.VMEM((e_loc, all_rows, d_model), BF16),
                    pltpu.SemaphoreType.DMA,
                    pltpu.SemaphoreType.DMA,
                    pltpu.SemaphoreType.DMA,
                ],
                compiler_params=pltpu.CompilerParams(
                    dimension_semantics=("arbitrary",), collective_id=3, has_side_effects=True, vmem_limit_bytes=VMEM_LIMIT),
            )(recv, w_in, w_out)

            out, aux = pl.pallas_call(
                functools.partial(back_kernel, n_groups=groups * N_DEV),
                name="back",
                grid=(steps,),
                in_specs=[
                    pl.BlockSpec((experts, rows, d_model), lambda i: (0, i, 0)),
                    pl.BlockSpec((2, seq, d_model), lambda i: (i, 0, 0)),
                    pl.BlockSpec((2, 8, seq), lambda i: (i, 0, 0)),
                    pl.BlockSpec((N_DEV, 8, 128), lambda i: (0, 0, 0)),
                ],
                out_specs=[
                    pl.BlockSpec((2, seq, d_model), lambda i: (i, 0, 0)),
                    pl.BlockSpec((8, 128), lambda i: (0, 0)),
                ],
                out_shape=[
                    jax.ShapeDtypeStruct((groups, seq, d_model), BF16),
                    jax.ShapeDtypeStruct((8, 128), F32),
                ],
                compiler_params=pltpu.CompilerParams(dimension_semantics=("arbitrary",), vmem_limit_bytes=VMEM_LIMIT),
            )(ret, hidden, meta, auxr)
            return out, aux

        front_specs = [
            pl.BlockSpec((2, seq, d_model), lambda i: (i, 0, 0)),
            whole((groups, seq)), whole((groups, seq)),
            pl.BlockSpec((2, 2, seq), lambda i: (i, 0, 0)),
            whole((d_model,)), whole((hw, d_model)), whole((hw, d_model)), whole((hw, d_model)), whole((hw, d_model)),
            whole((d_model,)), whole((d_model, experts)),
        ]
        quads = steps // 2
        fix_rows = quads * FIX
        dma = pltpu.SemaphoreType.DMA
        hidden_p, meta_p, fix, pack, msg = pl.pallas_call(
            functools.partial(packed_front_kernel, heads=heads, head_dim=head_dim, capacity=capacity),
            name="packed_front",
            grid=(steps,),
            in_specs=front_specs,
            out_specs=[
                pl.BlockSpec((2, seq, d_model), lambda i: (i, 0, 0)),
                pl.BlockSpec((2, 8, seq), lambda i: (i, 0, 0)),
                anywhere, anywhere, anywhere,
            ],
            out_shape=[
                jax.ShapeDtypeStruct((groups, seq, d_model), BF16),
                jax.ShapeDtypeStruct((groups, 8, seq), F32),
                jax.ShapeDtypeStruct((e_loc, N_DEV * fix_rows, d_model), BF16),
                jax.ShapeDtypeStruct((N_DEV, PACK, d_model), BF16),
                jax.ShapeDtypeStruct((N_DEV, 16, 128), F32),
            ],
            scratch_shapes=[
                pltpu.VMEM((hw, 2 * seq), BF16),
                pltpu.VMEM((2 * seq, hw), BF16),
                pltpu.VMEM((hw, 2 * seq), BF16),
                pltpu.VMEM((hw, 2 * seq), BF16),
                pltpu.VMEM((2, 4, seq, seq), F32),
                pltpu.VMEM((2, 4, seq, seq), BF16),
                pltpu.VMEM((3 * experts, d_model), BF16),
                pltpu.VMEM((4 * seq, d_model), BF16),
                pltpu.VMEM((8, 4 * seq), jnp.int32),
                pltpu.VMEM((4, experts, 128), F32),
                pltpu.VMEM((8, 128), F32),
                pltpu.VMEM((N_DEV, 128), F32),
                pltpu.VMEM((N_DEV, 128), F32),
                pltpu.VMEM((N_DEV, 256), F32),
                pltpu.VMEM((N_DEV, quads * LOCAL, d_model), BF16),
                pltpu.VMEM((quads, N_DEV, e_loc, FIX, d_model), BF16),
                pltpu.VMEM((N_DEV, PACK, d_model), BF16),
                pltpu.VMEM((N_DEV, 16, 128), F32),
                dma, dma, dma, dma, dma, dma, dma((3,)),
            ],
            compiler_params=pltpu.CompilerParams(
                dimension_semantics=("arbitrary",), collective_id=0, has_side_effects=True, vmem_limit_bytes=VMEM_LIMIT),
        )(tokens, pad_mask, second_draw, choices.transpose(0, 2, 1), norm_attn, wq, wk, wv, wo, norm_moe, w_gate)

        def packed_path():
            back, back_pack = pl.pallas_call(
                packed_expert_kernel,
                name="packed_experts",
                grid=(e_loc,),
                in_specs=[
                    pl.BlockSpec((1, N_DEV * fix_rows, d_model), lambda i: (i, 0, 0)),
                    whole((N_DEV, PACK, d_model)), whole((N_DEV, 16, 128)),
                    pl.BlockSpec((1, d_model, ff), lambda i: (i, 0, 0)),
                    pl.BlockSpec((1, ff, d_model), lambda i: (i, 0, 0)),
                ],
                out_specs=[anywhere, anywhere],
                out_shape=[
                    jax.ShapeDtypeStruct((experts, fix_rows, d_model), BF16),
                    jax.ShapeDtypeStruct((N_DEV, PACK, d_model), BF16),
                ],
                scratch_shapes=[
                    pltpu.VMEM((N_DEV * fix_rows, ff), BF16),
                    pltpu.VMEM((e_loc, N_DEV * EXTRA, d_model), BF16),
                    pltpu.VMEM((e_loc, N_DEV * fix_rows, d_model), BF16),
                    pltpu.VMEM((e_loc, N_DEV * EXTRA, d_model), BF16),
                    pltpu.VMEM((N_DEV, PACK, d_model), BF16),
                    dma, dma, dma, dma, dma((2,)),
                ],
                compiler_params=pltpu.CompilerParams(
                    dimension_semantics=("arbitrary",), collective_id=1, has_side_effects=True, vmem_limit_bytes=VMEM_LIMIT),
            )(fix, pack, msg, w_in, w_out)
            return pl.pallas_call(
                functools.partial(packed_back_kernel, n_groups=groups * N_DEV),
                name="packed_back",
                grid=(steps,),
                in_specs=[
                    pl.BlockSpec((experts, FIX, d_model), lambda i: (0, i // 2, 0)),
                    whole((N_DEV, PACK, d_model)),
                    pl.BlockSpec((2, seq, d_model), lambda i: (i, 0, 0)),
                    pl.BlockSpec((2, 8, seq), lambda i: (i, 0, 0)),
                    whole((N_DEV, 16, 128)),
                ],
                out_specs=[
                    pl.BlockSpec((2, seq, d_model), lambda i: (i, 0, 0)),
                    pl.BlockSpec((8, 128), lambda i: (0, 0)),
                ],
                out_shape=[
                    jax.ShapeDtypeStruct((groups, seq, d_model), BF16),
                    jax.ShapeDtypeStruct((8, 128), F32),
                ],
                compiler_params=pltpu.CompilerParams(dimension_semantics=("arbitrary",), vmem_limit_bytes=VMEM_LIMIT),
            )(back, back_pack, hidden_p, meta_p, msg)

        spilled = jnp.max(msg[:, 9, 0]) > 0.0
        out, aux = lax.cond(spilled, full_path, packed_path)
        return out, aux[0, 0]

    by_group = P("ep")
    replicated = P()
    in_specs = (by_group, by_group, by_group, by_group, replicated, replicated, replicated, replicated, replicated, replicated, replicated, by_group, by_group)
    return jax.shard_map(local_step, mesh=mesh, in_specs=in_specs, out_specs=(by_group, replicated), check_vma=False)
```

```python
import functools
import jax
import jax.numpy as jnp
from jax import lax
from jax.experimental import pallas as pl
from jax.experimental.pallas import tpu as pltpu
from jax.sharding import PartitionSpec as P

NORM_EPS = 1e-6
N_DEV = 16
MESH = pl.DeviceIdType.MESH
F32 = jnp.float32
BF16 = jnp.bfloat16
ORDER = (0, 9, 2, 11, 4, 13, 6, 15, 8, 1, 10, 3, 12, 5, 14, 7)
VMEM_LIMIT = 62 * 1024 * 1024


def partner(me, mask):
    out = 0
    for bit in range(4):
        val = lax.rem(me // (1 << bit), 2)
        out = out + (1 << bit) * ((1 - val) if (mask >> bit) & 1 else val)
    return out


def greet(me):
    barrier = pltpu.get_barrier_semaphore()
    for mask in range(1, N_DEV):
        pl.semaphore_signal(barrier, inc=1, device_id=(partner(me, mask),), device_id_type=MESH)


def rms_norm(values_f, scale_vec):
    inv_rms = lax.rsqrt(jnp.mean(values_f * values_f, axis=-1, keepdims=True) + NORM_EPS)
    return (values_f * inv_rms * scale_vec).astype(BF16)


def dot(a, b):
    return jnp.dot(a, b, preferred_element_type=F32)


def dot_nt(a, b):
    return lax.dot_general(a, b, (((1,), (1,)), ((), ())), preferred_element_type=F32)


def split_gate(wgate_ref, wg_s):
    experts = wgate_ref.shape[1]
    wg = wgate_ref[...].T
    hi = wg.astype(BF16)
    rest = wg - hi.astype(F32)
    mid = rest.astype(BF16)
    low = (rest - mid.astype(F32)).astype(BF16)
    wg_s[0:experts] = hi
    wg_s[experts:2 * experts] = mid
    wg_s[2 * experts:3 * experts] = low


def attend(
    step, tokens_ref, pad_ref, norm_attn_ref, wq_ref, wk_ref, wv_ref, wo_ref, norm_moe_ref, hidden_ref,
    q_s, k_s, v_s, ctx_s, s_s, p_s, wg_s, heads, head_dim, experts,
):
    seq = tokens_ref.shape[1]
    d_model = tokens_ref.shape[2]
    x = tokens_ref[...].reshape(2 * seq, d_model)
    a = rms_norm(x.astype(F32), norm_attn_ref[...][None, :])
    q_s[...] = dot_nt(wq_ref[...], a).astype(BF16)
    k_s[...] = dot_nt(a, wk_ref[...]).astype(BF16)
    v_s[...] = dot_nt(wv_ref[...], a).astype(BF16)

    width = 2 * head_dim
    lane = lax.broadcasted_iota(jnp.int32, (1, width), 1)
    scale = head_dim ** -0.5
    sides = [jnp.where(lane < head_dim, scale, 0.0).astype(BF16), jnp.where(lane < head_dim, 0.0, scale).astype(BF16)]
    cut = seq // 2
    late_key = lax.broadcasted_iota(jnp.int32, (seq - cut, 128), 0) + cut
    batch = s_s.shape[1]
    lanes = 128
    buf = 0
    for grp in range(2):
        tok = pl.ds(grp * seq, seq)
        length = jnp.sum(pad_ref[pl.ds(2 * step + grp, 1), :], axis=1, keepdims=True)
        keep_late = late_key < length
        for first in range(0, heads, batch):
            for i in range(batch):
                off = (first + i) // 2 * width
                k = k_s[tok, pl.ds(off, width)] * sides[(first + i) % 2]
                s_s[buf, i] = dot(k, q_s[pl.ds(off, width), tok])
            for i in range(batch):
                for col in range(0, seq, lanes):
                    cols = pl.ds(col, lanes)
                    early = s_s[buf, i, pl.ds(0, cut), cols]
                    late = jnp.where(keep_late, s_s[buf, i, pl.ds(cut, seq - cut), cols], -1e30)
                    top = jnp.maximum(jnp.max(early, axis=0, keepdims=True), jnp.max(late, axis=0, keepdims=True))
                    early = jnp.exp(early - top)
                    late = jnp.exp(late - top)
                    inv = 1.0 / (jnp.sum(early, axis=0, keepdims=True) + jnp.sum(late, axis=0, keepdims=True))
                    p_s[buf, i, pl.ds(0, cut), cols] = (early * inv).astype(BF16)
                    p_s[buf, i, pl.ds(cut, seq - cut), cols] = (late * inv).astype(BF16)
            for i in range(batch):
                head = pl.ds((first + i) * head_dim, head_dim)
                ctx_s[head, tok] = dot(v_s[head, tok], p_s[buf, i]).astype(BF16)
            buf = 1 - buf

    attn = lax.dot_general(ctx_s[...], wo_ref[...], (((0,), (0,)), ((), ())), preferred_element_type=F32)
    hidden = (x.astype(F32) + attn).astype(BF16)
    hidden_ref[...] = hidden.reshape(2, seq, d_model)
    b = rms_norm(hidden.astype(F32), norm_moe_ref[...][None, :])
    lg = dot_nt(wg_s[...], b)
    logits = (lg[2 * experts:] + lg[experts:2 * experts]) + lg[:experts]
    ex = jnp.exp(logits - jnp.max(logits, axis=0, keepdims=True))
    return b, ex / jnp.sum(ex, axis=0, keepdims=True)


def full_front_kernel(hidden_ref, meta_ref, norm_moe_ref, recv_ref, send_s, send_sem, recv_sem, own_sem, *, experts, capacity):
    step = pl.program_id(0)
    steps = pl.num_programs(0)
    me = lax.axis_index("ep")
    seq = hidden_ref.shape[1]
    d_model = hidden_ref.shape[2]
    e_loc = experts // N_DEV
    half = e_loc // 2
    slots = experts * capacity
    rows = 2 * capacity
    per_src = steps * rows

    def send_pair(pair):
        for place, mask in enumerate(ORDER):
            dev = partner(me, mask)
            src = send_s.at[pair, dev]
            dst = recv_ref.at[:, pl.ds(pl.multiple_of(place * per_src + pair * rows, rows), rows), :]
            if mask == 0:
                pltpu.make_async_copy(src, dst, own_sem).start()
            else:
                pltpu.make_async_remote_copy(
                    src_ref=src, dst_ref=dst, send_sem=send_sem, recv_sem=recv_sem,
                    device_id=(dev,), device_id_type=MESH).start()

    @pl.when(step == 0)
    def _():
        greet(me)

    @pl.when(step == 1)
    def _():
        pl.semaphore_wait(pltpu.get_barrier_semaphore(), N_DEV - 1)

    @pl.when(step > 0)
    def _():
        send_pair(step - 1)

    slot_id = lax.broadcasted_iota(jnp.int32, (slots, seq), 0)
    picked = []
    for grp in range(2):
        b = rms_norm(hidden_ref[grp].astype(F32), norm_moe_ref[...][None, :])

        def place_of(code):
            e = code // capacity
            dev = e // e_loc
            r = e - dev * e_loc
            upper = r // half
            side = upper if grp == 0 else 1 - upper
            at = ((dev * half + r - upper * half) * 2 + side) * capacity + code - e * capacity
            return jnp.where(code >= 0, at, -1)

        d1 = place_of(meta_ref[grp, 4:5, :].astype(jnp.int32))
        d2 = place_of(meta_ref[grp, 5:6, :].astype(jnp.int32))
        disp_mat = jnp.where((slot_id == d1) | (slot_id == d2), 1.0, 0.0).astype(BF16)
        picked.append(dot(disp_mat, b).reshape(N_DEV * half, rows, d_model))

    top = lax.broadcasted_iota(jnp.int32, (1, rows, 1), 1) < capacity
    lower = jnp.where(top, picked[0], picked[1]).astype(BF16)
    upper = jnp.where(top, picked[1], picked[0]).astype(BF16)
    send_s[step, :, 0:half] = lower.reshape(N_DEV, half, rows, d_model)
    send_s[step, :, half:e_loc] = upper.reshape(N_DEV, half, rows, d_model)

    @pl.when(step == steps - 1)
    def _():
        send_pair(steps - 1)
        others = pl.ds(0, N_DEV - 1)
        pltpu.make_async_copy(send_s.at[:, others], send_s.at[:, others], send_sem).wait()
        pltpu.make_async_copy(send_s.at[:, 0], send_s.at[:, 0], own_sem).wait()
        arrived = recv_ref.at[:, pl.ds(0, (N_DEV - 1) * per_src), :]
        pltpu.make_async_copy(arrived, arrived, recv_sem).wait()


def expert_kernel(recv_ref, w_in_ref, w_out_ref, ret_ref, act_s, z_s, send_sem, recv_sem, local_sem, *, tile):
    e = pl.program_id(0)
    n_exp = pl.num_programs(0)
    me = lax.axis_index("ep")
    rows = recv_ref.shape[1]
    ff = w_in_ref.shape[2]
    per_src = rows // N_DEV
    n_tiles = rows // tile
    chunk = 1024

    @pl.when(e == 0)
    def _():
        greet(me)

    def run(t, carry):
        at = pl.ds(pl.multiple_of(t * tile, tile), tile)
        x = recv_ref[0, at, :]
        for f in range(ff // chunk):
            act = dot(x, w_in_ref[0, :, pl.ds(f * chunk, chunk)])
            act_s[:, pl.ds(f * chunk, chunk)] = jnp.maximum(act, 0.0).astype(BF16)
        z_s[e, at, :] = dot(act_s[...], w_out_ref[0]).astype(BF16)
        return carry

    lax.fori_loop(0, n_tiles, run, 0)

    @pl.when(e == 0)
    def _():
        pl.semaphore_wait(pltpu.get_barrier_semaphore(), N_DEV - 1)

    for place, mask in enumerate(ORDER):
        dev = partner(me, mask)
        src = z_s.at[e, pl.ds(place * per_src, per_src), :]
        dst = ret_ref.at[me * n_exp + e]
        if mask == 0:
            pltpu.make_async_copy(src, dst, local_sem).start()
        else:
            pltpu.make_async_remote_copy(
                src_ref=src, dst_ref=dst, send_sem=send_sem, recv_sem=recv_sem,
                device_id=(dev,), device_id_type=MESH).start()

    @pl.when(e == n_exp - 1)
    def _():
        sent = z_s.at[:, pl.ds(0, (N_DEV - 1) * per_src), :]
        pltpu.make_async_copy(sent, sent, send_sem).wait()
        own = z_s.at[:, pl.ds(0, per_src), :]
        pltpu.make_async_copy(own, own, local_sem).wait()
        arrived = ret_ref.at[pl.ds(0, (N_DEV - 1) * n_exp)]
        pltpu.make_async_copy(arrived, arrived, recv_sem).wait()


def back_kernel(ret_ref, hidden_ref, meta_ref, msg_ref, out_ref, aux_ref, *, n_groups, capacity):
    experts, rows, d_model = ret_ref.shape
    seq = hidden_ref.shape[1]
    z = ret_ref[...].reshape(experts * rows, d_model)
    slot_id = lax.broadcasted_iota(jnp.int32, (seq, experts * rows), 1)
    e_loc = experts // N_DEV
    for grp in range(2):
        meta = meta_ref[grp].T

        def place_of(code):
            e = code // capacity
            r = e - e // e_loc * e_loc
            upper = r // (e_loc // 2)
            side = upper if grp == 0 else 1 - upper
            return jnp.where(code >= 0, (e * 2 + side) * capacity + code - e * capacity, -1)

        c1 = place_of(meta[:, 4:5].astype(jnp.int32))
        c2 = place_of(meta[:, 5:6].astype(jnp.int32))
        comb = jnp.where(slot_id == c1, meta[:, 2:3], 0.0) + jnp.where(slot_id == c2, meta[:, 3:4], 0.0)
        moe = dot(comb.astype(BF16), z)
        out_ref[grp] = (hidden_ref[grp].astype(F32) + moe).astype(BF16)

    @pl.when(pl.program_id(0) == 0)
    def _():
        total = jnp.sum(msg_ref[:, 0:8, :], axis=0)
        total = jnp.sum(jnp.sum(total, axis=1, keepdims=True), axis=0, keepdims=True)
        aux_ref[...] = jnp.broadcast_to(total * (experts / n_groups), aux_ref.shape)


FIX = 8
LOCAL = 48
PACK = 112
EXTRA = 32
TEAM = 4
POOL = 80


def twice(value):
    return jnp.concatenate([value, value], axis=1)


def packed_front_kernel(
    tokens_ref, pad_ref, draw_ref, choices_ref, norm_attn_ref, wq_ref, wk_ref, wv_ref, wo_ref, norm_moe_ref, wgate_ref,
    hidden_ref, meta_ref, fix_ref, pack_ref, msg_ref,
    q_s, k_s, v_s, ctx_s, s_s, p_s, wg_s, b_s, slot_s, count_s, aux_s, flag_s, code_s, goal_s,
    local_s, fix_s, pack_s, msg_s, fix_send, fix_recv, pack_send, pack_recv, msg_send, msg_recv, own_sem,
    *, heads, head_dim, capacity,
):
    step = pl.program_id(0)
    steps = pl.num_programs(0)
    quad = step // 2
    quads = steps // 2
    me = lax.axis_index("ep")
    seq = tokens_ref.shape[1]
    d_model = tokens_ref.shape[2]
    experts = wgate_ref.shape[1]
    e_loc = experts // N_DEV

    def remote(src, dst, send_sem, recv_sem, dev, mask, own):
        if mask == 0:
            pltpu.make_async_copy(src, dst, own_sem.at[own]).start()
        else:
            pltpu.make_async_remote_copy(
                src_ref=src, dst_ref=dst, send_sem=send_sem, recv_sem=recv_sem,
                device_id=(dev,), device_id_type=MESH).start()

    def send_quad(which):
        for place, mask in enumerate(ORDER):
            dev = partner(me, mask)
            row = pl.multiple_of(place * quads * FIX + which * FIX, FIX)
            remote(fix_s.at[which, dev], fix_ref.at[:, pl.ds(row, FIX), :], fix_send, fix_recv, dev, mask, 0)

    @pl.when(step == 0)
    def _():
        greet(me)
        split_gate(wgate_ref, wg_s)
        aux_s[...] = jnp.zeros_like(aux_s)
        flag_s[...] = jnp.zeros_like(flag_s)
        code_s[...] = jnp.zeros_like(code_s)
        goal_s[...] = jnp.zeros_like(goal_s)
        count_s[...] = jnp.zeros_like(count_s)

    @pl.when(step == 2)
    def _():
        pl.semaphore_wait(pltpu.get_barrier_semaphore(), N_DEV - 1)

    @pl.when((step > 0) & (lax.rem(step, 2) == 0))
    def _():
        send_quad(quad - 1)

    b, gate_probs = attend(
        step, tokens_ref, pad_ref, norm_attn_ref, wq_ref, wk_ref, wv_ref, wo_ref, norm_moe_ref, hidden_ref,
        q_s, k_s, v_s, ctx_s, s_s, p_s, wg_s, heads, head_dim, experts)
    side = lax.rem(step, 2)
    b_s[pl.ds(pl.multiple_of(side * 2 * seq, 2 * seq), 2 * seq), :] = b

    eid = lax.broadcasted_iota(jnp.int32, (experts, seq), 0)
    tri = jnp.where(lax.broadcasted_iota(jnp.int32, (seq, seq), 0) <= lax.broadcasted_iota(jnp.int32, (seq, seq), 1), 1.0, 0.0)
    tri = jnp.concatenate([tri, jnp.ones((seq, 128), F32)], axis=1).astype(BF16)
    row_e = lax.broadcasted_iota(jnp.int32, (experts, experts), 0)
    col_e = lax.broadcasted_iota(jnp.int32, (experts, experts), 1)
    same = row_e // e_loc == col_e // e_loc
    mix = jnp.concatenate([jnp.where(same & (col_e < row_e), 1.0, 0.0), jnp.where(same, 1.0, 0.0)], axis=0).astype(BF16)
    spot = lax.broadcasted_iota(jnp.int32, (experts, 128), 1).astype(F32)
    code0 = (lax.rem(lax.broadcasted_iota(jnp.int32, (experts, 128), 0), e_loc) * EXTRA + 1).astype(F32)
    meta_row = lax.broadcasted_iota(jnp.int32, (8, seq), 0)
    for grp in range(2):
        p = gate_probs[:, grp * seq:(grp + 1) * seq]
        valid = pad_ref[pl.ds(2 * step + grp, 1), :] == 1
        draw = draw_ref[pl.ds(2 * step + grp, 1), :]
        e1 = choices_ref[grp, 0:1, :]
        e2 = choices_ref[grp, 1:2, :]
        hot1 = eid == e1
        hot2 = eid == e2
        p1 = jnp.sum(jnp.where(hot1, p, 0.0), axis=0, keepdims=True)
        p2 = jnp.sum(jnp.where(hot2, p, 0.0), axis=0, keepdims=True)
        g1 = p1 / (p1 + p2)
        g2 = p2 / (p1 + p2)
        want2 = valid & (draw < 2.0 * g2)
        take1 = jnp.where(hot1 & valid, 1.0, 0.0)
        take2 = jnp.where(hot2 & want2, 1.0, 0.0)
        cum = dot(jnp.concatenate([take1, take2], axis=0).astype(BF16), tri)
        cum1 = cum[:experts, :seq]
        cum2 = cum[experts:, :seq]
        count1 = cum[:experts, seq:]
        count2 = cum[experts:, seq:]
        first = jnp.minimum(count1, float(capacity))
        pos1 = jnp.sum((cum1 - 1.0) * take1, axis=0, keepdims=True)
        pos2 = jnp.sum((cum2 - 1.0 + twice(first)) * take2, axis=0, keepdims=True)
        keep1 = valid & (pos1 < capacity)
        keep2 = want2 & (pos2 < capacity)

        share = jnp.where(valid, p, 0.0) * twice(count1 * (1.0 / (seq * seq)))
        share = jnp.sum(share.reshape(experts // 8, 8, seq), axis=0)
        for col in range(seq // 128):
            aux_s[...] += share[:, col * 128:(col + 1) * 128]

        before = count_s[0]
        after = before + jnp.minimum(first + count2, float(capacity))
        new = jnp.maximum(after - FIX, 0.0) - jnp.maximum(before - FIX, 0.0)
        sums = dot(mix, new.astype(BF16))
        packed = count_s[1]
        begin = packed + sums[:experts]
        shift = begin - jnp.maximum(before, float(FIX)) + before
        local = shift - count_s[3]
        inside = (spot >= begin) & (spot < begin + new)
        code = jnp.where(inside, code0 + count_s[2] + spot - begin, 0.0)
        code_s[...] += jnp.sum(code.reshape(N_DEV, e_loc, 128), axis=1)
        count_s[0] = after
        count_s[1] = packed + sums[experts:]
        count_s[2] += new

        def places(e, take, pos, keep):
            index = pos + jnp.sum(twice(before) * take, axis=0, keepdims=True)
            in_pack = pos + jnp.sum(twice(shift) * take, axis=0, keepdims=True)
            in_local = pos + jnp.sum(twice(local) * take, axis=0, keepdims=True)
            e = e.astype(F32)
            dev = jnp.floor(e * (1.0 / e_loc))
            fixed = keep & (index < FIX)
            loose = keep & (index >= FIX)
            at_fix = jnp.where(fixed, e * FIX + index, -1.0)
            at_local = jnp.where(loose, dev * LOCAL + in_local, -1.0)
            at_back = jnp.where(loose, experts * FIX + dev * PACK + in_pack, at_fix)
            return at_fix, at_local, at_back, jnp.where(keep, e * capacity + pos, -1.0)

        f1, l1, c1, w1 = places(e1, take1, pos1, keep1)
        f2, l2, c2, w2 = places(e2, take2, pos2, keep2)
        meta = jnp.where(meta_row == 0, c1, 0.0)
        meta = jnp.where(meta_row == 1, c2, meta)
        meta = jnp.where(meta_row == 2, g1, meta)
        meta = jnp.where(meta_row == 3, g2, meta)
        meta = jnp.where(meta_row == 4, w1, meta)
        meta = jnp.where(meta_row == 5, w2, meta)
        meta_ref[grp] = meta
        tok = pl.ds(pl.multiple_of(side * 2 * seq + grp * seq, seq), seq)
        slot_s[:, tok] = jnp.where(meta_row == 0, f1, jnp.where(meta_row == 1, f2, jnp.where(meta_row == 2, l1, l2))).astype(jnp.int32)

    @pl.when(side == 1)
    def _():
        def gather(first_row, base, count, skip):
            ids = lax.broadcasted_iota(jnp.int32, (count, 4 * seq - skip), 0) + base
            hit = (ids == slot_s[first_row:first_row + 1, skip:]) | (ids == slot_s[first_row + 1:first_row + 2, skip:])
            return dot(jnp.where(hit, 1.0, 0.0).astype(BF16), b_s[skip:, :]).astype(BF16)

        per_dev = e_loc * FIX
        for base in range(0, N_DEV, 4):
            rows = gather(0, base * per_dev, 4 * per_dev, 0)
            fix_s[quad, base:base + 4] = rows.reshape(4, e_loc, FIX, d_model)
        for base in range(0, N_DEV, 4):
            rows = gather(2, base * LOCAL, 4 * LOCAL, 2 * seq)
            local_s[base:base + 4, pl.ds(pl.multiple_of(quad * LOCAL, LOCAL), LOCAL), :] = rows.reshape(4, LOCAL, d_model)

        def per_device(value):
            return value.reshape(N_DEV, e_loc, 128)[:, 0, :]

        start = per_device(count_s[3])
        filled = per_device(count_s[1]) - start
        at = lax.broadcasted_iota(jnp.int32, (N_DEV, 256), 1).astype(F32) - (quad * LOCAL).astype(F32)
        live = (at >= 0.0) & (at < float(LOCAL)) & (at < twice(filled))
        goal_s[...] = jnp.where(live, twice(start) + at + 1.0, goal_s[...])
        flag_s[...] = jnp.maximum(flag_s[...], jnp.where(filled > LOCAL, 1.0, 0.0))
        count_s[0] = jnp.zeros_like(count_s[0])
        count_s[3] = count_s[1]

    @pl.when(step == steps - 1)
    def _():
        send_quad(quads - 1)
        width = goal_s.shape[1] * 3 // 4
        rows = lax.broadcasted_iota(jnp.int32, (PACK, width), 0).astype(F32) + 1.0
        for dev in range(N_DEV):
            hit = jnp.where(rows == goal_s[dev:dev + 1, 0:width], 1.0, 0.0).astype(BF16)
            pack_s[dev] = dot(hit, local_s[dev]).astype(BF16)
        over = jnp.where((count_s[1] > PACK) | (count_s[2] > EXTRA), 1.0, 0.0)
        over = jnp.max(jnp.max(over.reshape(N_DEV, e_loc, 128), axis=1), axis=0, keepdims=True)
        over = jnp.maximum(over, jnp.max(flag_s[...], axis=0, keepdims=True))
        tally = count_s[2].T[0:1, :]
        for dev in range(N_DEV):
            msg_s[dev, 0:8] = aux_s[...]
            lower = lax.broadcasted_iota(jnp.int32, (8, 128), 0)
            msg_s[dev, 8:16] = jnp.where(lower == 0, code_s[dev:dev + 1, :], jnp.where(lower == 1, over, jnp.where(lower == 2, tally, 0.0)))
        for place, mask in enumerate(ORDER):
            dev = partner(me, mask)
            remote(pack_s.at[dev], pack_ref.at[place], pack_send, pack_recv, dev, mask, 1)
        for place, mask in enumerate(ORDER):
            dev = partner(me, mask)
            remote(msg_s.at[dev], msg_ref.at[place], msg_send, msg_recv, dev, mask, 2)

        def settle(ref, sem):
            pltpu.make_async_copy(ref, ref, sem).wait()

        others = pl.ds(0, N_DEV - 1)
        settle(fix_s.at[:, 0], own_sem.at[0])
        settle(pack_s.at[0], own_sem.at[1])
        settle(msg_s.at[0], own_sem.at[2])
        settle(fix_s.at[:, others], fix_send)
        settle(pack_s.at[others], pack_send)
        settle(msg_s.at[others], msg_send)
        settle(fix_ref.at[:, pl.ds(0, (N_DEV - 1) * quads * FIX), :], fix_recv)
        settle(pack_ref.at[others], pack_recv)
        settle(msg_ref.at[others], msg_recv)


def packed_expert_kernel(
    fix_ref, pack_ref, msg_ref, w_in_ref, w_out_ref, back_ref, back_pack_ref,
    act_s, x_s, z_s, zx_s, code_s, pack_s, fix_send, fix_recv, pack_send, pack_recv, own_sem,
):
    e = pl.program_id(0)
    n_exp = pl.num_programs(0)
    me = lax.axis_index("ep")
    rows = fix_ref.shape[1]
    d_model = fix_ref.shape[2]
    ff = w_in_ref.shape[2]
    per_src = rows // N_DEV
    chunk = 1024

    def mlp(x):
        for f in range(ff // chunk):
            act = dot(x, w_in_ref[0, :, pl.ds(f * chunk, chunk)])
            act_s[0:x.shape[0], pl.ds(f * chunk, chunk)] = jnp.maximum(act, 0.0).astype(BF16)
        return dot(act_s[0:x.shape[0], :], w_out_ref[0]).astype(BF16)

    def spread(place):
        ids = lax.broadcasted_iota(jnp.int32, (x_s.shape[0] * POOL, PACK), 0).astype(F32) + 1.0
        return jnp.where(ids == code_s[place:place + 1, 0:PACK], 1.0, 0.0).astype(BF16)

    def remote(src, dst, send_sem, recv_sem, mask, own):
        if mask == 0:
            pltpu.make_async_copy(src, dst, own_sem.at[own]).start()
        else:
            pltpu.make_async_remote_copy(
                src_ref=src, dst_ref=dst, send_sem=send_sem, recv_sem=recv_sem,
                device_id=(partner(me, mask),), device_id_type=MESH).start()

    @pl.when(e == 0)
    def _():
        greet(me)

    z_s[e] = mlp(fix_ref[0])

    @pl.when(e == 0)
    def _():
        pl.semaphore_wait(pltpu.get_barrier_semaphore(), N_DEV - 1)

    for place, mask in enumerate(ORDER):
        remote(z_s.at[e, pl.ds(place * per_src, per_src), :], back_ref.at[me * n_exp + e], fix_send, fix_recv, mask, 0)

    @pl.when(e == 0)
    def _():
        code = jnp.concatenate([msg_ref[place, 8:9, :] for place in range(N_DEV)], axis=0)
        n_loc = x_s.shape[0]
        hits = [(code > ex * EXTRA) & (code <= (ex + 1) * EXTRA) for ex in range(n_loc)]
        row = lax.broadcasted_iota(jnp.int32, (N_DEV, N_DEV), 0)
        col = lax.broadcasted_iota(jnp.int32, (N_DEV, N_DEV), 1)
        prior = jnp.where((row // TEAM == col // TEAM) & (col < row), 1.0, 0.0).astype(BF16)
        spans = dot(prior, jnp.concatenate([jnp.where(hit, 1.0, 0.0) for hit in hits], axis=1).astype(BF16))
        shared = jnp.zeros_like(code)
        for ex, hit in enumerate(hits):
            begin = jnp.sum(spans[:, ex * 128:(ex + 1) * 128], axis=1, keepdims=True)
            shared = jnp.where(hit, code + begin + float(ex * (POOL - EXTRA)), shared)
        code_s[...] = shared
        for team in range(N_DEV // TEAM):
            x = dot(spread(team * TEAM), pack_ref[team * TEAM])
            for place in range(team * TEAM + 1, (team + 1) * TEAM):
                x = x + dot(spread(place), pack_ref[place])
            x_s[:, pl.ds(team * POOL, POOL), :] = x.astype(BF16).reshape(n_loc, POOL, d_model)

    zx_s[e] = mlp(x_s[e])

    @pl.when(e == n_exp - 1)
    def _():
        for place, mask in enumerate(ORDER):
            z = zx_s[:, pl.ds(place // TEAM * POOL, POOL), :].reshape(x_s.shape[0] * POOL, d_model)
            pack_s[place] = lax.dot_general(
                spread(place), z, (((0,), (0,)), ((), ())), preferred_element_type=F32).astype(BF16)
            if place > 0:
                remote(pack_s.at[place - 1], back_pack_ref.at[me], pack_send, pack_recv, ORDER[place - 1], 1)
        remote(pack_s.at[N_DEV - 1], back_pack_ref.at[me], pack_send, pack_recv, ORDER[N_DEV - 1], 1)

        def settle(ref, sem):
            pltpu.make_async_copy(ref, ref, sem).wait()

        others = pl.ds(0, N_DEV - 1)
        settle(z_s.at[:, pl.ds(0, per_src), :], own_sem.at[0])
        settle(pack_s.at[0], own_sem.at[1])
        settle(z_s.at[:, pl.ds(0, (N_DEV - 1) * per_src), :], fix_send)
        settle(pack_s.at[others], pack_send)
        settle(back_ref.at[pl.ds(0, (N_DEV - 1) * n_exp)], fix_recv)
        settle(back_pack_ref.at[others], pack_recv)


def packed_back_kernel(fix_ref, pack_ref, hidden_ref, meta_ref, msg_ref, out_ref, aux_ref, *, n_groups):
    experts, rows, d_model = fix_ref.shape
    seq = hidden_ref.shape[1]
    z = fix_ref[...].reshape(experts * rows, d_model)
    zx = pack_ref[...].reshape(N_DEV * PACK, d_model)
    fix_id = lax.broadcasted_iota(jnp.int32, (seq, experts * rows), 1)
    pack_id = lax.broadcasted_iota(jnp.int32, (seq, N_DEV * PACK), 1) + experts * rows
    for grp in range(2):
        meta = meta_ref[grp].T
        c1 = meta[:, 0:1].astype(jnp.int32)
        c2 = meta[:, 1:2].astype(jnp.int32)
        g1 = meta[:, 2:3]
        g2 = meta[:, 3:4]

        def gates(ids):
            return jnp.where(ids == c1, g1, jnp.where(ids == c2, g2, 0.0)).astype(BF16)

        moe = dot(gates(fix_id), z) + dot(gates(pack_id), zx)
        out_ref[grp] = (hidden_ref[grp].astype(F32) + moe).astype(BF16)

    @pl.when(pl.program_id(0) == 0)
    def _():
        total = jnp.sum(msg_ref[:, 0:8, :], axis=0)
        total = jnp.sum(jnp.sum(total, axis=1, keepdims=True), axis=0, keepdims=True)
        aux_ref[...] = jnp.broadcast_to(total * (experts / n_groups), aux_ref.shape)


def solution(mesh):
    def local_step(tokens, pad_mask, second_draw, choices, norm_attn, w_query, w_key, w_value, w_attn_out, norm_moe, w_gate, w_in, w_out):
        groups, seq, d_model = tokens.shape
        _, heads, head_dim = w_query.shape
        experts = w_gate.shape[1]
        ff = w_in.shape[2]
        e_loc = experts // N_DEV
        capacity = (2 * seq + experts - 1) // experts
        hw = heads * head_dim
        rows = 2 * capacity
        steps = groups // 2
        all_rows = N_DEV * steps * rows

        wq, wk, wv = (w.transpose(1, 2, 0).reshape(hw, d_model) for w in (w_query, w_key, w_value))
        wo = w_attn_out.reshape(hw, d_model)

        def whole(shape):
            return pl.BlockSpec(shape, lambda i: (0,) * len(shape), pipeline_mode=pl.Buffered(1))

        anywhere = pl.BlockSpec(memory_space=pl.ANY)
        front_specs = [
            pl.BlockSpec((2, seq, d_model), lambda i: (i, 0, 0)),
            whole((groups, seq)), whole((groups, seq)),
            pl.BlockSpec((2, 2, seq), lambda i: (i, 0, 0)),
            whole((d_model,)), whole((hw, d_model)), whole((hw, d_model)), whole((hw, d_model)), whole((hw, d_model)),
            whole((d_model,)), whole((d_model, experts)),
        ]
        quads = steps // 2
        fix_rows = quads * FIX
        dma = pltpu.SemaphoreType.DMA
        hidden_p, meta_p, fix, pack, msg = pl.pallas_call(
            functools.partial(packed_front_kernel, heads=heads, head_dim=head_dim, capacity=capacity),
            name="packed_front",
            grid=(steps,),
            in_specs=front_specs,
            out_specs=[
                pl.BlockSpec((2, seq, d_model), lambda i: (i, 0, 0)),
                pl.BlockSpec((2, 8, seq), lambda i: (i, 0, 0)),
                anywhere, anywhere, anywhere,
            ],
            out_shape=[
                jax.ShapeDtypeStruct((groups, seq, d_model), BF16),
                jax.ShapeDtypeStruct((groups, 8, seq), F32),
                jax.ShapeDtypeStruct((e_loc, N_DEV * fix_rows, d_model), BF16),
                jax.ShapeDtypeStruct((N_DEV, PACK, d_model), BF16),
                jax.ShapeDtypeStruct((N_DEV, 16, 128), F32),
            ],
            scratch_shapes=[
                pltpu.VMEM((hw, 2 * seq), BF16),
                pltpu.VMEM((2 * seq, hw), BF16),
                pltpu.VMEM((hw, 2 * seq), BF16),
                pltpu.VMEM((hw, 2 * seq), BF16),
                pltpu.VMEM((2, 4, seq, seq), F32),
                pltpu.VMEM((2, 4, seq, seq), BF16),
                pltpu.VMEM((3 * experts, d_model), BF16),
                pltpu.VMEM((4 * seq, d_model), BF16),
                pltpu.VMEM((8, 4 * seq), jnp.int32),
                pltpu.VMEM((4, experts, 128), F32),
                pltpu.VMEM((8, 128), F32),
                pltpu.VMEM((N_DEV, 128), F32),
                pltpu.VMEM((N_DEV, 128), F32),
                pltpu.VMEM((N_DEV, 256), F32),
                pltpu.VMEM((N_DEV, quads * LOCAL, d_model), BF16),
                pltpu.VMEM((quads, N_DEV, e_loc, FIX, d_model), BF16),
                pltpu.VMEM((N_DEV, PACK, d_model), BF16),
                pltpu.VMEM((N_DEV, 16, 128), F32),
                dma, dma, dma, dma, dma, dma, dma((3,)),
            ],
            compiler_params=pltpu.CompilerParams(
                dimension_semantics=("arbitrary",), collective_id=0, has_side_effects=True, vmem_limit_bytes=VMEM_LIMIT),
        )(tokens, pad_mask, second_draw, choices.transpose(0, 2, 1), norm_attn, wq, wk, wv, wo, norm_moe, w_gate)

        def packed_path():
            back, back_pack = pl.pallas_call(
                packed_expert_kernel,
                name="packed_experts",
                grid=(e_loc,),
                in_specs=[
                    pl.BlockSpec((1, N_DEV * fix_rows, d_model), lambda i: (i, 0, 0)),
                    whole((N_DEV, PACK, d_model)), whole((N_DEV, 16, 128)),
                    pl.BlockSpec((1, d_model, ff), lambda i: (i, 0, 0)),
                    pl.BlockSpec((1, ff, d_model), lambda i: (i, 0, 0)),
                ],
                out_specs=[anywhere, anywhere],
                out_shape=[
                    jax.ShapeDtypeStruct((experts, fix_rows, d_model), BF16),
                    jax.ShapeDtypeStruct((N_DEV, PACK, d_model), BF16),
                ],
                scratch_shapes=[
                    pltpu.VMEM((N_DEV * fix_rows, ff), BF16),
                    pltpu.VMEM((e_loc, N_DEV // TEAM * POOL, d_model), BF16),
                    pltpu.VMEM((e_loc, N_DEV * fix_rows, d_model), BF16),
                    pltpu.VMEM((e_loc, N_DEV // TEAM * POOL, d_model), BF16),
                    pltpu.VMEM((N_DEV, 128), F32),
                    pltpu.VMEM((N_DEV, PACK, d_model), BF16),
                    dma, dma, dma, dma, dma((2,)),
                ],
                compiler_params=pltpu.CompilerParams(
                    dimension_semantics=("arbitrary",), collective_id=1, has_side_effects=True, vmem_limit_bytes=VMEM_LIMIT),
            )(fix, pack, msg, w_in, w_out)
            return pl.pallas_call(
                functools.partial(packed_back_kernel, n_groups=groups * N_DEV),
                name="packed_back",
                grid=(steps,),
                in_specs=[
                    pl.BlockSpec((experts, FIX, d_model), lambda i: (0, i // 2, 0)),
                    whole((N_DEV, PACK, d_model)),
                    pl.BlockSpec((2, seq, d_model), lambda i: (i, 0, 0)),
                    pl.BlockSpec((2, 8, seq), lambda i: (i, 0, 0)),
                    whole((N_DEV, 16, 128)),
                ],
                out_specs=[
                    pl.BlockSpec((2, seq, d_model), lambda i: (i, 0, 0)),
                    pl.BlockSpec((8, 128), lambda i: (0, 0)),
                ],
                out_shape=[
                    jax.ShapeDtypeStruct((groups, seq, d_model), BF16),
                    jax.ShapeDtypeStruct((8, 128), F32),
                ],
                compiler_params=pltpu.CompilerParams(dimension_semantics=("arbitrary",), vmem_limit_bytes=VMEM_LIMIT),
            )(back, back_pack, hidden_p, meta_p, msg)

        def full_path():
            recv = pl.pallas_call(
                functools.partial(full_front_kernel, experts=experts, capacity=capacity),
                name="full_front",
                grid=(steps,),
                in_specs=[
                    pl.BlockSpec((2, seq, d_model), lambda i: (i, 0, 0)),
                    pl.BlockSpec((2, 8, seq), lambda i: (i, 0, 0)),
                    whole((d_model,)),
                ],
                out_specs=anywhere,
                out_shape=jax.ShapeDtypeStruct((e_loc, all_rows, d_model), BF16),
                scratch_shapes=[pltpu.VMEM((steps, N_DEV, e_loc, rows, d_model), BF16), dma, dma, dma],
                compiler_params=pltpu.CompilerParams(
                    dimension_semantics=("arbitrary",), collective_id=2, has_side_effects=True, vmem_limit_bytes=VMEM_LIMIT),
            )(hidden_p, meta_p, norm_moe)
            tile = all_rows // 4
            ret = pl.pallas_call(
                functools.partial(expert_kernel, tile=tile),
                name="full_experts",
                grid=(e_loc,),
                in_specs=[
                    pl.BlockSpec((1, all_rows, d_model), lambda i: (i, 0, 0)),
                    pl.BlockSpec((1, d_model, ff), lambda i: (i, 0, 0)),
                    pl.BlockSpec((1, ff, d_model), lambda i: (i, 0, 0)),
                ],
                out_specs=anywhere,
                out_shape=jax.ShapeDtypeStruct((experts, steps * rows, d_model), BF16),
                scratch_shapes=[pltpu.VMEM((tile, ff), BF16), pltpu.VMEM((e_loc, all_rows, d_model), BF16), dma, dma, dma],
                compiler_params=pltpu.CompilerParams(
                    dimension_semantics=("arbitrary",), collective_id=3, has_side_effects=True, vmem_limit_bytes=VMEM_LIMIT),
            )(recv, w_in, w_out)
            return pl.pallas_call(
                functools.partial(back_kernel, n_groups=groups * N_DEV, capacity=capacity),
                name="full_back",
                grid=(steps,),
                in_specs=[
                    pl.BlockSpec((experts, rows, d_model), lambda i: (0, i, 0)),
                    pl.BlockSpec((2, seq, d_model), lambda i: (i, 0, 0)),
                    pl.BlockSpec((2, 8, seq), lambda i: (i, 0, 0)),
                    whole((N_DEV, 16, 128)),
                ],
                out_specs=[
                    pl.BlockSpec((2, seq, d_model), lambda i: (i, 0, 0)),
                    pl.BlockSpec((8, 128), lambda i: (0, 0)),
                ],
                out_shape=[
                    jax.ShapeDtypeStruct((groups, seq, d_model), BF16),
                    jax.ShapeDtypeStruct((8, 128), F32),
                ],
                compiler_params=pltpu.CompilerParams(dimension_semantics=("arbitrary",), vmem_limit_bytes=VMEM_LIMIT),
            )(ret, hidden_p, meta_p, msg)

        shared = jnp.sum(msg[:, 10, :].reshape(N_DEV // TEAM, TEAM, experts), axis=1)
        spilled = (jnp.max(msg[:, 9, 0]) > 0.0) | (jnp.max(shared) > POOL)
        out, aux = lax.cond(spilled, full_path, packed_path)
        return out, aux[0, 0]

    by_group = P("ep")
    replicated = P()
    in_specs = (by_group, by_group, by_group, by_group, replicated, replicated, replicated, replicated, replicated, replicated, replicated, by_group, by_group)
    return jax.shard_map(local_step, mesh=mesh, in_specs=in_specs, out_specs=(by_group, replicated), check_vma=False)
```

```python
import functools
import jax
import jax.numpy as jnp
from jax import lax
from jax.experimental import pallas as pl
from jax.experimental.pallas import tpu as pltpu
from jax.sharding import PartitionSpec as P

NORM_EPS = 1e-6
N_DEV = 16
MESH = pl.DeviceIdType.MESH
F32 = jnp.float32
BF16 = jnp.bfloat16
ORDER = (0, 9, 2, 11, 4, 13, 6, 15, 8, 1, 10, 3, 12, 5, 14, 7)
VMEM_LIMIT = 62 * 1024 * 1024


def partner(me, mask):
    out = 0
    for bit in range(4):
        val = lax.rem(me // (1 << bit), 2)
        out = out + (1 << bit) * ((1 - val) if (mask >> bit) & 1 else val)
    return out


def greet(me):
    barrier = pltpu.get_barrier_semaphore()
    for mask in range(1, N_DEV):
        pl.semaphore_signal(barrier, inc=1, device_id=(partner(me, mask),), device_id_type=MESH)


def rms_norm(values_f, scale_vec):
    inv_rms = lax.rsqrt(jnp.mean(values_f * values_f, axis=-1, keepdims=True) + NORM_EPS)
    return (values_f * inv_rms * scale_vec).astype(BF16)


def dot(a, b):
    return jnp.dot(a, b, preferred_element_type=F32)


def dot_nt(a, b):
    return lax.dot_general(a, b, (((1,), (1,)), ((), ())), preferred_element_type=F32)


def split_gate(wgate_ref, wg_s):
    experts = wgate_ref.shape[1]
    wg = wgate_ref[...].T
    hi = wg.astype(BF16)
    rest = wg - hi.astype(F32)
    mid = rest.astype(BF16)
    low = (rest - mid.astype(F32)).astype(BF16)
    wg_s[0:experts] = hi
    wg_s[experts:2 * experts] = mid
    wg_s[2 * experts:3 * experts] = low


def attend(
    step, tokens_ref, pad_ref, norm_attn_ref, wq_ref, wk_ref, wv_ref, wo_ref, norm_moe_ref, hidden_ref,
    q_s, k_s, v_s, ctx_s, s_s, p_s, wg_s, heads, head_dim, experts,
):
    seq = tokens_ref.shape[1]
    d_model = tokens_ref.shape[2]
    x = tokens_ref[...].reshape(2 * seq, d_model)
    a = rms_norm(x.astype(F32), norm_attn_ref[...][None, :])
    q_s[...] = dot_nt(wq_ref[...], a).astype(BF16)
    k_s[...] = dot_nt(a, wk_ref[...]).astype(BF16)
    v_s[...] = dot_nt(wv_ref[...], a).astype(BF16)

    width = 2 * head_dim
    lane = lax.broadcasted_iota(jnp.int32, (1, width), 1)
    scale = head_dim ** -0.5
    sides = [jnp.where(lane < head_dim, scale, 0.0).astype(BF16), jnp.where(lane < head_dim, 0.0, scale).astype(BF16)]
    cut = seq // 2
    late_key = lax.broadcasted_iota(jnp.int32, (seq - cut, 128), 0) + cut
    batch = s_s.shape[1]
    lanes = 128
    buf = 0
    for grp in range(2):
        tok = pl.ds(grp * seq, seq)
        length = jnp.sum(pad_ref[pl.ds(2 * step + grp, 1), :], axis=1, keepdims=True)
        keep_late = late_key < length
        for first in range(0, heads, batch):
            for i in range(batch):
                off = (first + i) // 2 * width
                k = k_s[tok, pl.ds(off, width)] * sides[(first + i) % 2]
                s_s[buf, i] = dot(k, q_s[pl.ds(off, width), tok])
            for i in range(batch):
                for col in range(0, seq, lanes):
                    cols = pl.ds(col, lanes)
                    early = s_s[buf, i, pl.ds(0, cut), cols]
                    late = jnp.where(keep_late, s_s[buf, i, pl.ds(cut, seq - cut), cols], -1e30)
                    top = jnp.maximum(jnp.max(early, axis=0, keepdims=True), jnp.max(late, axis=0, keepdims=True))
                    early = jnp.exp(early - top)
                    late = jnp.exp(late - top)
                    inv = 1.0 / (jnp.sum(early, axis=0, keepdims=True) + jnp.sum(late, axis=0, keepdims=True))
                    p_s[buf, i, pl.ds(0, cut), cols] = (early * inv).astype(BF16)
                    p_s[buf, i, pl.ds(cut, seq - cut), cols] = (late * inv).astype(BF16)
            for i in range(batch):
                head = pl.ds((first + i) * head_dim, head_dim)
                ctx_s[head, tok] = dot(v_s[head, tok], p_s[buf, i]).astype(BF16)
            buf = 1 - buf

    attn = lax.dot_general(ctx_s[...], wo_ref[...], (((0,), (0,)), ((), ())), preferred_element_type=F32)
    hidden = (x.astype(F32) + attn).astype(BF16)
    hidden_ref[...] = hidden.reshape(2, seq, d_model)
    b = rms_norm(hidden.astype(F32), norm_moe_ref[...][None, :])
    lg = dot_nt(wg_s[...], b)
    logits = (lg[2 * experts:] + lg[experts:2 * experts]) + lg[:experts]
    ex = jnp.exp(logits - jnp.max(logits, axis=0, keepdims=True))
    return b, ex / jnp.sum(ex, axis=0, keepdims=True)


def full_front_kernel(hidden_ref, meta_ref, norm_moe_ref, recv_ref, send_s, send_sem, recv_sem, own_sem, *, experts, capacity):
    step = pl.program_id(0)
    steps = pl.num_programs(0)
    me = lax.axis_index("ep")
    seq = hidden_ref.shape[1]
    d_model = hidden_ref.shape[2]
    e_loc = experts // N_DEV
    half = e_loc // 2
    slots = experts * capacity
    rows = 2 * capacity
    per_src = steps * rows

    def send_pair(pair):
        for place, mask in enumerate(ORDER):
            dev = partner(me, mask)
            src = send_s.at[pair, dev]
            dst = recv_ref.at[:, pl.ds(pl.multiple_of(place * per_src + pair * rows, rows), rows), :]
            if mask == 0:
                pltpu.make_async_copy(src, dst, own_sem).start()
            else:
                pltpu.make_async_remote_copy(
                    src_ref=src, dst_ref=dst, send_sem=send_sem, recv_sem=recv_sem,
                    device_id=(dev,), device_id_type=MESH).start()

    @pl.when(step == 0)
    def _():
        greet(me)

    @pl.when(step == 1)
    def _():
        pl.semaphore_wait(pltpu.get_barrier_semaphore(), N_DEV - 1)

    @pl.when(step > 0)
    def _():
        send_pair(step - 1)

    slot_id = lax.broadcasted_iota(jnp.int32, (slots, seq), 0)
    picked = []
    for grp in range(2):
        b = rms_norm(hidden_ref[grp].astype(F32), norm_moe_ref[...][None, :])

        def place_of(code):
            e = code // capacity
            dev = e // e_loc
            r = e - dev * e_loc
            upper = r // half
            side = upper if grp == 0 else 1 - upper
            at = ((dev * half + r - upper * half) * 2 + side) * capacity + code - e * capacity
            return jnp.where(code >= 0, at, -1)

        d1 = place_of(meta_ref[grp, 4:5, :].astype(jnp.int32))
        d2 = place_of(meta_ref[grp, 5:6, :].astype(jnp.int32))
        disp_mat = jnp.where((slot_id == d1) | (slot_id == d2), 1.0, 0.0).astype(BF16)
        picked.append(dot(disp_mat, b).reshape(N_DEV * half, rows, d_model))

    top = lax.broadcasted_iota(jnp.int32, (1, rows, 1), 1) < capacity
    lower = jnp.where(top, picked[0], picked[1]).astype(BF16)
    upper = jnp.where(top, picked[1], picked[0]).astype(BF16)
    send_s[step, :, 0:half] = lower.reshape(N_DEV, half, rows, d_model)
    send_s[step, :, half:e_loc] = upper.reshape(N_DEV, half, rows, d_model)

    @pl.when(step == steps - 1)
    def _():
        send_pair(steps - 1)
        others = pl.ds(0, N_DEV - 1)
        pltpu.make_async_copy(send_s.at[:, others], send_s.at[:, others], send_sem).wait()
        pltpu.make_async_copy(send_s.at[:, 0], send_s.at[:, 0], own_sem).wait()
        arrived = recv_ref.at[:, pl.ds(0, (N_DEV - 1) * per_src), :]
        pltpu.make_async_copy(arrived, arrived, recv_sem).wait()


def expert_kernel(recv_ref, w_in_ref, w_out_ref, ret_ref, act_s, z_s, send_sem, recv_sem, local_sem, *, tile):
    e = pl.program_id(0)
    n_exp = pl.num_programs(0)
    me = lax.axis_index("ep")
    rows = recv_ref.shape[1]
    ff = w_in_ref.shape[2]
    per_src = rows // N_DEV
    n_tiles = rows // tile
    chunk = 1024

    @pl.when(e == 0)
    def _():
        greet(me)

    def run(t, carry):
        at = pl.ds(pl.multiple_of(t * tile, tile), tile)
        x = recv_ref[0, at, :]
        for f in range(ff // chunk):
            act = dot(x, w_in_ref[0, :, pl.ds(f * chunk, chunk)])
            act_s[:, pl.ds(f * chunk, chunk)] = jnp.maximum(act, 0.0).astype(BF16)
        z_s[e, at, :] = dot(act_s[...], w_out_ref[0]).astype(BF16)
        return carry

    lax.fori_loop(0, n_tiles, run, 0)

    @pl.when(e == 0)
    def _():
        pl.semaphore_wait(pltpu.get_barrier_semaphore(), N_DEV - 1)

    for place, mask in enumerate(ORDER):
        dev = partner(me, mask)
        src = z_s.at[e, pl.ds(place * per_src, per_src), :]
        dst = ret_ref.at[me * n_exp + e]
        if mask == 0:
            pltpu.make_async_copy(src, dst, local_sem).start()
        else:
            pltpu.make_async_remote_copy(
                src_ref=src, dst_ref=dst, send_sem=send_sem, recv_sem=recv_sem,
                device_id=(dev,), device_id_type=MESH).start()

    @pl.when(e == n_exp - 1)
    def _():
        sent = z_s.at[:, pl.ds(0, (N_DEV - 1) * per_src), :]
        pltpu.make_async_copy(sent, sent, send_sem).wait()
        own = z_s.at[:, pl.ds(0, per_src), :]
        pltpu.make_async_copy(own, own, local_sem).wait()
        arrived = ret_ref.at[pl.ds(0, (N_DEV - 1) * n_exp)]
        pltpu.make_async_copy(arrived, arrived, recv_sem).wait()


def back_kernel(ret_ref, hidden_ref, meta_ref, msg_ref, out_ref, aux_ref, *, n_groups, capacity):
    experts, rows, d_model = ret_ref.shape
    seq = hidden_ref.shape[1]
    z = ret_ref[...].reshape(experts * rows, d_model)
    slot_id = lax.broadcasted_iota(jnp.int32, (seq, experts * rows), 1)
    e_loc = experts // N_DEV
    for grp in range(2):
        meta = meta_ref[grp].T

        def place_of(code):
            e = code // capacity
            r = e - e // e_loc * e_loc
            upper = r // (e_loc // 2)
            side = upper if grp == 0 else 1 - upper
            return jnp.where(code >= 0, (e * 2 + side) * capacity + code - e * capacity, -1)

        c1 = place_of(meta[:, 4:5].astype(jnp.int32))
        c2 = place_of(meta[:, 5:6].astype(jnp.int32))
        comb = jnp.where(slot_id == c1, meta[:, 2:3], 0.0) + jnp.where(slot_id == c2, meta[:, 3:4], 0.0)
        moe = dot(comb.astype(BF16), z)
        out_ref[grp] = (hidden_ref[grp].astype(F32) + moe).astype(BF16)

    @pl.when(pl.program_id(0) == 0)
    def _():
        aux_ref[0, 0] = jnp.sum(msg_ref[:, 0:8, :]) * (experts / n_groups)


FIX = 8
LOCAL = 48
PACK = 112
EXTRA = 32
TEAM = 4
POOL = 80
WINDOW = 64


def twice(value):
    return jnp.concatenate([value, value], axis=1)


def packed_front_kernel(
    tokens_ref, pad_ref, draw_ref, choices_ref, norm_attn_ref, wq_ref, wk_ref, wv_ref, wo_ref, norm_moe_ref, wgate_ref,
    hidden_ref, meta_ref, pack_s, starts_ref, fix_ref, msg_ref,
    q_s, k_s, v_s, ctx_s, s_s, p_s, wg_s, b_s, slot_s, count_s, aux_s, flag_s, code_s, goal_s,
    local_s, fix_s, msg_s, fix_send, fix_recv, msg_send, msg_recv, own_sem,
    *, heads, head_dim, capacity,
):
    step = pl.program_id(0)
    steps = pl.num_programs(0)
    quad = step // 2
    quads = steps // 2
    me = lax.axis_index("ep")
    seq = tokens_ref.shape[1]
    d_model = tokens_ref.shape[2]
    experts = wgate_ref.shape[1]
    e_loc = experts // N_DEV

    def remote(src, dst, send_sem, recv_sem, dev, mask, own):
        if mask == 0:
            pltpu.make_async_copy(src, dst, own_sem.at[own]).start()
        else:
            pltpu.make_async_remote_copy(
                src_ref=src, dst_ref=dst, send_sem=send_sem, recv_sem=recv_sem,
                device_id=(dev,), device_id_type=MESH).start()

    def send_quad(which):
        for place, mask in enumerate(ORDER):
            dev = partner(me, mask)
            row = pl.multiple_of(place * quads * FIX + which * FIX, FIX)
            remote(fix_s.at[which, dev], fix_ref.at[:, pl.ds(row, FIX), :], fix_send, fix_recv, dev, mask, 0)

    @pl.when(step == 0)
    def _():
        greet(me)
        split_gate(wgate_ref, wg_s)
        aux_s[...] = jnp.zeros_like(aux_s)
        flag_s[...] = jnp.zeros_like(flag_s)
        code_s[...] = jnp.zeros_like(code_s)
        goal_s[...] = jnp.zeros_like(goal_s)
        count_s[...] = jnp.zeros_like(count_s)

    @pl.when(step == 2)
    def _():
        pl.semaphore_wait(pltpu.get_barrier_semaphore(), N_DEV - 1)

    @pl.when((step > 0) & (lax.rem(step, 2) == 0))
    def _():
        send_quad(quad - 1)

    b, gate_probs = attend(
        step, tokens_ref, pad_ref, norm_attn_ref, wq_ref, wk_ref, wv_ref, wo_ref, norm_moe_ref, hidden_ref,
        q_s, k_s, v_s, ctx_s, s_s, p_s, wg_s, heads, head_dim, experts)
    side = lax.rem(step, 2)
    b_s[pl.ds(pl.multiple_of(side * 2 * seq, 2 * seq), 2 * seq), :] = b

    eid = lax.broadcasted_iota(jnp.int32, (experts, seq), 0)
    tri = jnp.where(lax.broadcasted_iota(jnp.int32, (seq, seq), 0) <= lax.broadcasted_iota(jnp.int32, (seq, seq), 1), 1.0, 0.0)
    tri = jnp.concatenate([tri, jnp.ones((seq, 128), F32)], axis=1).astype(BF16)
    row_e = lax.broadcasted_iota(jnp.int32, (experts, experts), 0)
    col_e = lax.broadcasted_iota(jnp.int32, (experts, experts), 1)
    same = row_e // e_loc == col_e // e_loc
    mix = jnp.concatenate([jnp.where(same & (col_e < row_e), 1.0, 0.0), jnp.where(same, 1.0, 0.0)], axis=0).astype(BF16)
    spot = lax.broadcasted_iota(jnp.int32, (experts, 128), 1).astype(F32)
    code0 = (lax.rem(lax.broadcasted_iota(jnp.int32, (experts, 128), 0), e_loc) * EXTRA + 1).astype(F32)
    meta_row = lax.broadcasted_iota(jnp.int32, (8, seq), 0)

    def window_start():
        return jnp.minimum(jnp.floor(count_s[3] * (1.0 / 16)) * 16.0, float(PACK - WINDOW))

    for grp in range(2):
        p = gate_probs[:, grp * seq:(grp + 1) * seq]
        valid = pad_ref[pl.ds(2 * step + grp, 1), :] == 1
        draw = draw_ref[pl.ds(2 * step + grp, 1), :]
        e1 = choices_ref[grp, 0:1, :]
        e2 = choices_ref[grp, 1:2, :]
        hot1 = eid == e1
        hot2 = eid == e2
        p1 = jnp.sum(jnp.where(hot1, p, 0.0), axis=0, keepdims=True)
        p2 = jnp.sum(jnp.where(hot2, p, 0.0), axis=0, keepdims=True)
        g1 = p1 / (p1 + p2)
        g2 = p2 / (p1 + p2)
        want2 = valid & (draw < 2.0 * g2)
        take1 = jnp.where(hot1 & valid, 1.0, 0.0)
        take2 = jnp.where(hot2 & want2, 1.0, 0.0)
        cum = dot(jnp.concatenate([take1, take2], axis=0).astype(BF16), tri)
        cum1 = cum[:experts, :seq]
        cum2 = cum[experts:, :seq]
        count1 = cum[:experts, seq:]
        count2 = cum[experts:, seq:]
        first = jnp.minimum(count1, float(capacity))
        pos1 = jnp.sum((cum1 - 1.0) * take1, axis=0, keepdims=True)
        pos2 = jnp.sum((cum2 - 1.0 + twice(first)) * take2, axis=0, keepdims=True)
        keep1 = valid & (pos1 < capacity)
        keep2 = want2 & (pos2 < capacity)

        share = jnp.where(valid, p, 0.0) * twice(count1 * (1.0 / (seq * seq)))
        share = jnp.sum(share.reshape(experts // 8, 8, seq), axis=0)
        for col in range(seq // 128):
            aux_s[...] += share[:, col * 128:(col + 1) * 128]

        before = count_s[0]
        after = before + jnp.minimum(first + count2, float(capacity))
        new = jnp.maximum(after - FIX, 0.0) - jnp.maximum(before - FIX, 0.0)
        sums = dot(mix, new.astype(BF16))
        packed = count_s[1]
        begin = packed + sums[:experts]
        shift = begin - jnp.maximum(before, float(FIX)) + before
        local = shift - count_s[3]
        window = shift - window_start()
        inside = (spot >= begin) & (spot < begin + new)
        code = jnp.where(inside, code0 + count_s[2] + spot - begin, 0.0)
        code_s[...] += jnp.sum(code.reshape(N_DEV, e_loc, 128), axis=1)
        count_s[0] = after
        count_s[1] = packed + sums[experts:]
        count_s[2] += new

        def places(e, take, pos, keep):
            index = pos + jnp.sum(twice(before) * take, axis=0, keepdims=True)
            in_window = pos + jnp.sum(twice(window) * take, axis=0, keepdims=True)
            in_local = pos + jnp.sum(twice(local) * take, axis=0, keepdims=True)
            e = e.astype(F32)
            dev = jnp.floor(e * (1.0 / e_loc))
            fixed = keep & (index < FIX)
            loose = keep & (index >= FIX)
            at_fix = jnp.where(fixed, e * FIX + index, -1.0)
            at_local = jnp.where(loose, dev * LOCAL + in_local, -1.0)
            at_back = jnp.where(loose, experts * FIX + dev * WINDOW + in_window, at_fix)
            return at_fix, at_local, at_back, jnp.where(keep, e * capacity + pos, -1.0)

        f1, l1, c1, w1 = places(e1, take1, pos1, keep1)
        f2, l2, c2, w2 = places(e2, take2, pos2, keep2)
        meta = jnp.where(meta_row == 0, c1, 0.0)
        meta = jnp.where(meta_row == 1, c2, meta)
        meta = jnp.where(meta_row == 2, g1, meta)
        meta = jnp.where(meta_row == 3, g2, meta)
        meta = jnp.where(meta_row == 4, w1, meta)
        meta = jnp.where(meta_row == 5, w2, meta)
        meta_ref[grp] = meta
        tok = pl.ds(pl.multiple_of(side * 2 * seq + grp * seq, seq), seq)
        slot_s[:, tok] = jnp.where(meta_row == 0, f1, jnp.where(meta_row == 1, f2, jnp.where(meta_row == 2, l1, l2))).astype(jnp.int32)

    @pl.when(side == 1)
    def _():
        def gather(first_row, base, count, skip):
            ids = lax.broadcasted_iota(jnp.int32, (count, 4 * seq - skip), 0) + base
            hit = (ids == slot_s[first_row:first_row + 1, skip:]) | (ids == slot_s[first_row + 1:first_row + 2, skip:])
            return dot(jnp.where(hit, 1.0, 0.0).astype(BF16), b_s[skip:, :]).astype(BF16)

        per_dev = e_loc * FIX
        for base in range(0, N_DEV, 4):
            rows = gather(0, base * per_dev, 4 * per_dev, 0)
            fix_s[quad, base:base + 4] = rows.reshape(4, e_loc, FIX, d_model)
        for base in range(0, N_DEV, 4):
            rows = gather(2, base * LOCAL, 4 * LOCAL, 2 * seq)
            local_s[base:base + 4, pl.ds(pl.multiple_of(quad * LOCAL, LOCAL), LOCAL), :] = rows.reshape(4, LOCAL, d_model)

        def per_device(value):
            return value.reshape(N_DEV, e_loc, 128)[:, 0, :]

        start = per_device(count_s[3])
        filled = per_device(count_s[1]) - start
        at = lax.broadcasted_iota(jnp.int32, (N_DEV, 256), 1).astype(F32) - (quad * LOCAL).astype(F32)
        live = (at >= 0.0) & (at < float(LOCAL)) & (at < twice(filled))
        goal_s[...] = jnp.where(live, twice(start) + at + 1.0, goal_s[...])
        flag_s[...] = jnp.maximum(flag_s[...], jnp.where(filled > LOCAL, 1.0, 0.0))
        starts_ref[pl.ds(quad, 1), :] = window_start().T[0:1, :].astype(jnp.int32)
        count_s[0] = jnp.zeros_like(count_s[0])
        count_s[3] = count_s[1]

    @pl.when(step == steps - 1)
    def _():
        send_quad(quads - 1)
        over = jnp.where((count_s[1] > PACK) | (count_s[2] > EXTRA), 1.0, 0.0)
        over = jnp.max(jnp.max(over.reshape(N_DEV, e_loc, 128), axis=1), axis=0, keepdims=True)
        over = jnp.maximum(over, jnp.max(flag_s[...], axis=0, keepdims=True))
        tally = count_s[2].T[0:1, :]
        for dev in range(N_DEV):
            msg_s[dev, 0:8] = aux_s[...]
            lower = lax.broadcasted_iota(jnp.int32, (8, 128), 0)
            msg_s[dev, 8:16] = jnp.where(lower == 0, code_s[dev:dev + 1, :], jnp.where(lower == 1, over, jnp.where(lower == 2, tally, 0.0)))
        for place, mask in enumerate(ORDER):
            dev = partner(me, mask)
            remote(msg_s.at[dev], msg_ref.at[place], msg_send, msg_recv, dev, mask, 1)

        width = goal_s.shape[1] * 3 // 4
        rows = lax.broadcasted_iota(jnp.int32, (PACK, width), 0).astype(F32) + 1.0
        for dev in range(N_DEV):
            hit = jnp.where(rows == goal_s[dev:dev + 1, 0:width], 1.0, 0.0).astype(BF16)
            pack_s[dev] = dot(hit, local_s[dev]).astype(BF16)

        def settle(ref, sem):
            pltpu.make_async_copy(ref, ref, sem).wait()

        others = pl.ds(0, N_DEV - 1)
        settle(fix_s.at[:, 0], own_sem.at[0])
        settle(msg_s.at[0], own_sem.at[1])
        settle(fix_s.at[:, others], fix_send)
        settle(msg_s.at[others], msg_send)
        settle(fix_ref.at[:, pl.ds(0, (N_DEV - 1) * quads * FIX), :], fix_recv)
        settle(msg_ref.at[others], msg_recv)


def packed_expert_kernel(
    fix_ref, mine_ref, msg_ref, w_in_ref, w_out_ref, back_ref, back_pack_ref,
    act_s, x_s, z_s, zx_s, code_s, pack_ref, pack_s, in_send, in_recv, fix_send, fix_recv, pack_send, pack_recv, own_sem,
):
    step = pl.program_id(0)
    n_exp = pl.num_programs(0) // 2
    e = lax.rem(step, n_exp)
    me = lax.axis_index("ep")
    rows = fix_ref.shape[1]
    d_model = fix_ref.shape[2]
    ff = w_in_ref.shape[2]
    per_src = rows // N_DEV
    chunk = 1024

    def mlp(x):
        for f in range(ff // chunk):
            act = dot(x, w_in_ref[0, :, pl.ds(f * chunk, chunk)])
            act_s[0:x.shape[0], pl.ds(f * chunk, chunk)] = jnp.maximum(act, 0.0).astype(BF16)
        return dot(act_s[0:x.shape[0], :], w_out_ref[0]).astype(BF16)

    def spread(place):
        ids = lax.broadcasted_iota(jnp.int32, (x_s.shape[0] * POOL, PACK), 0).astype(F32) + 1.0
        return jnp.where(ids == code_s[place:place + 1, 0:PACK], 1.0, 0.0).astype(BF16)

    def remote(src, dst, send_sem, recv_sem, mask, own):
        if mask == 0:
            pltpu.make_async_copy(src, dst, own_sem.at[own]).start()
        else:
            pltpu.make_async_remote_copy(
                src_ref=src, dst_ref=dst, send_sem=send_sem, recv_sem=recv_sem,
                device_id=(partner(me, mask),), device_id_type=MESH).start()

    def settle(ref, sem):
        pltpu.make_async_copy(ref, ref, sem).wait()

    others = pl.ds(0, N_DEV - 1)

    @pl.when(step == 0)
    def _():
        greet(me)
        pl.semaphore_wait(pltpu.get_barrier_semaphore(), N_DEV - 1)
        for place, mask in enumerate(ORDER):
            remote(mine_ref.at[partner(me, mask)], pack_ref.at[place], in_send, in_recv, mask, 0)

    @pl.when(step < n_exp)
    def _():
        z_s[e] = mlp(fix_ref[0])
        for place, mask in enumerate(ORDER):
            remote(z_s.at[e, pl.ds(place * per_src, per_src), :], back_ref.at[me * n_exp + e], fix_send, fix_recv, mask, 1)

    @pl.when(step == n_exp)
    def _():
        settle(pack_ref.at[0], own_sem.at[0])
        settle(pack_ref.at[others], in_recv)
        code = jnp.concatenate([msg_ref[place, 8:9, :] for place in range(N_DEV)], axis=0)
        n_loc = x_s.shape[0]
        hits = [(code > ex * EXTRA) & (code <= (ex + 1) * EXTRA) for ex in range(n_loc)]
        row = lax.broadcasted_iota(jnp.int32, (N_DEV, N_DEV), 0)
        col = lax.broadcasted_iota(jnp.int32, (N_DEV, N_DEV), 1)
        prior = jnp.where((row // TEAM == col // TEAM) & (col < row), 1.0, 0.0).astype(BF16)
        spans = dot(prior, jnp.concatenate([jnp.where(hit, 1.0, 0.0) for hit in hits], axis=1).astype(BF16))
        shared = jnp.zeros_like(code)
        for ex, hit in enumerate(hits):
            begin = jnp.sum(spans[:, ex * 128:(ex + 1) * 128], axis=1, keepdims=True)
            shared = jnp.where(hit, code + begin + float(ex * (POOL - EXTRA)), shared)
        code_s[...] = shared
        for team in range(N_DEV // TEAM):
            x = dot(spread(team * TEAM), pack_ref[team * TEAM])
            for place in range(team * TEAM + 1, (team + 1) * TEAM):
                x = x + dot(spread(place), pack_ref[place])
            x_s[:, pl.ds(team * POOL, POOL), :] = x.astype(BF16).reshape(n_loc, POOL, d_model)

    @pl.when(step >= n_exp)
    def _():
        zx_s[e] = mlp(x_s[e])

    @pl.when(step == 2 * n_exp - 1)
    def _():
        for place, mask in enumerate(ORDER):
            z = zx_s[:, pl.ds(place // TEAM * POOL, POOL), :].reshape(x_s.shape[0] * POOL, d_model)
            pack_s[place] = lax.dot_general(
                spread(place), z, (((0,), (0,)), ((), ())), preferred_element_type=F32).astype(BF16)
            if place > 0:
                remote(pack_s.at[place - 1], back_pack_ref.at[me], pack_send, pack_recv, ORDER[place - 1], 2)
        remote(pack_s.at[N_DEV - 1], back_pack_ref.at[me], pack_send, pack_recv, ORDER[N_DEV - 1], 2)
        settle(z_s.at[:, pl.ds(0, per_src), :], own_sem.at[1])
        settle(pack_s.at[0], own_sem.at[2])
        settle(mine_ref.at[others], in_send)
        settle(z_s.at[:, pl.ds(0, (N_DEV - 1) * per_src), :], fix_send)
        settle(pack_s.at[others], pack_send)
        settle(back_ref.at[pl.ds(0, (N_DEV - 1) * n_exp)], fix_recv)
        settle(back_pack_ref.at[others], pack_recv)


def packed_back_kernel(starts_ref, fix_ref, pack_ref, hidden_ref, meta_ref, msg_ref, out_ref, aux_ref, window_s, *, n_groups):
    experts, rows, d_model = fix_ref.shape
    seq = hidden_ref.shape[1]
    z = fix_ref[...].reshape(experts * rows, d_model)
    step = pl.program_id(0)

    @pl.when(lax.rem(step, 2) == 0)
    def _():
        for dev in range(N_DEV):
            start = pl.multiple_of(starts_ref[step // 2, dev * (experts // N_DEV)], 16)
            window_s[dev * WINDOW:(dev + 1) * WINDOW, :] = pack_ref[dev, pl.ds(start, WINDOW), :]

    zx = window_s[...]
    fix_id = lax.broadcasted_iota(jnp.int32, (seq, experts * rows), 1)
    pack_id = lax.broadcasted_iota(jnp.int32, (seq, N_DEV * WINDOW), 1) + experts * rows
    for grp in range(2):
        meta = meta_ref[grp].T
        c1 = meta[:, 0:1].astype(jnp.int32)
        c2 = meta[:, 1:2].astype(jnp.int32)
        g1 = meta[:, 2:3]
        g2 = meta[:, 3:4]

        def gates(ids):
            return jnp.where(ids == c1, g1, jnp.where(ids == c2, g2, 0.0)).astype(BF16)

        moe = dot(gates(fix_id), z) + dot(gates(pack_id), zx)
        out_ref[grp] = (hidden_ref[grp].astype(F32) + moe).astype(BF16)

    @pl.when(pl.program_id(0) == 0)
    def _():
        aux_ref[0, 0] = jnp.sum(msg_ref[:, 0:8, :]) * (experts / n_groups)


def solution(mesh):
    def local_step(tokens, pad_mask, second_draw, choices, norm_attn, w_query, w_key, w_value, w_attn_out, norm_moe, w_gate, w_in, w_out):
        groups, seq, d_model = tokens.shape
        _, heads, head_dim = w_query.shape
        experts = w_gate.shape[1]
        ff = w_in.shape[2]
        e_loc = experts // N_DEV
        capacity = (2 * seq + experts - 1) // experts
        hw = heads * head_dim
        rows = 2 * capacity
        steps = groups // 2
        all_rows = N_DEV * steps * rows

        wq, wk, wv = (w.transpose(1, 2, 0).reshape(hw, d_model) for w in (w_query, w_key, w_value))
        wo = w_attn_out.reshape(hw, d_model)

        def whole(shape):
            return pl.BlockSpec(shape, lambda i: (0,) * len(shape), pipeline_mode=pl.Buffered(1))

        anywhere = pl.BlockSpec(memory_space=pl.ANY)
        front_specs = [
            pl.BlockSpec((2, seq, d_model), lambda i: (i, 0, 0)),
            whole((groups, seq)), whole((groups, seq)),
            pl.BlockSpec((2, 2, seq), lambda i: (i, 0, 0)),
            whole((d_model,)), whole((hw, d_model)), whole((hw, d_model)), whole((hw, d_model)), whole((hw, d_model)),
            whole((d_model,)), whole((d_model, experts)),
        ]
        quads = steps // 2
        fix_rows = quads * FIX
        dma = pltpu.SemaphoreType.DMA
        hidden_p, meta_p, mine, starts, fix, msg = pl.pallas_call(
            functools.partial(packed_front_kernel, heads=heads, head_dim=head_dim, capacity=capacity),
            name="packed_front",
            grid=(steps,),
            in_specs=front_specs,
            out_specs=[
                pl.BlockSpec((2, seq, d_model), lambda i: (i, 0, 0)),
                pl.BlockSpec((2, 8, seq), lambda i: (i, 0, 0)),
                pl.BlockSpec((N_DEV, PACK, d_model), lambda i: (0, 0, 0)),
                pl.BlockSpec((8, 128), lambda i: (0, 0)),
                anywhere, anywhere,
            ],
            out_shape=[
                jax.ShapeDtypeStruct((groups, seq, d_model), BF16),
                jax.ShapeDtypeStruct((groups, 8, seq), F32),
                jax.ShapeDtypeStruct((N_DEV, PACK, d_model), BF16),
                jax.ShapeDtypeStruct((8, 128), jnp.int32),
                jax.ShapeDtypeStruct((e_loc, N_DEV * fix_rows, d_model), BF16),
                jax.ShapeDtypeStruct((N_DEV, 16, 128), F32),
            ],
            scratch_shapes=[
                pltpu.VMEM((hw, 2 * seq), BF16),
                pltpu.VMEM((2 * seq, hw), BF16),
                pltpu.VMEM((hw, 2 * seq), BF16),
                pltpu.VMEM((hw, 2 * seq), BF16),
                pltpu.VMEM((2, 4, seq, seq), F32),
                pltpu.VMEM((2, 4, seq, seq), BF16),
                pltpu.VMEM((3 * experts, d_model), BF16),
                pltpu.VMEM((4 * seq, d_model), BF16),
                pltpu.VMEM((8, 4 * seq), jnp.int32),
                pltpu.VMEM((4, experts, 128), F32),
                pltpu.VMEM((8, 128), F32),
                pltpu.VMEM((N_DEV, 128), F32),
                pltpu.VMEM((N_DEV, 128), F32),
                pltpu.VMEM((N_DEV, 256), F32),
                pltpu.VMEM((N_DEV, quads * LOCAL, d_model), BF16),
                pltpu.VMEM((quads, N_DEV, e_loc, FIX, d_model), BF16),
                pltpu.VMEM((N_DEV, 16, 128), F32),
                dma, dma, dma, dma, dma((2,)),
            ],
            compiler_params=pltpu.CompilerParams(
                dimension_semantics=("arbitrary",), collective_id=0, has_side_effects=True, vmem_limit_bytes=VMEM_LIMIT),
        )(tokens, pad_mask, second_draw, choices.transpose(0, 2, 1), norm_attn, wq, wk, wv, wo, norm_moe, w_gate)

        def packed_path():
            back, back_pack = pl.pallas_call(
                packed_expert_kernel,
                name="packed_experts",
                grid=(2 * e_loc,),
                in_specs=[
                    pl.BlockSpec((1, N_DEV * fix_rows, d_model), lambda i: (jnp.minimum(i, e_loc - 1), 0, 0)),
                    whole((N_DEV, PACK, d_model)), whole((N_DEV, 16, 128)),
                    pl.BlockSpec((1, d_model, ff), lambda i: (lax.rem(i, e_loc), 0, 0)),
                    pl.BlockSpec((1, ff, d_model), lambda i: (lax.rem(i, e_loc), 0, 0)),
                ],
                out_specs=[anywhere, anywhere],
                out_shape=[
                    jax.ShapeDtypeStruct((experts, fix_rows, d_model), BF16),
                    jax.ShapeDtypeStruct((N_DEV, PACK, d_model), BF16),
                ],
                scratch_shapes=[
                    pltpu.VMEM((N_DEV * fix_rows, ff), BF16),
                    pltpu.VMEM((e_loc, N_DEV // TEAM * POOL, d_model), BF16),
                    pltpu.VMEM((e_loc, N_DEV * fix_rows, d_model), BF16),
                    pltpu.VMEM((e_loc, N_DEV // TEAM * POOL, d_model), BF16),
                    pltpu.VMEM((N_DEV, 128), F32),
                    pltpu.VMEM((N_DEV, PACK, d_model), BF16),
                    pltpu.VMEM((N_DEV, PACK, d_model), BF16),
                    dma, dma, dma, dma, dma, dma, dma((3,)),
                ],
                compiler_params=pltpu.CompilerParams(
                    dimension_semantics=("arbitrary",), collective_id=1, has_side_effects=True, vmem_limit_bytes=VMEM_LIMIT),
            )(fix, mine, msg, w_in, w_out)
            return pl.pallas_call(
                functools.partial(packed_back_kernel, n_groups=groups * N_DEV),
                name="packed_back",
                grid_spec=pltpu.PrefetchScalarGridSpec(
                    num_scalar_prefetch=1,
                    grid=(steps,),
                    in_specs=[
                        pl.BlockSpec((experts, FIX, d_model), lambda i, starts: (0, i // 2, 0)),
                        pl.BlockSpec((N_DEV, PACK, d_model), lambda i, starts: (0, 0, 0), pipeline_mode=pl.Buffered(1)),
                        pl.BlockSpec((2, seq, d_model), lambda i, starts: (i, 0, 0)),
                        pl.BlockSpec((2, 8, seq), lambda i, starts: (i, 0, 0)),
                        pl.BlockSpec((N_DEV, 16, 128), lambda i, starts: (0, 0, 0), pipeline_mode=pl.Buffered(1)),
                    ],
                    out_specs=[
                        pl.BlockSpec((2, seq, d_model), lambda i, starts: (i, 0, 0)),
                        pl.BlockSpec(memory_space=pltpu.SMEM),
                    ],
                    scratch_shapes=[pltpu.VMEM((N_DEV * WINDOW, d_model), BF16)],
                ),
                out_shape=[
                    jax.ShapeDtypeStruct((groups, seq, d_model), BF16),
                    jax.ShapeDtypeStruct((1, 1), F32),
                ],
                compiler_params=pltpu.CompilerParams(dimension_semantics=("arbitrary",), vmem_limit_bytes=VMEM_LIMIT),
            )(starts, back, back_pack, hidden_p, meta_p, msg)

        def full_path():
            recv = pl.pallas_call(
                functools.partial(full_front_kernel, experts=experts, capacity=capacity),
                name="full_front",
                grid=(steps,),
                in_specs=[
                    pl.BlockSpec((2, seq, d_model), lambda i: (i, 0, 0)),
                    pl.BlockSpec((2, 8, seq), lambda i: (i, 0, 0)),
                    whole((d_model,)),
                ],
                out_specs=anywhere,
                out_shape=jax.ShapeDtypeStruct((e_loc, all_rows, d_model), BF16),
                scratch_shapes=[pltpu.VMEM((steps, N_DEV, e_loc, rows, d_model), BF16), dma, dma, dma],
                compiler_params=pltpu.CompilerParams(
                    dimension_semantics=("arbitrary",), collective_id=2, has_side_effects=True, vmem_limit_bytes=VMEM_LIMIT),
            )(hidden_p, meta_p, norm_moe)
            tile = all_rows // 4
            ret = pl.pallas_call(
                functools.partial(expert_kernel, tile=tile),
                name="full_experts",
                grid=(e_loc,),
                in_specs=[
                    pl.BlockSpec((1, all_rows, d_model), lambda i: (i, 0, 0)),
                    pl.BlockSpec((1, d_model, ff), lambda i: (i, 0, 0)),
                    pl.BlockSpec((1, ff, d_model), lambda i: (i, 0, 0)),
                ],
                out_specs=anywhere,
                out_shape=jax.ShapeDtypeStruct((experts, steps * rows, d_model), BF16),
                scratch_shapes=[pltpu.VMEM((tile, ff), BF16), pltpu.VMEM((e_loc, all_rows, d_model), BF16), dma, dma, dma],
                compiler_params=pltpu.CompilerParams(
                    dimension_semantics=("arbitrary",), collective_id=3, has_side_effects=True, vmem_limit_bytes=VMEM_LIMIT),
            )(recv, w_in, w_out)
            return pl.pallas_call(
                functools.partial(back_kernel, n_groups=groups * N_DEV, capacity=capacity),
                name="full_back",
                grid=(steps,),
                in_specs=[
                    pl.BlockSpec((experts, rows, d_model), lambda i: (0, i, 0)),
                    pl.BlockSpec((2, seq, d_model), lambda i: (i, 0, 0)),
                    pl.BlockSpec((2, 8, seq), lambda i: (i, 0, 0)),
                    whole((N_DEV, 16, 128)),
                ],
                out_specs=[
                    pl.BlockSpec((2, seq, d_model), lambda i: (i, 0, 0)),
                    pl.BlockSpec(memory_space=pltpu.SMEM),
                ],
                out_shape=[
                    jax.ShapeDtypeStruct((groups, seq, d_model), BF16),
                    jax.ShapeDtypeStruct((1, 1), F32),
                ],
                compiler_params=pltpu.CompilerParams(dimension_semantics=("arbitrary",), vmem_limit_bytes=VMEM_LIMIT),
            )(ret, hidden_p, meta_p, msg)

        shared = jnp.sum(msg[:, 10, :].reshape(N_DEV // TEAM, TEAM, experts), axis=1)
        spilled = (jnp.max(msg[:, 9, 0]) > 0.0) | (jnp.max(shared) > POOL)
        out, aux = lax.cond(spilled, full_path, packed_path)
        return out, aux.reshape(())

    by_group = P("ep")
    replicated = P()
    in_specs = (by_group, by_group, by_group, by_group, replicated, replicated, replicated, replicated, replicated, replicated, replicated, by_group, by_group)
    return jax.shard_map(local_step, mesh=mesh, in_specs=in_specs, out_specs=(by_group, replicated), check_vma=False)
```

```python
import functools
import jax
import jax.numpy as jnp
from jax import lax
from jax.experimental import pallas as pl
from jax.experimental.pallas import tpu as pltpu
from jax.sharding import PartitionSpec as P

NORM_EPS = 1e-6
N_DEV = 16
MESH = pl.DeviceIdType.MESH
F32 = jnp.float32
BF16 = jnp.bfloat16
ORDER = (0, 9, 2, 11, 4, 13, 6, 15, 8, 1, 10, 3, 12, 5, 14, 7)
VMEM_LIMIT = 62 * 1024 * 1024


def partner(me, mask):
    out = 0
    for bit in range(4):
        val = lax.rem(me // (1 << bit), 2)
        out = out + (1 << bit) * ((1 - val) if (mask >> bit) & 1 else val)
    return out


def greet(me):
    barrier = pltpu.get_barrier_semaphore()
    for mask in range(1, N_DEV):
        pl.semaphore_signal(barrier, inc=1, device_id=(partner(me, mask),), device_id_type=MESH)


def rms_norm(values_f, scale_vec):
    inv_rms = lax.rsqrt(jnp.mean(values_f * values_f, axis=-1, keepdims=True) + NORM_EPS)
    return (values_f * inv_rms * scale_vec).astype(BF16)


def dot(a, b):
    return jnp.dot(a, b, preferred_element_type=F32)


def dot_nt(a, b):
    return lax.dot_general(a, b, (((1,), (1,)), ((), ())), preferred_element_type=F32)


def split_gate(wgate_ref, wg_s):
    experts = wgate_ref.shape[1]
    wg = wgate_ref[...].T
    hi = wg.astype(BF16)
    rest = wg - hi.astype(F32)
    mid = rest.astype(BF16)
    low = (rest - mid.astype(F32)).astype(BF16)
    wg_s[0:experts] = hi
    wg_s[experts:2 * experts] = mid
    wg_s[2 * experts:3 * experts] = low


def attend(
    step, tokens_ref, pad_ref, norm_attn_ref, wq_ref, wk_ref, wv_ref, wo_ref, norm_moe_ref, hidden_ref,
    q_s, k_s, v_s, ctx_s, s_s, p_s, wg_s, heads, head_dim, experts,
):
    seq = tokens_ref.shape[1]
    d_model = tokens_ref.shape[2]
    x = tokens_ref[...].reshape(2 * seq, d_model)
    a = rms_norm(x.astype(F32), norm_attn_ref[...][None, :])
    q_s[...] = dot_nt(wq_ref[...], a).astype(BF16)
    k_s[...] = dot_nt(a, wk_ref[...]).astype(BF16)
    v_s[...] = dot_nt(wv_ref[...], a).astype(BF16)

    width = 2 * head_dim
    lane = lax.broadcasted_iota(jnp.int32, (1, width), 1)
    scale = head_dim ** -0.5
    sides = [jnp.where(lane < head_dim, scale, 0.0).astype(BF16), jnp.where(lane < head_dim, 0.0, scale).astype(BF16)]
    cut = seq // 2
    late_key = lax.broadcasted_iota(jnp.int32, (seq - cut, 128), 0) + cut
    batch = s_s.shape[1]
    lanes = 128
    buf = 0
    for grp in range(2):
        tok = pl.ds(grp * seq, seq)
        length = jnp.sum(pad_ref[pl.ds(2 * step + grp, 1), :], axis=1, keepdims=True)
        keep_late = late_key < length
        for first in range(0, heads, batch):
            for i in range(batch):
                off = (first + i) // 2 * width
                k = k_s[tok, pl.ds(off, width)] * sides[(first + i) % 2]
                s_s[buf, i] = dot(k, q_s[pl.ds(off, width), tok])
            for i in range(batch):
                for col in range(0, seq, lanes):
                    cols = pl.ds(col, lanes)
                    early = s_s[buf, i, pl.ds(0, cut), cols]
                    late = jnp.where(keep_late, s_s[buf, i, pl.ds(cut, seq - cut), cols], -1e30)
                    top = jnp.maximum(jnp.max(early, axis=0, keepdims=True), jnp.max(late, axis=0, keepdims=True))
                    early = jnp.exp(early - top)
                    late = jnp.exp(late - top)
                    inv = 1.0 / (jnp.sum(early, axis=0, keepdims=True) + jnp.sum(late, axis=0, keepdims=True))
                    p_s[buf, i, pl.ds(0, cut), cols] = (early * inv).astype(BF16)
                    p_s[buf, i, pl.ds(cut, seq - cut), cols] = (late * inv).astype(BF16)
            for i in range(batch):
                head = pl.ds((first + i) * head_dim, head_dim)
                ctx_s[head, tok] = dot(v_s[head, tok], p_s[buf, i]).astype(BF16)
            buf = 1 - buf

    attn = lax.dot_general(ctx_s[...], wo_ref[...], (((0,), (0,)), ((), ())), preferred_element_type=F32)
    hidden = (x.astype(F32) + attn).astype(BF16)
    hidden_ref[...] = hidden.reshape(2, seq, d_model)
    b = rms_norm(hidden.astype(F32), norm_moe_ref[...][None, :])
    lg = dot_nt(wg_s[...], b)
    logits = (lg[2 * experts:] + lg[experts:2 * experts]) + lg[:experts]
    ex = jnp.exp(logits - jnp.max(logits, axis=0, keepdims=True))
    return b, ex / jnp.sum(ex, axis=0, keepdims=True)


def full_front_kernel(hidden_ref, meta_ref, norm_moe_ref, recv_ref, send_s, send_sem, recv_sem, own_sem, *, experts, capacity):
    step = pl.program_id(0)
    steps = pl.num_programs(0)
    me = lax.axis_index("ep")
    seq = hidden_ref.shape[1]
    d_model = hidden_ref.shape[2]
    e_loc = experts // N_DEV
    half = e_loc // 2
    slots = experts * capacity
    rows = 2 * capacity
    per_src = steps * rows

    def send_pair(pair):
        for place, mask in enumerate(ORDER):
            dev = partner(me, mask)
            src = send_s.at[pair, dev]
            dst = recv_ref.at[:, pl.ds(pl.multiple_of(place * per_src + pair * rows, rows), rows), :]
            if mask == 0:
                pltpu.make_async_copy(src, dst, own_sem).start()
            else:
                pltpu.make_async_remote_copy(
                    src_ref=src, dst_ref=dst, send_sem=send_sem, recv_sem=recv_sem,
                    device_id=(dev,), device_id_type=MESH).start()

    @pl.when(step == 0)
    def _():
        greet(me)

    @pl.when(step == 1)
    def _():
        pl.semaphore_wait(pltpu.get_barrier_semaphore(), N_DEV - 1)

    @pl.when(step > 0)
    def _():
        send_pair(step - 1)

    slot_id = lax.broadcasted_iota(jnp.int32, (slots, seq), 0)
    picked = []
    for grp in range(2):
        b = rms_norm(hidden_ref[grp].astype(F32), norm_moe_ref[...][None, :])

        def place_of(code):
            e = code // capacity
            dev = e // e_loc
            r = e - dev * e_loc
            upper = r // half
            side = upper if grp == 0 else 1 - upper
            at = ((dev * half + r - upper * half) * 2 + side) * capacity + code - e * capacity
            return jnp.where(code >= 0, at, -1)

        d1 = place_of(meta_ref[grp, 4:5, :].astype(jnp.int32))
        d2 = place_of(meta_ref[grp, 5:6, :].astype(jnp.int32))
        disp_mat = jnp.where((slot_id == d1) | (slot_id == d2), 1.0, 0.0).astype(BF16)
        picked.append(dot(disp_mat, b).reshape(N_DEV * half, rows, d_model))

    top = lax.broadcasted_iota(jnp.int32, (1, rows, 1), 1) < capacity
    lower = jnp.where(top, picked[0], picked[1]).astype(BF16)
    upper = jnp.where(top, picked[1], picked[0]).astype(BF16)
    send_s[step, :, 0:half] = lower.reshape(N_DEV, half, rows, d_model)
    send_s[step, :, half:e_loc] = upper.reshape(N_DEV, half, rows, d_model)

    @pl.when(step == steps - 1)
    def _():
        send_pair(steps - 1)
        others = pl.ds(0, N_DEV - 1)
        pltpu.make_async_copy(send_s.at[:, others], send_s.at[:, others], send_sem).wait()
        pltpu.make_async_copy(send_s.at[:, 0], send_s.at[:, 0], own_sem).wait()
        arrived = recv_ref.at[:, pl.ds(0, (N_DEV - 1) * per_src), :]
        pltpu.make_async_copy(arrived, arrived, recv_sem).wait()


def expert_kernel(recv_ref, w_in_ref, w_out_ref, ret_ref, act_s, z_s, send_sem, recv_sem, local_sem, *, tile):
    e = pl.program_id(0)
    n_exp = pl.num_programs(0)
    me = lax.axis_index("ep")
    rows = recv_ref.shape[1]
    ff = w_in_ref.shape[2]
    per_src = rows // N_DEV
    n_tiles = rows // tile
    chunk = 1024

    @pl.when(e == 0)
    def _():
        greet(me)

    def run(t, carry):
        at = pl.ds(pl.multiple_of(t * tile, tile), tile)
        x = recv_ref[0, at, :]
        for f in range(ff // chunk):
            act = dot(x, w_in_ref[0, :, pl.ds(f * chunk, chunk)])
            act_s[:, pl.ds(f * chunk, chunk)] = jnp.maximum(act, 0.0).astype(BF16)
        z_s[e, at, :] = dot(act_s[...], w_out_ref[0]).astype(BF16)
        return carry

    lax.fori_loop(0, n_tiles, run, 0)

    @pl.when(e == 0)
    def _():
        pl.semaphore_wait(pltpu.get_barrier_semaphore(), N_DEV - 1)

    for place, mask in enumerate(ORDER):
        dev = partner(me, mask)
        src = z_s.at[e, pl.ds(place * per_src, per_src), :]
        dst = ret_ref.at[me * n_exp + e]
        if mask == 0:
            pltpu.make_async_copy(src, dst, local_sem).start()
        else:
            pltpu.make_async_remote_copy(
                src_ref=src, dst_ref=dst, send_sem=send_sem, recv_sem=recv_sem,
                device_id=(dev,), device_id_type=MESH).start()

    @pl.when(e == n_exp - 1)
    def _():
        sent = z_s.at[:, pl.ds(0, (N_DEV - 1) * per_src), :]
        pltpu.make_async_copy(sent, sent, send_sem).wait()
        own = z_s.at[:, pl.ds(0, per_src), :]
        pltpu.make_async_copy(own, own, local_sem).wait()
        arrived = ret_ref.at[pl.ds(0, (N_DEV - 1) * n_exp)]
        pltpu.make_async_copy(arrived, arrived, recv_sem).wait()


def back_kernel(ret_ref, hidden_ref, meta_ref, msg_ref, out_ref, aux_ref, *, n_groups, capacity):
    experts, rows, d_model = ret_ref.shape
    seq = hidden_ref.shape[1]
    z = ret_ref[...].reshape(experts * rows, d_model)
    slot_id = lax.broadcasted_iota(jnp.int32, (seq, experts * rows), 1)
    e_loc = experts // N_DEV
    for grp in range(2):
        meta = meta_ref[grp].T

        def place_of(code):
            e = code // capacity
            r = e - e // e_loc * e_loc
            upper = r // (e_loc // 2)
            side = upper if grp == 0 else 1 - upper
            return jnp.where(code >= 0, (e * 2 + side) * capacity + code - e * capacity, -1)

        c1 = place_of(meta[:, 4:5].astype(jnp.int32))
        c2 = place_of(meta[:, 5:6].astype(jnp.int32))
        comb = jnp.where(slot_id == c1, meta[:, 2:3], 0.0) + jnp.where(slot_id == c2, meta[:, 3:4], 0.0)
        moe = dot(comb.astype(BF16), z)
        out_ref[grp] = (hidden_ref[grp].astype(F32) + moe).astype(BF16)

    @pl.when(pl.program_id(0) == 0)
    def _():
        aux_ref[0, 0] = jnp.sum(msg_ref[:, 0:8, :]) * (experts / n_groups)


FIX = 8
LOCAL = 48
PACK = 104
EXTRA = 32
TEAM = 4
POOL = 80
WINDOW = 64


def twice(value):
    return jnp.concatenate([value, value], axis=1)


def packed_front_kernel(
    tokens_ref, pad_ref, draw_ref, choices_ref, norm_attn_ref, wq_ref, wk_ref, wv_ref, wo_ref, norm_moe_ref, wgate_ref,
    hidden_ref, meta_ref, pack_s, starts_ref, fix_ref, msg_ref,
    q_s, k_s, v_s, ctx_s, s_s, p_s, wg_s, b_s, slot_s, count_s, aux_s, flag_s, code_s, goal_s,
    local_s, fix_s, msg_s, fix_send, fix_recv, msg_send, msg_recv, own_sem,
    *, heads, head_dim, capacity,
):
    step = pl.program_id(0)
    steps = pl.num_programs(0)
    quad = step // 2
    quads = steps // 2
    me = lax.axis_index("ep")
    seq = tokens_ref.shape[1]
    d_model = tokens_ref.shape[2]
    experts = wgate_ref.shape[1]
    e_loc = experts // N_DEV

    def remote(src, dst, send_sem, recv_sem, dev, mask, own):
        if mask == 0:
            pltpu.make_async_copy(src, dst, own_sem.at[own]).start()
        else:
            pltpu.make_async_remote_copy(
                src_ref=src, dst_ref=dst, send_sem=send_sem, recv_sem=recv_sem,
                device_id=(dev,), device_id_type=MESH).start()

    def send_quad(which):
        for place, mask in enumerate(ORDER):
            dev = partner(me, mask)
            row = pl.multiple_of(place * quads * FIX + which * FIX, FIX)
            remote(fix_s.at[which, dev], fix_ref.at[:, pl.ds(row, FIX), :], fix_send, fix_recv, dev, mask, 0)

    @pl.when(step == 0)
    def _():
        greet(me)
        split_gate(wgate_ref, wg_s)
        aux_s[...] = jnp.zeros_like(aux_s)
        flag_s[...] = jnp.zeros_like(flag_s)
        code_s[...] = jnp.zeros_like(code_s)
        goal_s[...] = jnp.zeros_like(goal_s)
        count_s[...] = jnp.zeros_like(count_s)

    @pl.when(step == 2)
    def _():
        pl.semaphore_wait(pltpu.get_barrier_semaphore(), N_DEV - 1)

    @pl.when((step > 0) & (lax.rem(step, 2) == 0))
    def _():
        send_quad(quad - 1)

    b, gate_probs = attend(
        step, tokens_ref, pad_ref, norm_attn_ref, wq_ref, wk_ref, wv_ref, wo_ref, norm_moe_ref, hidden_ref,
        q_s, k_s, v_s, ctx_s, s_s, p_s, wg_s, heads, head_dim, experts)
    side = lax.rem(step, 2)
    b_s[pl.ds(pl.multiple_of(side * 2 * seq, 2 * seq), 2 * seq), :] = b

    eid = lax.broadcasted_iota(jnp.int32, (experts, seq), 0)
    tri = jnp.where(lax.broadcasted_iota(jnp.int32, (seq, seq), 0) <= lax.broadcasted_iota(jnp.int32, (seq, seq), 1), 1.0, 0.0)
    tri = jnp.concatenate([tri, jnp.ones((seq, 128), F32)], axis=1).astype(BF16)
    row_e = lax.broadcasted_iota(jnp.int32, (experts, experts), 0)
    col_e = lax.broadcasted_iota(jnp.int32, (experts, experts), 1)
    same = row_e // e_loc == col_e // e_loc
    mix = jnp.concatenate([jnp.where(same & (col_e < row_e), 1.0, 0.0), jnp.where(same, 1.0, 0.0)], axis=0).astype(BF16)
    spot = lax.broadcasted_iota(jnp.int32, (experts, 128), 1).astype(F32)
    code0 = (lax.rem(lax.broadcasted_iota(jnp.int32, (experts, 128), 0), e_loc) * EXTRA + 1).astype(F32)
    meta_row = lax.broadcasted_iota(jnp.int32, (8, seq), 0)

    def window_start():
        return jnp.minimum(jnp.floor(count_s[3] * (1.0 / 8)) * 8.0, float(PACK - WINDOW))

    for grp in range(2):
        p = gate_probs[:, grp * seq:(grp + 1) * seq]
        valid = pad_ref[pl.ds(2 * step + grp, 1), :] == 1
        draw = draw_ref[pl.ds(2 * step + grp, 1), :]
        e1 = choices_ref[grp, 0:1, :]
        e2 = choices_ref[grp, 1:2, :]
        hot1 = eid == e1
        hot2 = eid == e2
        p1 = jnp.sum(jnp.where(hot1, p, 0.0), axis=0, keepdims=True)
        p2 = jnp.sum(jnp.where(hot2, p, 0.0), axis=0, keepdims=True)
        g1 = p1 / (p1 + p2)
        g2 = p2 / (p1 + p2)
        want2 = valid & (draw < 2.0 * g2)
        take1 = jnp.where(hot1 & valid, 1.0, 0.0)
        take2 = jnp.where(hot2 & want2, 1.0, 0.0)
        cum = dot(jnp.concatenate([take1, take2], axis=0).astype(BF16), tri)
        cum1 = cum[:experts, :seq]
        cum2 = cum[experts:, :seq]
        count1 = cum[:experts, seq:]
        count2 = cum[experts:, seq:]
        first = jnp.minimum(count1, float(capacity))
        pos1 = jnp.sum((cum1 - 1.0) * take1, axis=0, keepdims=True)
        pos2 = jnp.sum((cum2 - 1.0 + twice(first)) * take2, axis=0, keepdims=True)
        keep1 = valid & (pos1 < capacity)
        keep2 = want2 & (pos2 < capacity)

        share = jnp.where(valid, p, 0.0) * twice(count1 * (1.0 / (seq * seq)))
        share = jnp.sum(share.reshape(experts // 8, 8, seq), axis=0)
        for col in range(seq // 128):
            aux_s[...] += share[:, col * 128:(col + 1) * 128]

        before = count_s[0]
        after = before + jnp.minimum(first + count2, float(capacity))
        new = jnp.maximum(after - FIX, 0.0) - jnp.maximum(before - FIX, 0.0)
        sums = dot(mix, new.astype(BF16))
        packed = count_s[1]
        begin = packed + sums[:experts]
        shift = begin - jnp.maximum(before, float(FIX)) + before
        local = shift - count_s[3]
        window = shift - window_start()
        inside = (spot >= begin) & (spot < begin + new)
        code = jnp.where(inside, code0 + count_s[2] + spot - begin, 0.0)
        code_s[...] += jnp.sum(code.reshape(N_DEV, e_loc, 128), axis=1)
        count_s[0] = after
        count_s[1] = packed + sums[experts:]
        count_s[2] += new

        def places(e, take, pos, keep):
            index = pos + jnp.sum(twice(before) * take, axis=0, keepdims=True)
            in_window = pos + jnp.sum(twice(window) * take, axis=0, keepdims=True)
            in_local = pos + jnp.sum(twice(local) * take, axis=0, keepdims=True)
            e = e.astype(F32)
            dev = jnp.floor(e * (1.0 / e_loc))
            fixed = keep & (index < FIX)
            loose = keep & (index >= FIX)
            at_fix = jnp.where(fixed, e * FIX + index, -1.0)
            at_local = jnp.where(loose, dev * LOCAL + in_local, -1.0)
            at_back = jnp.where(loose, experts * FIX + dev * WINDOW + in_window, at_fix)
            return at_fix, at_local, at_back, jnp.where(keep, e * capacity + pos, -1.0)

        f1, l1, c1, w1 = places(e1, take1, pos1, keep1)
        f2, l2, c2, w2 = places(e2, take2, pos2, keep2)
        meta = jnp.where(meta_row == 0, c1, 0.0)
        meta = jnp.where(meta_row == 1, c2, meta)
        meta = jnp.where(meta_row == 2, g1, meta)
        meta = jnp.where(meta_row == 3, g2, meta)
        meta = jnp.where(meta_row == 4, w1, meta)
        meta = jnp.where(meta_row == 5, w2, meta)
        meta_ref[grp] = meta
        tok = pl.ds(pl.multiple_of(side * 2 * seq + grp * seq, seq), seq)
        slot_s[:, tok] = jnp.where(meta_row == 0, f1, jnp.where(meta_row == 1, f2, jnp.where(meta_row == 2, l1, l2))).astype(jnp.int32)

    @pl.when(side == 1)
    def _():
        def gather(first_row, base, count, skip):
            ids = lax.broadcasted_iota(jnp.int32, (count, 4 * seq - skip), 0) + base
            hit = (ids == slot_s[first_row:first_row + 1, skip:]) | (ids == slot_s[first_row + 1:first_row + 2, skip:])
            return dot(jnp.where(hit, 1.0, 0.0).astype(BF16), b_s[skip:, :]).astype(BF16)

        per_dev = e_loc * FIX
        for base in range(0, N_DEV, 4):
            rows = gather(0, base * per_dev, 4 * per_dev, 0)
            fix_s[quad, base:base + 4] = rows.reshape(4, e_loc, FIX, d_model)
        for base in range(0, N_DEV, 4):
            rows = gather(2, base * LOCAL, 4 * LOCAL, 2 * seq)
            local_s[base:base + 4, pl.ds(pl.multiple_of(quad * LOCAL, LOCAL), LOCAL), :] = rows.reshape(4, LOCAL, d_model)

        def per_device(value):
            return value.reshape(N_DEV, e_loc, 128)[:, 0, :]

        start = per_device(count_s[3])
        filled = per_device(count_s[1]) - start
        at = lax.broadcasted_iota(jnp.int32, (N_DEV, 256), 1).astype(F32) - (quad * LOCAL).astype(F32)
        live = (at >= 0.0) & (at < float(LOCAL)) & (at < twice(filled))
        goal_s[...] = jnp.where(live, twice(start) + at + 1.0, goal_s[...])
        flag_s[...] = jnp.maximum(flag_s[...], jnp.where(filled > LOCAL, 1.0, 0.0))
        starts_ref[pl.ds(quad, 1), :] = window_start().T[0:1, :].astype(jnp.int32)
        count_s[0] = jnp.zeros_like(count_s[0])
        count_s[3] = count_s[1]

    @pl.when(step == steps - 1)
    def _():
        send_quad(quads - 1)
        over = jnp.where((count_s[1] > PACK) | (count_s[2] > EXTRA), 1.0, 0.0)
        over = jnp.max(jnp.max(over.reshape(N_DEV, e_loc, 128), axis=1), axis=0, keepdims=True)
        over = jnp.maximum(over, jnp.max(flag_s[...], axis=0, keepdims=True))
        tally = count_s[2].T[0:1, :]
        for dev in range(N_DEV):
            msg_s[dev, 0:8] = aux_s[...]
            lower = lax.broadcasted_iota(jnp.int32, (8, 128), 0)
            msg_s[dev, 8:16] = jnp.where(lower == 0, code_s[dev:dev + 1, :], jnp.where(lower == 1, over, jnp.where(lower == 2, tally, 0.0)))
        for place, mask in enumerate(ORDER):
            dev = partner(me, mask)
            remote(msg_s.at[dev], msg_ref.at[place], msg_send, msg_recv, dev, mask, 1)

        width = goal_s.shape[1] * 3 // 4
        rows = lax.broadcasted_iota(jnp.int32, (PACK, width), 0).astype(F32) + 1.0
        for dev in range(N_DEV):
            hit = jnp.where(rows == goal_s[dev:dev + 1, 0:width], 1.0, 0.0).astype(BF16)
            pack_s[dev] = dot(hit, local_s[dev]).astype(BF16)

        def settle(ref, sem):
            pltpu.make_async_copy(ref, ref, sem).wait()

        others = pl.ds(0, N_DEV - 1)
        settle(fix_s.at[:, 0], own_sem.at[0])
        settle(msg_s.at[0], own_sem.at[1])
        settle(fix_s.at[:, others], fix_send)
        settle(msg_s.at[others], msg_send)
        settle(fix_ref.at[:, pl.ds(0, (N_DEV - 1) * quads * FIX), :], fix_recv)
        settle(msg_ref.at[others], msg_recv)


def gate_rows(meta, count, base):
    cols = meta.T
    ids = lax.broadcasted_iota(jnp.int32, (cols.shape[0], count), 1) + base
    first = ids == cols[:, 0:1].astype(jnp.int32)
    second = ids == cols[:, 1:2].astype(jnp.int32)
    return jnp.where(first, cols[:, 2:3], jnp.where(second, cols[:, 3:4], 0.0)).astype(BF16)


def combine_fixed(fix_ref, hidden_ref, meta_ref, part_ref):
    experts, rows, d_model = fix_ref.shape
    z = fix_ref[...].reshape(experts * rows, d_model)
    for grp in range(2):
        part_ref[grp] = hidden_ref[grp].astype(F32) + dot(gate_rows(meta_ref[grp], experts * rows, 0), z)


def packed_expert_kernel(
    fix_ref, mine_ref, msg_ref, w_in_ref, w_out_ref, hidden_ref, meta_ref, back_ref, back_pack_ref, part_ref,
    act_s, x_s, z_s, zx_s, code_s, pack_ref, pack_s, in_send, in_recv, fix_send, fix_recv, pack_send, pack_recv, own_sem,
):
    step = pl.program_id(0)
    n_exp = pl.num_programs(0) // 2
    e = lax.rem(step, n_exp)
    me = lax.axis_index("ep")
    rows = fix_ref.shape[1]
    d_model = fix_ref.shape[2]
    ff = w_in_ref.shape[2]
    per_src = rows // N_DEV
    chunk = 1024

    def mlp(x):
        for f in range(ff // chunk):
            act = dot(x, w_in_ref[0, :, pl.ds(f * chunk, chunk)])
            act_s[0:x.shape[0], pl.ds(f * chunk, chunk)] = jnp.maximum(act, 0.0).astype(BF16)
        return dot(act_s[0:x.shape[0], :], w_out_ref[0]).astype(BF16)

    def spread(place):
        ids = lax.broadcasted_iota(jnp.int32, (x_s.shape[0] * POOL, PACK), 0).astype(F32) + 1.0
        return jnp.where(ids == code_s[place:place + 1, 0:PACK], 1.0, 0.0).astype(BF16)

    def remote(src, dst, send_sem, recv_sem, mask, own):
        if mask == 0:
            pltpu.make_async_copy(src, dst, own_sem.at[own]).start()
        else:
            pltpu.make_async_remote_copy(
                src_ref=src, dst_ref=dst, send_sem=send_sem, recv_sem=recv_sem,
                device_id=(partner(me, mask),), device_id_type=MESH).start()

    def settle(ref, sem):
        pltpu.make_async_copy(ref, ref, sem).wait()

    others = pl.ds(0, N_DEV - 1)

    @pl.when(step == 0)
    def _():
        greet(me)
        pl.semaphore_wait(pltpu.get_barrier_semaphore(), N_DEV - 1)
        for place, mask in enumerate(ORDER):
            remote(mine_ref.at[partner(me, mask)], pack_ref.at[place], in_send, in_recv, mask, 0)

    @pl.when(step < n_exp)
    def _():
        z_s[e] = mlp(fix_ref[0])
        for place, mask in enumerate(ORDER):
            remote(z_s.at[e, pl.ds(place * per_src, per_src), :], back_ref.at[me * n_exp + e], fix_send, fix_recv, mask, 1)

    @pl.when(step == n_exp)
    def _():
        settle(pack_ref.at[0], own_sem.at[0])
        settle(pack_ref.at[others], in_recv)
        code = jnp.concatenate([msg_ref[place, 8:9, :] for place in range(N_DEV)], axis=0)
        n_loc = x_s.shape[0]
        hits = [(code > ex * EXTRA) & (code <= (ex + 1) * EXTRA) for ex in range(n_loc)]
        row = lax.broadcasted_iota(jnp.int32, (N_DEV, N_DEV), 0)
        col = lax.broadcasted_iota(jnp.int32, (N_DEV, N_DEV), 1)
        prior = jnp.where((row // TEAM == col // TEAM) & (col < row), 1.0, 0.0).astype(BF16)
        spans = dot(prior, jnp.concatenate([jnp.where(hit, 1.0, 0.0) for hit in hits], axis=1).astype(BF16))
        shared = jnp.zeros_like(code)
        for ex, hit in enumerate(hits):
            begin = jnp.sum(spans[:, ex * 128:(ex + 1) * 128], axis=1, keepdims=True)
            shared = jnp.where(hit, code + begin + float(ex * (POOL - EXTRA)), shared)
        code_s[...] = shared
        for team in range(N_DEV // TEAM):
            x = dot(spread(team * TEAM), pack_ref[team * TEAM])
            for place in range(team * TEAM + 1, (team + 1) * TEAM):
                x = x + dot(spread(place), pack_ref[place])
            x_s[:, pl.ds(team * POOL, POOL), :] = x.astype(BF16).reshape(n_loc, POOL, d_model)

    @pl.when(step >= n_exp)
    def _():
        zx_s[e] = mlp(x_s[e])

    @pl.when(step == 2 * n_exp - 1)
    def _():
        for place, mask in enumerate(ORDER):
            z = zx_s[:, pl.ds(place // TEAM * POOL, POOL), :].reshape(x_s.shape[0] * POOL, d_model)
            pack_s[place] = lax.dot_general(
                spread(place), z, (((0,), (0,)), ((), ())), preferred_element_type=F32).astype(BF16)
            if place > 0:
                remote(pack_s.at[place - 1], back_pack_ref.at[me], pack_send, pack_recv, ORDER[place - 1], 2)
        remote(pack_s.at[N_DEV - 1], back_pack_ref.at[me], pack_send, pack_recv, ORDER[N_DEV - 1], 2)
        settle(z_s.at[:, pl.ds(0, per_src), :], own_sem.at[1])
        settle(back_ref.at[pl.ds(0, (N_DEV - 1) * n_exp)], fix_recv)
        groups, seq, _ = hidden_ref.shape
        experts = back_ref.shape[0]
        pltpu.emit_pipeline(
            combine_fixed,
            grid=(groups // 2,),
            in_specs=[
                pl.BlockSpec((experts, FIX, d_model), lambda i: (0, i // 2, 0)),
                pl.BlockSpec((2, seq, d_model), lambda i: (i, 0, 0)),
                pl.BlockSpec((2, 8, seq), lambda i: (i, 0, 0)),
            ],
            out_specs=[pl.BlockSpec((2, seq, d_model), lambda i: (i, 0, 0))],
        )(back_ref, hidden_ref, meta_ref, part_ref)
        settle(pack_s.at[0], own_sem.at[2])
        settle(mine_ref.at[others], in_send)
        settle(z_s.at[:, pl.ds(0, (N_DEV - 1) * per_src), :], fix_send)
        settle(pack_s.at[others], pack_send)
        settle(back_pack_ref.at[others], pack_recv)


def packed_back_kernel(starts_ref, pack_ref, part_ref, meta_ref, msg_ref, out_ref, aux_ref, window_s, *, n_groups, experts):
    seq = part_ref.shape[1]
    e_loc = experts // N_DEV
    step = pl.program_id(0)

    @pl.when(lax.rem(step, 2) == 0)
    def _():
        for dev in range(N_DEV):
            start = pl.multiple_of(starts_ref[step // 2, dev * e_loc], 8)
            window_s[dev * WINDOW:(dev + 1) * WINDOW, :] = pack_ref[dev, pl.ds(start, WINDOW), :]

    for grp in range(2):
        moe = dot(gate_rows(meta_ref[grp], N_DEV * WINDOW, experts * FIX), window_s[...])
        out_ref[grp] = (part_ref[grp] + moe).astype(BF16)

    @pl.when(step == 0)
    def _():
        aux_ref[0, 0] = jnp.sum(msg_ref[:, 0:8, :]) * (experts / n_groups)


def solution(mesh):
    def local_step(tokens, pad_mask, second_draw, choices, norm_attn, w_query, w_key, w_value, w_attn_out, norm_moe, w_gate, w_in, w_out):
        groups, seq, d_model = tokens.shape
        _, heads, head_dim = w_query.shape
        experts = w_gate.shape[1]
        ff = w_in.shape[2]
        e_loc = experts // N_DEV
        capacity = (2 * seq + experts - 1) // experts
        hw = heads * head_dim
        rows = 2 * capacity
        steps = groups // 2
        all_rows = N_DEV * steps * rows

        wq, wk, wv = (w.transpose(1, 2, 0).reshape(hw, d_model) for w in (w_query, w_key, w_value))
        wo = w_attn_out.reshape(hw, d_model)

        def whole(shape):
            return pl.BlockSpec(shape, lambda i: (0,) * len(shape), pipeline_mode=pl.Buffered(1))

        anywhere = pl.BlockSpec(memory_space=pl.ANY)
        front_specs = [
            pl.BlockSpec((2, seq, d_model), lambda i: (i, 0, 0)),
            whole((groups, seq)), whole((groups, seq)),
            pl.BlockSpec((2, 2, seq), lambda i: (i, 0, 0)),
            whole((d_model,)), whole((hw, d_model)), whole((hw, d_model)), whole((hw, d_model)), whole((hw, d_model)),
            whole((d_model,)), whole((d_model, experts)),
        ]
        quads = steps // 2
        fix_rows = quads * FIX
        dma = pltpu.SemaphoreType.DMA
        hidden_p, meta_p, mine, starts, fix, msg = pl.pallas_call(
            functools.partial(packed_front_kernel, heads=heads, head_dim=head_dim, capacity=capacity),
            name="packed_front",
            grid=(steps,),
            in_specs=front_specs,
            out_specs=[
                pl.BlockSpec((2, seq, d_model), lambda i: (i, 0, 0)),
                pl.BlockSpec((2, 8, seq), lambda i: (i, 0, 0)),
                pl.BlockSpec((N_DEV, PACK, d_model), lambda i: (0, 0, 0)),
                pl.BlockSpec((8, 128), lambda i: (0, 0)),
                anywhere, anywhere,
            ],
            out_shape=[
                jax.ShapeDtypeStruct((groups, seq, d_model), BF16),
                jax.ShapeDtypeStruct((groups, 8, seq), F32),
                jax.ShapeDtypeStruct((N_DEV, PACK, d_model), BF16),
                jax.ShapeDtypeStruct((8, 128), jnp.int32),
                jax.ShapeDtypeStruct((e_loc, N_DEV * fix_rows, d_model), BF16),
                jax.ShapeDtypeStruct((N_DEV, 16, 128), F32),
            ],
            scratch_shapes=[
                pltpu.VMEM((hw, 2 * seq), BF16),
                pltpu.VMEM((2 * seq, hw), BF16),
                pltpu.VMEM((hw, 2 * seq), BF16),
                pltpu.VMEM((hw, 2 * seq), BF16),
                pltpu.VMEM((2, 4, seq, seq), F32),
                pltpu.VMEM((2, 4, seq, seq), BF16),
                pltpu.VMEM((3 * experts, d_model), BF16),
                pltpu.VMEM((4 * seq, d_model), BF16),
                pltpu.VMEM((8, 4 * seq), jnp.int32),
                pltpu.VMEM((4, experts, 128), F32),
                pltpu.VMEM((8, 128), F32),
                pltpu.VMEM((N_DEV, 128), F32),
                pltpu.VMEM((N_DEV, 128), F32),
                pltpu.VMEM((N_DEV, 256), F32),
                pltpu.VMEM((N_DEV, quads * LOCAL, d_model), BF16),
                pltpu.VMEM((quads, N_DEV, e_loc, FIX, d_model), BF16),
                pltpu.VMEM((N_DEV, 16, 128), F32),
                dma, dma, dma, dma, dma((2,)),
            ],
            compiler_params=pltpu.CompilerParams(
                dimension_semantics=("arbitrary",), collective_id=0, has_side_effects=True, vmem_limit_bytes=VMEM_LIMIT),
        )(tokens, pad_mask, second_draw, choices.transpose(0, 2, 1), norm_attn, wq, wk, wv, wo, norm_moe, w_gate)

        def packed_path():
            back, back_pack, part = pl.pallas_call(
                packed_expert_kernel,
                name="packed_experts",
                grid=(2 * e_loc,),
                in_specs=[
                    pl.BlockSpec((1, N_DEV * fix_rows, d_model), lambda i: (jnp.minimum(i, e_loc - 1), 0, 0)),
                    whole((N_DEV, PACK, d_model)), whole((N_DEV, 16, 128)),
                    pl.BlockSpec((1, d_model, ff), lambda i: (lax.rem(i, e_loc), 0, 0)),
                    pl.BlockSpec((1, ff, d_model), lambda i: (lax.rem(i, e_loc), 0, 0)),
                    anywhere, anywhere,
                ],
                out_specs=[anywhere, anywhere, anywhere],
                out_shape=[
                    jax.ShapeDtypeStruct((experts, fix_rows, d_model), BF16),
                    jax.ShapeDtypeStruct((N_DEV, PACK, d_model), BF16),
                    jax.ShapeDtypeStruct((groups, seq, d_model), F32),
                ],
                scratch_shapes=[
                    pltpu.VMEM((N_DEV * fix_rows, ff), BF16),
                    pltpu.VMEM((e_loc, N_DEV // TEAM * POOL, d_model), BF16),
                    pltpu.VMEM((e_loc, N_DEV * fix_rows, d_model), BF16),
                    pltpu.VMEM((e_loc, N_DEV // TEAM * POOL, d_model), BF16),
                    pltpu.VMEM((N_DEV, 128), F32),
                    pltpu.VMEM((N_DEV, PACK, d_model), BF16),
                    pltpu.VMEM((N_DEV, PACK, d_model), BF16),
                    dma, dma, dma, dma, dma, dma, dma((3,)),
                ],
                compiler_params=pltpu.CompilerParams(
                    dimension_semantics=("arbitrary",), collective_id=1, has_side_effects=True, vmem_limit_bytes=VMEM_LIMIT),
            )(fix, mine, msg, w_in, w_out, hidden_p, meta_p)
            return pl.pallas_call(
                functools.partial(packed_back_kernel, n_groups=groups * N_DEV, experts=experts),
                name="packed_back",
                grid_spec=pltpu.PrefetchScalarGridSpec(
                    num_scalar_prefetch=1,
                    grid=(steps,),
                    in_specs=[
                        pl.BlockSpec((N_DEV, PACK, d_model), lambda i, starts: (0, 0, 0), pipeline_mode=pl.Buffered(1)),
                        pl.BlockSpec((2, seq, d_model), lambda i, starts: (i, 0, 0)),
                        pl.BlockSpec((2, 8, seq), lambda i, starts: (i, 0, 0)),
                        pl.BlockSpec((N_DEV, 16, 128), lambda i, starts: (0, 0, 0), pipeline_mode=pl.Buffered(1)),
                    ],
                    out_specs=[
                        pl.BlockSpec((2, seq, d_model), lambda i, starts: (i, 0, 0)),
                        pl.BlockSpec(memory_space=pltpu.SMEM),
                    ],
                    scratch_shapes=[pltpu.VMEM((N_DEV * WINDOW, d_model), BF16)],
                ),
                out_shape=[
                    jax.ShapeDtypeStruct((groups, seq, d_model), BF16),
                    jax.ShapeDtypeStruct((1, 1), F32),
                ],
                compiler_params=pltpu.CompilerParams(dimension_semantics=("arbitrary",), vmem_limit_bytes=VMEM_LIMIT),
            )(starts, back_pack, part, meta_p, msg)

        def full_path():
            recv = pl.pallas_call(
                functools.partial(full_front_kernel, experts=experts, capacity=capacity),
                name="full_front",
                grid=(steps,),
                in_specs=[
                    pl.BlockSpec((2, seq, d_model), lambda i: (i, 0, 0)),
                    pl.BlockSpec((2, 8, seq), lambda i: (i, 0, 0)),
                    whole((d_model,)),
                ],
                out_specs=anywhere,
                out_shape=jax.ShapeDtypeStruct((e_loc, all_rows, d_model), BF16),
                scratch_shapes=[pltpu.VMEM((steps, N_DEV, e_loc, rows, d_model), BF16), dma, dma, dma],
                compiler_params=pltpu.CompilerParams(
                    dimension_semantics=("arbitrary",), collective_id=2, has_side_effects=True, vmem_limit_bytes=VMEM_LIMIT),
            )(hidden_p, meta_p, norm_moe)
            tile = all_rows // 4
            ret = pl.pallas_call(
                functools.partial(expert_kernel, tile=tile),
                name="full_experts",
                grid=(e_loc,),
                in_specs=[
                    pl.BlockSpec((1, all_rows, d_model), lambda i: (i, 0, 0)),
                    pl.BlockSpec((1, d_model, ff), lambda i: (i, 0, 0)),
                    pl.BlockSpec((1, ff, d_model), lambda i: (i, 0, 0)),
                ],
                out_specs=anywhere,
                out_shape=jax.ShapeDtypeStruct((experts, steps * rows, d_model), BF16),
                scratch_shapes=[pltpu.VMEM((tile, ff), BF16), pltpu.VMEM((e_loc, all_rows, d_model), BF16), dma, dma, dma],
                compiler_params=pltpu.CompilerParams(
                    dimension_semantics=("arbitrary",), collective_id=3, has_side_effects=True, vmem_limit_bytes=VMEM_LIMIT),
            )(recv, w_in, w_out)
            return pl.pallas_call(
                functools.partial(back_kernel, n_groups=groups * N_DEV, capacity=capacity),
                name="full_back",
                grid=(steps,),
                in_specs=[
                    pl.BlockSpec((experts, rows, d_model), lambda i: (0, i, 0)),
                    pl.BlockSpec((2, seq, d_model), lambda i: (i, 0, 0)),
                    pl.BlockSpec((2, 8, seq), lambda i: (i, 0, 0)),
                    whole((N_DEV, 16, 128)),
                ],
                out_specs=[
                    pl.BlockSpec((2, seq, d_model), lambda i: (i, 0, 0)),
                    pl.BlockSpec(memory_space=pltpu.SMEM),
                ],
                out_shape=[
                    jax.ShapeDtypeStruct((groups, seq, d_model), BF16),
                    jax.ShapeDtypeStruct((1, 1), F32),
                ],
                compiler_params=pltpu.CompilerParams(dimension_semantics=("arbitrary",), vmem_limit_bytes=VMEM_LIMIT),
            )(ret, hidden_p, meta_p, msg)

        shared = jnp.sum(msg[:, 10, :].reshape(N_DEV // TEAM, TEAM, experts), axis=1)
        spilled = (jnp.max(msg[:, 9, 0]) > 0.0) | (jnp.max(shared) > POOL)
        out, aux = lax.cond(spilled, full_path, packed_path)
        return out, aux.reshape(())

    by_group = P("ep")
    replicated = P()
    in_specs = (by_group, by_group, by_group, by_group, replicated, replicated, replicated, replicated, replicated, replicated, replicated, by_group, by_group)
    return jax.shard_map(local_step, mesh=mesh, in_specs=in_specs, out_specs=(by_group, replicated), check_vma=False)
```

```python
import functools
import jax
import jax.numpy as jnp
from jax import lax
from jax.experimental import pallas as pl
from jax.experimental.pallas import tpu as pltpu
from jax.sharding import PartitionSpec as P

NORM_EPS = 1e-6
N_DEV = 16
MESH = pl.DeviceIdType.MESH
F32 = jnp.float32
BF16 = jnp.bfloat16
ORDER = (0, 9, 2, 11, 4, 13, 6, 15, 8, 1, 10, 3, 12, 5, 14, 7)
VMEM_LIMIT = 62 * 1024 * 1024


def partner(me, mask):
    out = 0
    for bit in range(4):
        val = lax.rem(me // (1 << bit), 2)
        out = out + (1 << bit) * ((1 - val) if (mask >> bit) & 1 else val)
    return out


def greet(me):
    barrier = pltpu.get_barrier_semaphore()
    for mask in range(1, N_DEV):
        pl.semaphore_signal(barrier, inc=1, device_id=(partner(me, mask),), device_id_type=MESH)


def rms_norm(values_f, scale_vec):
    inv_rms = lax.rsqrt(jnp.mean(values_f * values_f, axis=-1, keepdims=True) + NORM_EPS)
    return (values_f * inv_rms * scale_vec).astype(BF16)


def dot(a, b):
    return jnp.dot(a, b, preferred_element_type=F32)


def dot_nt(a, b):
    return lax.dot_general(a, b, (((1,), (1,)), ((), ())), preferred_element_type=F32)


def split_gate(wgate_ref, wg_s):
    experts = wgate_ref.shape[1]
    wg = wgate_ref[...].T
    hi = wg.astype(BF16)
    rest = wg - hi.astype(F32)
    mid = rest.astype(BF16)
    low = (rest - mid.astype(F32)).astype(BF16)
    wg_s[0:experts] = hi
    wg_s[experts:2 * experts] = mid
    wg_s[2 * experts:3 * experts] = low


def attend(
    step, tokens_ref, pad_ref, norm_attn_ref, wq_ref, wk_ref, wv_ref, wo_ref, norm_moe_ref, hidden_ref,
    q_s, k_s, v_s, ctx_s, s_s, p_s, wg_s, heads, head_dim, experts,
):
    seq = tokens_ref.shape[1]
    d_model = tokens_ref.shape[2]
    x = tokens_ref[...].reshape(2 * seq, d_model)
    a = rms_norm(x.astype(F32), norm_attn_ref[...][None, :])
    q_s[...] = dot_nt(wq_ref[...], a).astype(BF16)
    k_s[...] = dot_nt(a, wk_ref[...]).astype(BF16)
    v_s[...] = dot_nt(wv_ref[...], a).astype(BF16)

    width = 2 * head_dim
    lane = lax.broadcasted_iota(jnp.int32, (1, width), 1)
    scale = head_dim ** -0.5
    sides = [jnp.where(lane < head_dim, scale, 0.0).astype(BF16), jnp.where(lane < head_dim, 0.0, scale).astype(BF16)]
    cut = seq // 2
    late_key = lax.broadcasted_iota(jnp.int32, (seq - cut, 128), 0) + cut
    batch = s_s.shape[1]
    lanes = 128
    buf = 0
    for grp in range(2):
        tok = pl.ds(grp * seq, seq)
        length = jnp.sum(pad_ref[pl.ds(2 * step + grp, 1), :], axis=1, keepdims=True)
        keep_late = late_key < length
        for first in range(0, heads, batch):
            for i in range(batch):
                off = (first + i) // 2 * width
                k = k_s[tok, pl.ds(off, width)] * sides[(first + i) % 2]
                s_s[buf, i] = dot(k, q_s[pl.ds(off, width), tok])
            for i in range(batch):
                for col in range(0, seq, lanes):
                    cols = pl.ds(col, lanes)
                    early = s_s[buf, i, pl.ds(0, cut), cols]
                    late = jnp.where(keep_late, s_s[buf, i, pl.ds(cut, seq - cut), cols], -1e30)
                    top = jnp.maximum(jnp.max(early, axis=0, keepdims=True), jnp.max(late, axis=0, keepdims=True))
                    early = jnp.exp(early - top)
                    late = jnp.exp(late - top)
                    inv = 1.0 / (jnp.sum(early, axis=0, keepdims=True) + jnp.sum(late, axis=0, keepdims=True))
                    p_s[buf, i, pl.ds(0, cut), cols] = (early * inv).astype(BF16)
                    p_s[buf, i, pl.ds(cut, seq - cut), cols] = (late * inv).astype(BF16)
            for i in range(batch):
                head = pl.ds((first + i) * head_dim, head_dim)
                ctx_s[head, tok] = dot(v_s[head, tok], p_s[buf, i]).astype(BF16)
            buf = 1 - buf

    attn = lax.dot_general(ctx_s[...], wo_ref[...], (((0,), (0,)), ((), ())), preferred_element_type=F32)
    hidden = (x.astype(F32) + attn).astype(BF16)
    hidden_ref[...] = hidden.reshape(2, seq, d_model)
    b = rms_norm(hidden.astype(F32), norm_moe_ref[...][None, :])
    lg = dot_nt(wg_s[...], b)
    logits = (lg[2 * experts:] + lg[experts:2 * experts]) + lg[:experts]
    ex = jnp.exp(logits - jnp.max(logits, axis=0, keepdims=True))
    return b, ex / jnp.sum(ex, axis=0, keepdims=True)


def full_front_kernel(hidden_ref, meta_ref, norm_moe_ref, recv_ref, send_s, send_sem, recv_sem, own_sem, *, experts, capacity):
    step = pl.program_id(0)
    steps = pl.num_programs(0)
    me = lax.axis_index("ep")
    seq = hidden_ref.shape[1]
    d_model = hidden_ref.shape[2]
    e_loc = experts // N_DEV
    half = e_loc // 2
    slots = experts * capacity
    rows = 2 * capacity
    per_src = steps * rows

    def send_pair(pair):
        for place, mask in enumerate(ORDER):
            dev = partner(me, mask)
            src = send_s.at[pair, dev]
            dst = recv_ref.at[:, pl.ds(pl.multiple_of(place * per_src + pair * rows, rows), rows), :]
            if mask == 0:
                pltpu.make_async_copy(src, dst, own_sem).start()
            else:
                pltpu.make_async_remote_copy(
                    src_ref=src, dst_ref=dst, send_sem=send_sem, recv_sem=recv_sem,
                    device_id=(dev,), device_id_type=MESH).start()

    @pl.when(step == 0)
    def _():
        greet(me)

    @pl.when(step == 1)
    def _():
        pl.semaphore_wait(pltpu.get_barrier_semaphore(), N_DEV - 1)

    @pl.when(step > 0)
    def _():
        send_pair(step - 1)

    slot_id = lax.broadcasted_iota(jnp.int32, (slots, seq), 0)
    picked = []
    for grp in range(2):
        b = rms_norm(hidden_ref[grp].astype(F32), norm_moe_ref[...][None, :])

        def place_of(code):
            e = code // capacity
            dev = e // e_loc
            r = e - dev * e_loc
            upper = r // half
            side = upper if grp == 0 else 1 - upper
            at = ((dev * half + r - upper * half) * 2 + side) * capacity + code - e * capacity
            return jnp.where(code >= 0, at, -1)

        d1 = place_of(meta_ref[grp, 4:5, :].astype(jnp.int32))
        d2 = place_of(meta_ref[grp, 5:6, :].astype(jnp.int32))
        disp_mat = jnp.where((slot_id == d1) | (slot_id == d2), 1.0, 0.0).astype(BF16)
        picked.append(dot(disp_mat, b).reshape(N_DEV * half, rows, d_model))

    top = lax.broadcasted_iota(jnp.int32, (1, rows, 1), 1) < capacity
    lower = jnp.where(top, picked[0], picked[1]).astype(BF16)
    upper = jnp.where(top, picked[1], picked[0]).astype(BF16)
    send_s[step, :, 0:half] = lower.reshape(N_DEV, half, rows, d_model)
    send_s[step, :, half:e_loc] = upper.reshape(N_DEV, half, rows, d_model)

    @pl.when(step == steps - 1)
    def _():
        send_pair(steps - 1)
        others = pl.ds(0, N_DEV - 1)
        pltpu.make_async_copy(send_s.at[:, others], send_s.at[:, others], send_sem).wait()
        pltpu.make_async_copy(send_s.at[:, 0], send_s.at[:, 0], own_sem).wait()
        arrived = recv_ref.at[:, pl.ds(0, (N_DEV - 1) * per_src), :]
        pltpu.make_async_copy(arrived, arrived, recv_sem).wait()


def expert_kernel(recv_ref, w_in_ref, w_out_ref, ret_ref, act_s, z_s, send_sem, recv_sem, local_sem, *, tile):
    e = pl.program_id(0)
    n_exp = pl.num_programs(0)
    me = lax.axis_index("ep")
    rows = recv_ref.shape[1]
    ff = w_in_ref.shape[2]
    per_src = rows // N_DEV
    n_tiles = rows // tile
    chunk = 1024

    @pl.when(e == 0)
    def _():
        greet(me)

    def run(t, carry):
        at = pl.ds(pl.multiple_of(t * tile, tile), tile)
        x = recv_ref[0, at, :]
        for f in range(ff // chunk):
            act = dot(x, w_in_ref[0, :, pl.ds(f * chunk, chunk)])
            act_s[:, pl.ds(f * chunk, chunk)] = jnp.maximum(act, 0.0).astype(BF16)
        z_s[e, at, :] = dot(act_s[...], w_out_ref[0]).astype(BF16)
        return carry

    lax.fori_loop(0, n_tiles, run, 0)

    @pl.when(e == 0)
    def _():
        pl.semaphore_wait(pltpu.get_barrier_semaphore(), N_DEV - 1)

    for place, mask in enumerate(ORDER):
        dev = partner(me, mask)
        src = z_s.at[e, pl.ds(place * per_src, per_src), :]
        dst = ret_ref.at[me * n_exp + e]
        if mask == 0:
            pltpu.make_async_copy(src, dst, local_sem).start()
        else:
            pltpu.make_async_remote_copy(
                src_ref=src, dst_ref=dst, send_sem=send_sem, recv_sem=recv_sem,
                device_id=(dev,), device_id_type=MESH).start()

    @pl.when(e == n_exp - 1)
    def _():
        sent = z_s.at[:, pl.ds(0, (N_DEV - 1) * per_src), :]
        pltpu.make_async_copy(sent, sent, send_sem).wait()
        own = z_s.at[:, pl.ds(0, per_src), :]
        pltpu.make_async_copy(own, own, local_sem).wait()
        arrived = ret_ref.at[pl.ds(0, (N_DEV - 1) * n_exp)]
        pltpu.make_async_copy(arrived, arrived, recv_sem).wait()


def back_kernel(ret_ref, hidden_ref, meta_ref, msg_ref, out_ref, aux_ref, *, n_groups, capacity):
    experts, rows, d_model = ret_ref.shape
    seq = hidden_ref.shape[1]
    z = ret_ref[...].reshape(experts * rows, d_model)
    slot_id = lax.broadcasted_iota(jnp.int32, (seq, experts * rows), 1)
    e_loc = experts // N_DEV
    for grp in range(2):
        meta = meta_ref[grp].T

        def place_of(code):
            e = code // capacity
            r = e - e // e_loc * e_loc
            upper = r // (e_loc // 2)
            side = upper if grp == 0 else 1 - upper
            return jnp.where(code >= 0, (e * 2 + side) * capacity + code - e * capacity, -1)

        c1 = place_of(meta[:, 4:5].astype(jnp.int32))
        c2 = place_of(meta[:, 5:6].astype(jnp.int32))
        comb = jnp.where(slot_id == c1, meta[:, 2:3], 0.0) + jnp.where(slot_id == c2, meta[:, 3:4], 0.0)
        moe = dot(comb.astype(BF16), z)
        out_ref[grp] = (hidden_ref[grp].astype(F32) + moe).astype(BF16)

    @pl.when(pl.program_id(0) == 0)
    def _():
        aux_ref[0, 0] = jnp.sum(msg_ref[:, 0:8, :]) * (experts / n_groups)


FIX = 8
LOCAL = 48
PACK = 104
EXTRA = 32
TEAM = 4
POOL = 80
WINDOW = 64


def twice(value):
    return jnp.concatenate([value, value], axis=1)


def packed_front_kernel(
    tokens_ref, pad_ref, draw_ref, choices_ref, norm_attn_ref, wq_ref, wk_ref, wv_ref, wo_ref, norm_moe_ref, wgate_ref,
    hidden_ref, meta_ref, pack_s, starts_ref, fix_ref, msg_ref,
    q_s, k_s, v_s, ctx_s, s_s, p_s, wg_s, b_s, slot_s, count_s, aux_s, flag_s, code_s, goal_s,
    local_s, fix_s, msg_s, fix_send, fix_recv, msg_send, msg_recv, own_sem,
    *, heads, head_dim, capacity,
):
    step = pl.program_id(0)
    steps = pl.num_programs(0)
    quad = step // 2
    quads = steps // 2
    me = lax.axis_index("ep")
    seq = tokens_ref.shape[1]
    d_model = tokens_ref.shape[2]
    experts = wgate_ref.shape[1]
    e_loc = experts // N_DEV

    def remote(src, dst, send_sem, recv_sem, dev, mask, own):
        if mask == 0:
            pltpu.make_async_copy(src, dst, own_sem.at[own]).start()
        else:
            pltpu.make_async_remote_copy(
                src_ref=src, dst_ref=dst, send_sem=send_sem, recv_sem=recv_sem,
                device_id=(dev,), device_id_type=MESH).start()

    def send_quad(which):
        for place, mask in enumerate(ORDER):
            dev = partner(me, mask)
            row = pl.multiple_of(place * quads * FIX + which * FIX, FIX)
            remote(fix_s.at[which, dev], fix_ref.at[:, pl.ds(row, FIX), :], fix_send, fix_recv, dev, mask, 0)

    @pl.when(step == 0)
    def _():
        greet(me)
        split_gate(wgate_ref, wg_s)
        aux_s[...] = jnp.zeros_like(aux_s)
        flag_s[...] = jnp.zeros_like(flag_s)
        code_s[...] = jnp.zeros_like(code_s)
        goal_s[...] = jnp.zeros_like(goal_s)
        count_s[...] = jnp.zeros_like(count_s)

    @pl.when(step == 2)
    def _():
        pl.semaphore_wait(pltpu.get_barrier_semaphore(), N_DEV - 1)

    @pl.when((step > 0) & (lax.rem(step, 2) == 0))
    def _():
        send_quad(quad - 1)

    b, gate_probs = attend(
        step, tokens_ref, pad_ref, norm_attn_ref, wq_ref, wk_ref, wv_ref, wo_ref, norm_moe_ref, hidden_ref,
        q_s, k_s, v_s, ctx_s, s_s, p_s, wg_s, heads, head_dim, experts)
    side = lax.rem(step, 2)
    b_s[pl.ds(pl.multiple_of(side * 2 * seq, 2 * seq), 2 * seq), :] = b

    eid = lax.broadcasted_iota(jnp.int32, (experts, seq), 0)
    tri = jnp.where(lax.broadcasted_iota(jnp.int32, (seq, seq), 0) <= lax.broadcasted_iota(jnp.int32, (seq, seq), 1), 1.0, 0.0)
    tri = jnp.concatenate([tri, jnp.ones((seq, 128), F32)], axis=1).astype(BF16)
    row_e = lax.broadcasted_iota(jnp.int32, (experts, experts), 0)
    col_e = lax.broadcasted_iota(jnp.int32, (experts, experts), 1)
    same = row_e // e_loc == col_e // e_loc
    mix = jnp.concatenate([jnp.where(same & (col_e < row_e), 1.0, 0.0), jnp.where(same, 1.0, 0.0)], axis=0).astype(BF16)
    spot = lax.broadcasted_iota(jnp.int32, (experts, 128), 1).astype(F32)
    code0 = (lax.rem(lax.broadcasted_iota(jnp.int32, (experts, 128), 0), e_loc) * EXTRA + 1).astype(F32)
    meta_row = lax.broadcasted_iota(jnp.int32, (8, seq), 0)

    def window_start():
        return jnp.minimum(jnp.floor(count_s[3] * (1.0 / 8)) * 8.0, float(PACK - WINDOW))

    for grp in range(2):
        p = gate_probs[:, grp * seq:(grp + 1) * seq]
        valid = pad_ref[pl.ds(2 * step + grp, 1), :] == 1
        draw = draw_ref[pl.ds(2 * step + grp, 1), :]
        e1 = choices_ref[grp, 0:1, :]
        e2 = choices_ref[grp, 1:2, :]
        hot1 = eid == e1
        hot2 = eid == e2
        p1 = jnp.sum(jnp.where(hot1, p, 0.0), axis=0, keepdims=True)
        p2 = jnp.sum(jnp.where(hot2, p, 0.0), axis=0, keepdims=True)
        g1 = p1 / (p1 + p2)
        g2 = p2 / (p1 + p2)
        want2 = valid & (draw < 2.0 * g2)
        take1 = jnp.where(hot1 & valid, 1.0, 0.0)
        take2 = jnp.where(hot2 & want2, 1.0, 0.0)
        cum = dot(jnp.concatenate([take1, take2], axis=0).astype(BF16), tri)
        cum1 = cum[:experts, :seq]
        cum2 = cum[experts:, :seq]
        count1 = cum[:experts, seq:]
        count2 = cum[experts:, seq:]
        first = jnp.minimum(count1, float(capacity))
        pos1 = jnp.sum((cum1 - 1.0) * take1, axis=0, keepdims=True)
        pos2 = jnp.sum((cum2 - 1.0 + twice(first)) * take2, axis=0, keepdims=True)
        keep1 = valid & (pos1 < capacity)
        keep2 = want2 & (pos2 < capacity)

        share = jnp.where(valid, p, 0.0) * twice(count1 * (1.0 / (seq * seq)))
        share = jnp.sum(share.reshape(experts // 8, 8, seq), axis=0)
        for col in range(seq // 128):
            aux_s[...] += share[:, col * 128:(col + 1) * 128]

        before = count_s[0]
        after = before + jnp.minimum(first + count2, float(capacity))
        new = jnp.maximum(after - FIX, 0.0) - jnp.maximum(before - FIX, 0.0)
        sums = dot(mix, new.astype(BF16))
        packed = count_s[1]
        begin = packed + sums[:experts]
        shift = begin - jnp.maximum(before, float(FIX)) + before
        local = shift - count_s[3]
        window = shift - window_start()
        inside = (spot >= begin) & (spot < begin + new)
        code = jnp.where(inside, code0 + count_s[2] + spot - begin, 0.0)
        code_s[...] += jnp.sum(code.reshape(N_DEV, e_loc, 128), axis=1)
        count_s[0] = after
        count_s[1] = packed + sums[experts:]
        count_s[2] += new

        def places(e, take, pos, keep):
            index = pos + jnp.sum(twice(before) * take, axis=0, keepdims=True)
            in_window = pos + jnp.sum(twice(window) * take, axis=0, keepdims=True)
            in_local = pos + jnp.sum(twice(local) * take, axis=0, keepdims=True)
            e = e.astype(F32)
            dev = jnp.floor(e * (1.0 / e_loc))
            fixed = keep & (index < FIX)
            loose = keep & (index >= FIX)
            at_fix = jnp.where(fixed, e * FIX + index, -1.0)
            at_local = jnp.where(loose, dev * LOCAL + in_local, -1.0)
            at_back = jnp.where(loose, experts * FIX + dev * WINDOW + in_window, at_fix)
            return at_fix, at_local, at_back, jnp.where(keep, e * capacity + pos, -1.0)

        f1, l1, c1, w1 = places(e1, take1, pos1, keep1)
        f2, l2, c2, w2 = places(e2, take2, pos2, keep2)
        meta = jnp.where(meta_row == 0, c1, 0.0)
        meta = jnp.where(meta_row == 1, c2, meta)
        meta = jnp.where(meta_row == 2, g1, meta)
        meta = jnp.where(meta_row == 3, g2, meta)
        meta = jnp.where(meta_row == 4, w1, meta)
        meta = jnp.where(meta_row == 5, w2, meta)
        meta_ref[grp] = meta
        tok = pl.ds(pl.multiple_of(side * 2 * seq + grp * seq, seq), seq)
        slot_s[:, tok] = jnp.where(meta_row == 0, f1, jnp.where(meta_row == 1, f2, jnp.where(meta_row == 2, l1, l2))).astype(jnp.int32)

    @pl.when(side == 1)
    def _():
        def gather(first_row, base, count, skip):
            ids = lax.broadcasted_iota(jnp.int32, (count, 4 * seq - skip), 0) + base
            hit = (ids == slot_s[first_row:first_row + 1, skip:]) | (ids == slot_s[first_row + 1:first_row + 2, skip:])
            return dot(jnp.where(hit, 1.0, 0.0).astype(BF16), b_s[skip:, :]).astype(BF16)

        per_dev = e_loc * FIX
        for base in range(0, N_DEV, 4):
            rows = gather(0, base * per_dev, 4 * per_dev, 0)
            fix_s[quad, base:base + 4] = rows.reshape(4, e_loc, FIX, d_model)
        for base in range(0, N_DEV, 4):
            rows = gather(2, base * LOCAL, 4 * LOCAL, 2 * seq)
            local_s[base:base + 4, pl.ds(pl.multiple_of(quad * LOCAL, LOCAL), LOCAL), :] = rows.reshape(4, LOCAL, d_model)

        def per_device(value):
            return value.reshape(N_DEV, e_loc, 128)[:, 0, :]

        start = per_device(count_s[3])
        filled = per_device(count_s[1]) - start
        at = lax.broadcasted_iota(jnp.int32, (N_DEV, 256), 1).astype(F32) - (quad * LOCAL).astype(F32)
        live = (at >= 0.0) & (at < float(LOCAL)) & (at < twice(filled))
        goal_s[...] = jnp.where(live, twice(start) + at + 1.0, goal_s[...])
        flag_s[...] = jnp.maximum(flag_s[...], jnp.where(filled > LOCAL, 1.0, 0.0))
        starts_ref[pl.ds(quad, 1), :] = window_start().T[0:1, :].astype(jnp.int32)
        count_s[0] = jnp.zeros_like(count_s[0])
        count_s[3] = count_s[1]

    @pl.when(step == steps - 1)
    def _():
        send_quad(quads - 1)
        over = jnp.where((count_s[1] > PACK) | (count_s[2] > EXTRA), 1.0, 0.0)
        over = jnp.max(jnp.max(over.reshape(N_DEV, e_loc, 128), axis=1), axis=0, keepdims=True)
        over = jnp.maximum(over, jnp.max(flag_s[...], axis=0, keepdims=True))
        tally = count_s[2].T[0:1, :] + over * 1024.0
        for dev in range(N_DEV):
            msg_s[dev, 0:8] = aux_s[...]
            lower = lax.broadcasted_iota(jnp.int32, (8, 128), 0)
            msg_s[dev, 8:16] = jnp.where(lower == 0, code_s[dev:dev + 1, :], jnp.where(lower == 1, tally, 0.0))
        for place, mask in enumerate(ORDER):
            dev = partner(me, mask)
            remote(msg_s.at[dev], msg_ref.at[place], msg_send, msg_recv, dev, mask, 1)

        width = goal_s.shape[1] * 3 // 4
        rows = lax.broadcasted_iota(jnp.int32, (PACK, width), 0).astype(F32) + 1.0
        for dev in range(N_DEV):
            hit = jnp.where(rows == goal_s[dev:dev + 1, 0:width], 1.0, 0.0).astype(BF16)
            pack_s[dev] = dot(hit, local_s[dev]).astype(BF16)

        def settle(ref, sem):
            pltpu.make_async_copy(ref, ref, sem).wait()

        others = pl.ds(0, N_DEV - 1)
        settle(fix_s.at[:, 0], own_sem.at[0])
        settle(msg_s.at[0], own_sem.at[1])
        settle(fix_s.at[:, others], fix_send)
        settle(msg_s.at[others], msg_send)
        settle(fix_ref.at[:, pl.ds(0, (N_DEV - 1) * quads * FIX), :], fix_recv)
        settle(msg_ref.at[others], msg_recv)


def gate_rows(meta, count, base):
    cols = meta.T
    ids = lax.broadcasted_iota(jnp.int32, (cols.shape[0], count), 1) + base
    first = ids == cols[:, 0:1].astype(jnp.int32)
    second = ids == cols[:, 1:2].astype(jnp.int32)
    return jnp.where(first, cols[:, 2:3], jnp.where(second, cols[:, 3:4], 0.0)).astype(BF16)


def combine_fixed(fix_ref, hidden_ref, meta_ref, part_ref):
    experts, rows, d_model = fix_ref.shape
    z = fix_ref[...].reshape(experts * rows, d_model)
    for grp in range(2):
        part_ref[grp] = hidden_ref[grp].astype(F32) + dot(gate_rows(meta_ref[grp], experts * rows, 0), z)


def packed_expert_kernel(
    fix_ref, mine_ref, msg_ref, w_in_ref, w_out_ref, hidden_ref, meta_ref, back_ref, back_pack_ref, part_ref,
    w1_s, w2_s, w_sem, act_s, x_s, z_s, zx_s, code_s, pack_ref, pack_s, in_send, in_recv, fix_send, fix_recv, pack_send, pack_recv, own_sem,
):
    step = pl.program_id(0)
    n_exp = pl.num_programs(0) // 2
    e = lax.rem(step, n_exp)
    me = lax.axis_index("ep")
    rows = fix_ref.shape[1]
    d_model = fix_ref.shape[2]
    ff = w_in_ref.shape[2]
    slot = lax.rem(step, 2)
    per_src = rows // N_DEV
    chunk = 1024

    def mlp(x):
        for f in range(ff // chunk):
            act = dot(x, w1_s[slot, :, pl.ds(f * chunk, chunk)])
            act_s[0:x.shape[0], pl.ds(f * chunk, chunk)] = jnp.maximum(act, 0.0).astype(BF16)
        return dot(act_s[0:x.shape[0], :], w2_s[slot]).astype(BF16)

    def spread(place):
        ids = lax.broadcasted_iota(jnp.int32, (x_s.shape[0] * POOL, PACK), 0).astype(F32) + 1.0
        return jnp.where(ids == code_s[place:place + 1, 0:PACK], 1.0, 0.0).astype(BF16)

    def remote(src, dst, send_sem, recv_sem, mask, own):
        if mask == 0:
            pltpu.make_async_copy(src, dst, own_sem.at[own]).start()
        else:
            pltpu.make_async_remote_copy(
                src_ref=src, dst_ref=dst, send_sem=send_sem, recv_sem=recv_sem,
                device_id=(partner(me, mask),), device_id_type=MESH).start()

    def settle(ref, sem):
        pltpu.make_async_copy(ref, ref, sem).wait()

    others = pl.ds(0, N_DEV - 1)

    def weights(which, at):
        return (
            pltpu.make_async_copy(w_in_ref.at[which], w1_s.at[at], w_sem.at[0, at]),
            pltpu.make_async_copy(w_out_ref.at[which], w2_s.at[at], w_sem.at[1, at]),
        )

    @pl.when(step == 0)
    def _():
        for copy in weights(e, slot):
            copy.start()
        greet(me)
        pl.semaphore_wait(pltpu.get_barrier_semaphore(), N_DEV - 1)
        for place, mask in enumerate(ORDER):
            remote(mine_ref.at[partner(me, mask)], pack_ref.at[place], in_send, in_recv, mask, 0)

    @pl.when(step < 2 * n_exp - 1)
    def _():
        for copy in weights(lax.rem(step + 1, n_exp), 1 - slot):
            copy.start()

    for copy in weights(e, slot):
        copy.wait()

    @pl.when(step < n_exp)
    def _():
        z_s[e] = mlp(fix_ref[0])
        for place, mask in enumerate(ORDER):
            remote(z_s.at[e, pl.ds(place * per_src, per_src), :], back_ref.at[me * n_exp + e], fix_send, fix_recv, mask, 1)

    @pl.when(step == n_exp)
    def _():
        settle(pack_ref.at[0], own_sem.at[0])
        settle(pack_ref.at[others], in_recv)
        code = jnp.concatenate([msg_ref[place, 8:9, :] for place in range(N_DEV)], axis=0)
        n_loc = x_s.shape[0]
        hits = [(code > ex * EXTRA) & (code <= (ex + 1) * EXTRA) for ex in range(n_loc)]
        row = lax.broadcasted_iota(jnp.int32, (N_DEV, N_DEV), 0)
        col = lax.broadcasted_iota(jnp.int32, (N_DEV, N_DEV), 1)
        prior = jnp.where((row // TEAM == col // TEAM) & (col < row), 1.0, 0.0).astype(BF16)
        spans = dot(prior, jnp.concatenate([jnp.where(hit, 1.0, 0.0) for hit in hits], axis=1).astype(BF16))
        shared = jnp.zeros_like(code)
        for ex, hit in enumerate(hits):
            begin = jnp.sum(spans[:, ex * 128:(ex + 1) * 128], axis=1, keepdims=True)
            shared = jnp.where(hit, code + begin + float(ex * (POOL - EXTRA)), shared)
        code_s[...] = shared
        for team in range(N_DEV // TEAM):
            x = dot(spread(team * TEAM), pack_ref[team * TEAM])
            for place in range(team * TEAM + 1, (team + 1) * TEAM):
                x = x + dot(spread(place), pack_ref[place])
            x_s[:, pl.ds(team * POOL, POOL), :] = x.astype(BF16).reshape(n_loc, POOL, d_model)

    @pl.when(step >= n_exp)
    def _():
        zx_s[e] = mlp(x_s[e])

    @pl.when(step == 2 * n_exp - 1)
    def _():
        for place, mask in enumerate(ORDER):
            z = zx_s[:, pl.ds(place // TEAM * POOL, POOL), :].reshape(x_s.shape[0] * POOL, d_model)
            pack_s[place] = lax.dot_general(
                spread(place), z, (((0,), (0,)), ((), ())), preferred_element_type=F32).astype(BF16)
            if place > 0:
                remote(pack_s.at[place - 1], back_pack_ref.at[me], pack_send, pack_recv, ORDER[place - 1], 2)
        remote(pack_s.at[N_DEV - 1], back_pack_ref.at[me], pack_send, pack_recv, ORDER[N_DEV - 1], 2)
        settle(z_s.at[:, pl.ds(0, per_src), :], own_sem.at[1])
        settle(back_ref.at[pl.ds(0, (N_DEV - 1) * n_exp)], fix_recv)
        groups, seq, _ = hidden_ref.shape
        experts = back_ref.shape[0]
        pltpu.emit_pipeline(
            combine_fixed,
            grid=(groups // 2,),
            in_specs=[
                pl.BlockSpec((experts, FIX, d_model), lambda i: (0, i // 2, 0)),
                pl.BlockSpec((2, seq, d_model), lambda i: (i, 0, 0)),
                pl.BlockSpec((2, 8, seq), lambda i: (i, 0, 0)),
            ],
            out_specs=[pl.BlockSpec((2, seq, d_model), lambda i: (i, 0, 0))],
        )(back_ref, hidden_ref, meta_ref, part_ref)
        settle(pack_s.at[0], own_sem.at[2])
        settle(mine_ref.at[others], in_send)
        settle(z_s.at[:, pl.ds(0, (N_DEV - 1) * per_src), :], fix_send)
        settle(pack_s.at[others], pack_send)
        settle(back_pack_ref.at[others], pack_recv)


def packed_back_kernel(starts_ref, pack_ref, part_ref, meta_ref, msg_ref, out_ref, aux_ref, window_s, *, n_groups, experts):
    groups, seq, _ = part_ref.shape
    e_loc = experts // N_DEV
    step = pl.program_id(0)
    for dev in range(N_DEV):
        start = pl.multiple_of(starts_ref[step, dev * e_loc], 8)
        window_s[dev * WINDOW:(dev + 1) * WINDOW, :] = pack_ref[dev, pl.ds(start, WINDOW), :]

    for grp in range(0, groups, 2):
        gates = jnp.concatenate([gate_rows(meta_ref[grp + i], N_DEV * WINDOW, experts * FIX) for i in range(2)], axis=0)
        moe = dot(gates, window_s[...])
        for i in range(2):
            out_ref[grp + i] = (part_ref[grp + i] + moe[i * seq:(i + 1) * seq]).astype(BF16)

    @pl.when(step == 0)
    def _():
        aux_ref[0, 0] = jnp.sum(msg_ref[:, 0:8, :]) * (experts / n_groups)


def solution(mesh):
    def local_step(tokens, pad_mask, second_draw, choices, norm_attn, w_query, w_key, w_value, w_attn_out, norm_moe, w_gate, w_in, w_out):
        groups, seq, d_model = tokens.shape
        _, heads, head_dim = w_query.shape
        experts = w_gate.shape[1]
        ff = w_in.shape[2]
        e_loc = experts // N_DEV
        capacity = (2 * seq + experts - 1) // experts
        hw = heads * head_dim
        rows = 2 * capacity
        steps = groups // 2
        all_rows = N_DEV * steps * rows

        wq, wk, wv = (w.transpose(1, 2, 0).reshape(hw, d_model) for w in (w_query, w_key, w_value))
        wo = w_attn_out.reshape(hw, d_model)

        def whole(shape):
            return pl.BlockSpec(shape, lambda i: (0,) * len(shape), pipeline_mode=pl.Buffered(1))

        anywhere = pl.BlockSpec(memory_space=pl.ANY)
        front_specs = [
            pl.BlockSpec((2, seq, d_model), lambda i: (i, 0, 0)),
            whole((groups, seq)), whole((groups, seq)),
            pl.BlockSpec((2, 2, seq), lambda i: (i, 0, 0)),
            whole((d_model,)), whole((hw, d_model)), whole((hw, d_model)), whole((hw, d_model)), whole((hw, d_model)),
            whole((d_model,)), whole((d_model, experts)),
        ]
        quads = steps // 2
        fix_rows = quads * FIX
        dma = pltpu.SemaphoreType.DMA
        hidden_p, meta_p, mine, starts, fix, msg = pl.pallas_call(
            functools.partial(packed_front_kernel, heads=heads, head_dim=head_dim, capacity=capacity),
            name="packed_front",
            grid=(steps,),
            in_specs=front_specs,
            out_specs=[
                pl.BlockSpec((2, seq, d_model), lambda i: (i, 0, 0)),
                pl.BlockSpec((2, 8, seq), lambda i: (i, 0, 0)),
                pl.BlockSpec((N_DEV, PACK, d_model), lambda i: (0, 0, 0)),
                pl.BlockSpec((8, 128), lambda i: (0, 0)),
                anywhere, anywhere,
            ],
            out_shape=[
                jax.ShapeDtypeStruct((groups, seq, d_model), BF16),
                jax.ShapeDtypeStruct((groups, 8, seq), F32),
                jax.ShapeDtypeStruct((N_DEV, PACK, d_model), BF16),
                jax.ShapeDtypeStruct((8, 128), jnp.int32),
                jax.ShapeDtypeStruct((e_loc, N_DEV * fix_rows, d_model), BF16),
                jax.ShapeDtypeStruct((N_DEV, 16, 128), F32),
            ],
            scratch_shapes=[
                pltpu.VMEM((hw, 2 * seq), BF16),
                pltpu.VMEM((2 * seq, hw), BF16),
                pltpu.VMEM((hw, 2 * seq), BF16),
                pltpu.VMEM((hw, 2 * seq), BF16),
                pltpu.VMEM((2, heads, seq, seq), F32),
                pltpu.VMEM((2, heads, seq, seq), BF16),
                pltpu.VMEM((3 * experts, d_model), BF16),
                pltpu.VMEM((4 * seq, d_model), BF16),
                pltpu.VMEM((8, 4 * seq), jnp.int32),
                pltpu.VMEM((4, experts, 128), F32),
                pltpu.VMEM((8, 128), F32),
                pltpu.VMEM((N_DEV, 128), F32),
                pltpu.VMEM((N_DEV, 128), F32),
                pltpu.VMEM((N_DEV, 256), F32),
                pltpu.VMEM((N_DEV, quads * LOCAL, d_model), BF16),
                pltpu.VMEM((quads, N_DEV, e_loc, FIX, d_model), BF16),
                pltpu.VMEM((N_DEV, 16, 128), F32),
                dma, dma, dma, dma, dma((2,)),
            ],
            compiler_params=pltpu.CompilerParams(
                dimension_semantics=("arbitrary",), collective_id=0, has_side_effects=True, vmem_limit_bytes=VMEM_LIMIT),
        )(tokens, pad_mask, second_draw, choices.transpose(0, 2, 1), norm_attn, wq, wk, wv, wo, norm_moe, w_gate)

        def packed_path():
            back, back_pack, part = pl.pallas_call(
                packed_expert_kernel,
                name="packed_experts",
                grid=(2 * e_loc,),
                in_specs=[
                    pl.BlockSpec((1, N_DEV * fix_rows, d_model), lambda i: (jnp.minimum(i, e_loc - 1), 0, 0)),
                    whole((N_DEV, PACK, d_model)), whole((N_DEV, 16, 128)),
                    anywhere, anywhere, anywhere, anywhere,
                ],
                out_specs=[anywhere, anywhere, anywhere],
                out_shape=[
                    jax.ShapeDtypeStruct((experts, fix_rows, d_model), BF16),
                    jax.ShapeDtypeStruct((N_DEV, PACK, d_model), BF16),
                    jax.ShapeDtypeStruct((groups, seq, d_model), F32),
                ],
                scratch_shapes=[
                    pltpu.VMEM((2, d_model, ff), BF16),
                    pltpu.VMEM((2, ff, d_model), BF16),
                    dma((2, 2)),
                    pltpu.VMEM((N_DEV * fix_rows, ff), BF16),
                    pltpu.VMEM((e_loc, N_DEV // TEAM * POOL, d_model), BF16),
                    pltpu.VMEM((e_loc, N_DEV * fix_rows, d_model), BF16),
                    pltpu.VMEM((e_loc, N_DEV // TEAM * POOL, d_model), BF16),
                    pltpu.VMEM((N_DEV, 128), F32),
                    pltpu.VMEM((N_DEV, PACK, d_model), BF16),
                    pltpu.VMEM((N_DEV, PACK, d_model), BF16),
                    dma, dma, dma, dma, dma, dma, dma((3,)),
                ],
                compiler_params=pltpu.CompilerParams(
                    dimension_semantics=("arbitrary",), collective_id=1, has_side_effects=True, vmem_limit_bytes=VMEM_LIMIT),
            )(fix, mine, msg, w_in, w_out, hidden_p, meta_p)
            return pl.pallas_call(
                functools.partial(packed_back_kernel, n_groups=groups * N_DEV, experts=experts),
                name="packed_back",
                grid_spec=pltpu.PrefetchScalarGridSpec(
                    num_scalar_prefetch=1,
                    grid=(quads,),
                    in_specs=[
                        pl.BlockSpec((N_DEV, PACK, d_model), lambda i, starts: (0, 0, 0), pipeline_mode=pl.Buffered(1)),
                        pl.BlockSpec((4, seq, d_model), lambda i, starts: (i, 0, 0)),
                        pl.BlockSpec((4, 8, seq), lambda i, starts: (i, 0, 0)),
                        pl.BlockSpec((N_DEV, 16, 128), lambda i, starts: (0, 0, 0), pipeline_mode=pl.Buffered(1)),
                    ],
                    out_specs=[
                        pl.BlockSpec((4, seq, d_model), lambda i, starts: (i, 0, 0)),
                        pl.BlockSpec(memory_space=pltpu.SMEM),
                    ],
                    scratch_shapes=[pltpu.VMEM((N_DEV * WINDOW, d_model), BF16)],
                ),
                out_shape=[
                    jax.ShapeDtypeStruct((groups, seq, d_model), BF16),
                    jax.ShapeDtypeStruct((1, 1), F32),
                ],
                compiler_params=pltpu.CompilerParams(dimension_semantics=("arbitrary",), vmem_limit_bytes=VMEM_LIMIT),
            )(starts, back_pack, part, meta_p, msg)

        def full_path():
            recv = pl.pallas_call(
                functools.partial(full_front_kernel, experts=experts, capacity=capacity),
                name="full_front",
                grid=(steps,),
                in_specs=[
                    pl.BlockSpec((2, seq, d_model), lambda i: (i, 0, 0)),
                    pl.BlockSpec((2, 8, seq), lambda i: (i, 0, 0)),
                    whole((d_model,)),
                ],
                out_specs=anywhere,
                out_shape=jax.ShapeDtypeStruct((e_loc, all_rows, d_model), BF16),
                scratch_shapes=[pltpu.VMEM((steps, N_DEV, e_loc, rows, d_model), BF16), dma, dma, dma],
                compiler_params=pltpu.CompilerParams(
                    dimension_semantics=("arbitrary",), collective_id=2, has_side_effects=True, vmem_limit_bytes=VMEM_LIMIT),
            )(hidden_p, meta_p, norm_moe)
            tile = all_rows // 4
            ret = pl.pallas_call(
                functools.partial(expert_kernel, tile=tile),
                name="full_experts",
                grid=(e_loc,),
                in_specs=[
                    pl.BlockSpec((1, all_rows, d_model), lambda i: (i, 0, 0)),
                    pl.BlockSpec((1, d_model, ff), lambda i: (i, 0, 0)),
                    pl.BlockSpec((1, ff, d_model), lambda i: (i, 0, 0)),
                ],
                out_specs=anywhere,
                out_shape=jax.ShapeDtypeStruct((experts, steps * rows, d_model), BF16),
                scratch_shapes=[pltpu.VMEM((tile, ff), BF16), pltpu.VMEM((e_loc, all_rows, d_model), BF16), dma, dma, dma],
                compiler_params=pltpu.CompilerParams(
                    dimension_semantics=("arbitrary",), collective_id=3, has_side_effects=True, vmem_limit_bytes=VMEM_LIMIT),
            )(recv, w_in, w_out)
            return pl.pallas_call(
                functools.partial(back_kernel, n_groups=groups * N_DEV, capacity=capacity),
                name="full_back",
                grid=(steps,),
                in_specs=[
                    pl.BlockSpec((experts, rows, d_model), lambda i: (0, i, 0)),
                    pl.BlockSpec((2, seq, d_model), lambda i: (i, 0, 0)),
                    pl.BlockSpec((2, 8, seq), lambda i: (i, 0, 0)),
                    whole((N_DEV, 16, 128)),
                ],
                out_specs=[
                    pl.BlockSpec((2, seq, d_model), lambda i: (i, 0, 0)),
                    pl.BlockSpec(memory_space=pltpu.SMEM),
                ],
                out_shape=[
                    jax.ShapeDtypeStruct((groups, seq, d_model), BF16),
                    jax.ShapeDtypeStruct((1, 1), F32),
                ],
                compiler_params=pltpu.CompilerParams(dimension_semantics=("arbitrary",), vmem_limit_bytes=VMEM_LIMIT),
            )(ret, hidden_p, meta_p, msg)

        shared = jnp.sum(msg[:, 9, :].reshape(N_DEV // TEAM, TEAM, experts), axis=1)
        spilled = jnp.max(shared) > POOL
        out, aux = lax.cond(spilled, full_path, packed_path)
        return out, aux.reshape(())

    by_group = P("ep")
    replicated = P()
    in_specs = (by_group, by_group, by_group, by_group, replicated, replicated, replicated, replicated, replicated, replicated, replicated, by_group, by_group)
    return jax.shard_map(local_step, mesh=mesh, in_specs=in_specs, out_specs=(by_group, replicated), check_vma=False)
```

```python
import functools
import jax
import jax.numpy as jnp
from jax import lax
from jax.experimental import pallas as pl
from jax.experimental.pallas import tpu as pltpu
from jax.sharding import PartitionSpec as P

NORM_EPS = 1e-6
N_DEV = 16
MESH = pl.DeviceIdType.MESH
F32 = jnp.float32
BF16 = jnp.bfloat16
ORDER = (0, 9, 2, 11, 4, 13, 6, 15, 8, 1, 10, 3, 12, 5, 14, 7)
SENDS = tuple((ORDER.index(mask), mask) for mask in (6, 8, 10, 4, 12, 2, 14, 1, 7, 9, 11, 5, 13, 3, 15, 0))
VMEM_LIMIT = 62 * 1024 * 1024


def partner(me, mask):
    out = 0
    for bit in range(4):
        val = lax.rem(me // (1 << bit), 2)
        out = out + (1 << bit) * ((1 - val) if (mask >> bit) & 1 else val)
    return out


def greet(me):
    barrier = pltpu.get_barrier_semaphore()
    for mask in range(1, N_DEV):
        pl.semaphore_signal(barrier, inc=1, device_id=(partner(me, mask),), device_id_type=MESH)


def rms_norm(values_f, scale_vec):
    inv_rms = lax.rsqrt(jnp.mean(values_f * values_f, axis=-1, keepdims=True) + NORM_EPS)
    return (values_f * inv_rms * scale_vec).astype(BF16)


def dot(a, b):
    return jnp.dot(a, b, preferred_element_type=F32)


def dot_nt(a, b):
    return lax.dot_general(a, b, (((1,), (1,)), ((), ())), preferred_element_type=F32)


def split_gate(wgate_ref, wg_s):
    experts = wgate_ref.shape[1]
    wg = wgate_ref[...].T
    hi = wg.astype(BF16)
    rest = wg - hi.astype(F32)
    mid = rest.astype(BF16)
    low = (rest - mid.astype(F32)).astype(BF16)
    wg_s[0:experts] = hi
    wg_s[experts:2 * experts] = mid
    wg_s[2 * experts:3 * experts] = low


def attend(
    step, tokens_ref, pad_ref, norm_attn_ref, wq_ref, wk_ref, wv_ref, wo_ref, norm_moe_ref, hidden_ref,
    q_s, k_s, v_s, ctx_s, s_s, p_s, wg_s, heads, head_dim, experts,
):
    seq = tokens_ref.shape[1]
    d_model = tokens_ref.shape[2]
    x = tokens_ref[...].reshape(2 * seq, d_model)
    a = rms_norm(x.astype(F32), norm_attn_ref[...][None, :])
    q_s[...] = dot_nt(wq_ref[...], a).astype(BF16)
    k_s[...] = dot_nt(a, wk_ref[...]).astype(BF16)
    v_s[...] = dot_nt(wv_ref[...], a).astype(BF16)

    width = 2 * head_dim
    lane = lax.broadcasted_iota(jnp.int32, (1, width), 1)
    scale = head_dim ** -0.5
    sides = [jnp.where(lane < head_dim, scale, 0.0).astype(BF16), jnp.where(lane < head_dim, 0.0, scale).astype(BF16)]
    cut = seq // 2
    late_key = lax.broadcasted_iota(jnp.int32, (seq - cut, 128), 0) + cut
    batch = s_s.shape[1]
    lanes = 128
    buf = 0
    for grp in range(2):
        tok = pl.ds(grp * seq, seq)
        length = jnp.sum(pad_ref[pl.ds(2 * step + grp, 1), :], axis=1, keepdims=True)
        keep_late = late_key < length
        for first in range(0, heads, batch):
            for i in range(batch):
                off = (first + i) // 2 * width
                k = k_s[tok, pl.ds(off, width)] * sides[(first + i) % 2]
                s_s[buf, i] = dot(k, q_s[pl.ds(off, width), tok])
            for i in range(batch):
                for col in range(0, seq, lanes):
                    cols = pl.ds(col, lanes)
                    early = s_s[buf, i, pl.ds(0, cut), cols]
                    late = jnp.where(keep_late, s_s[buf, i, pl.ds(cut, seq - cut), cols], -1e30)
                    top = jnp.maximum(jnp.max(early, axis=0, keepdims=True), jnp.max(late, axis=0, keepdims=True))
                    early = jnp.exp(early - top)
                    late = jnp.exp(late - top)
                    inv = 1.0 / (jnp.sum(early, axis=0, keepdims=True) + jnp.sum(late, axis=0, keepdims=True))
                    p_s[buf, i, pl.ds(0, cut), cols] = (early * inv).astype(BF16)
                    p_s[buf, i, pl.ds(cut, seq - cut), cols] = (late * inv).astype(BF16)
            for i in range(batch):
                head = pl.ds((first + i) * head_dim, head_dim)
                ctx_s[head, tok] = dot(v_s[head, tok], p_s[buf, i]).astype(BF16)
            buf = 1 - buf

    attn = lax.dot_general(ctx_s[...], wo_ref[...], (((0,), (0,)), ((), ())), preferred_element_type=F32)
    hidden = (x.astype(F32) + attn).astype(BF16)
    hidden_ref[...] = hidden.reshape(2, seq, d_model)
    b = rms_norm(hidden.astype(F32), norm_moe_ref[...][None, :])
    lg = dot_nt(wg_s[...], b)
    logits = (lg[2 * experts:] + lg[experts:2 * experts]) + lg[:experts]
    ex = jnp.exp(logits - jnp.max(logits, axis=0, keepdims=True))
    return b, ex / jnp.sum(ex, axis=0, keepdims=True)


def full_front_kernel(hidden_ref, meta_ref, norm_moe_ref, recv_ref, send_s, send_sem, recv_sem, own_sem, *, experts, capacity):
    step = pl.program_id(0)
    steps = pl.num_programs(0)
    me = lax.axis_index("ep")
    seq = hidden_ref.shape[1]
    d_model = hidden_ref.shape[2]
    e_loc = experts // N_DEV
    half = e_loc // 2
    slots = experts * capacity
    rows = 2 * capacity
    per_src = steps * rows

    def send_pair(pair):
        for place, mask in SENDS:
            dev = partner(me, mask)
            src = send_s.at[pair, dev]
            dst = recv_ref.at[:, pl.ds(pl.multiple_of(place * per_src + pair * rows, rows), rows), :]
            if mask == 0:
                pltpu.make_async_copy(src, dst, own_sem).start()
            else:
                pltpu.make_async_remote_copy(
                    src_ref=src, dst_ref=dst, send_sem=send_sem, recv_sem=recv_sem,
                    device_id=(dev,), device_id_type=MESH).start()

    @pl.when(step == 0)
    def _():
        greet(me)

    @pl.when(step == 1)
    def _():
        pl.semaphore_wait(pltpu.get_barrier_semaphore(), N_DEV - 1)

    @pl.when(step > 0)
    def _():
        send_pair(step - 1)

    slot_id = lax.broadcasted_iota(jnp.int32, (slots, seq), 0)
    picked = []
    for grp in range(2):
        b = rms_norm(hidden_ref[grp].astype(F32), norm_moe_ref[...][None, :])

        def place_of(code):
            e = code // capacity
            dev = e // e_loc
            r = e - dev * e_loc
            upper = r // half
            side = upper if grp == 0 else 1 - upper
            at = ((dev * half + r - upper * half) * 2 + side) * capacity + code - e * capacity
            return jnp.where(code >= 0, at, -1)

        d1 = place_of(meta_ref[grp, 4:5, :].astype(jnp.int32))
        d2 = place_of(meta_ref[grp, 5:6, :].astype(jnp.int32))
        disp_mat = jnp.where((slot_id == d1) | (slot_id == d2), 1.0, 0.0).astype(BF16)
        picked.append(dot(disp_mat, b).reshape(N_DEV * half, rows, d_model))

    top = lax.broadcasted_iota(jnp.int32, (1, rows, 1), 1) < capacity
    lower = jnp.where(top, picked[0], picked[1]).astype(BF16)
    upper = jnp.where(top, picked[1], picked[0]).astype(BF16)
    send_s[step, :, 0:half] = lower.reshape(N_DEV, half, rows, d_model)
    send_s[step, :, half:e_loc] = upper.reshape(N_DEV, half, rows, d_model)

    @pl.when(step == steps - 1)
    def _():
        send_pair(steps - 1)
        others = pl.ds(0, N_DEV - 1)
        pltpu.make_async_copy(send_s.at[:, others], send_s.at[:, others], send_sem).wait()
        pltpu.make_async_copy(send_s.at[:, 0], send_s.at[:, 0], own_sem).wait()
        arrived = recv_ref.at[:, pl.ds(0, (N_DEV - 1) * per_src), :]
        pltpu.make_async_copy(arrived, arrived, recv_sem).wait()


def expert_kernel(recv_ref, w_in_ref, w_out_ref, ret_ref, act_s, z_s, send_sem, recv_sem, local_sem, *, tile):
    e = pl.program_id(0)
    n_exp = pl.num_programs(0)
    me = lax.axis_index("ep")
    rows = recv_ref.shape[1]
    ff = w_in_ref.shape[2]
    per_src = rows // N_DEV
    n_tiles = rows // tile
    chunk = 1024

    @pl.when(e == 0)
    def _():
        greet(me)

    def run(t, carry):
        at = pl.ds(pl.multiple_of(t * tile, tile), tile)
        x = recv_ref[0, at, :]
        for f in range(ff // chunk):
            act = dot(x, w_in_ref[0, :, pl.ds(f * chunk, chunk)])
            act_s[:, pl.ds(f * chunk, chunk)] = jnp.maximum(act, 0.0).astype(BF16)
        z_s[e, at, :] = dot(act_s[...], w_out_ref[0]).astype(BF16)
        return carry

    lax.fori_loop(0, n_tiles, run, 0)

    @pl.when(e == 0)
    def _():
        pl.semaphore_wait(pltpu.get_barrier_semaphore(), N_DEV - 1)

    for place, mask in SENDS:
        dev = partner(me, mask)
        src = z_s.at[e, pl.ds(place * per_src, per_src), :]
        dst = ret_ref.at[me * n_exp + e]
        if mask == 0:
            pltpu.make_async_copy(src, dst, local_sem).start()
        else:
            pltpu.make_async_remote_copy(
                src_ref=src, dst_ref=dst, send_sem=send_sem, recv_sem=recv_sem,
                device_id=(dev,), device_id_type=MESH).start()

    @pl.when(e == n_exp - 1)
    def _():
        sent = z_s.at[:, pl.ds(0, (N_DEV - 1) * per_src), :]
        pltpu.make_async_copy(sent, sent, send_sem).wait()
        own = z_s.at[:, pl.ds(0, per_src), :]
        pltpu.make_async_copy(own, own, local_sem).wait()
        arrived = ret_ref.at[pl.ds(0, (N_DEV - 1) * n_exp)]
        pltpu.make_async_copy(arrived, arrived, recv_sem).wait()


def back_kernel(ret_ref, hidden_ref, meta_ref, msg_ref, out_ref, aux_ref, *, n_groups, capacity):
    experts, rows, d_model = ret_ref.shape
    seq = hidden_ref.shape[1]
    z = ret_ref[...].reshape(experts * rows, d_model)
    slot_id = lax.broadcasted_iota(jnp.int32, (seq, experts * rows), 1)
    e_loc = experts // N_DEV
    for grp in range(2):
        meta = meta_ref[grp].T

        def place_of(code):
            e = code // capacity
            r = e - e // e_loc * e_loc
            upper = r // (e_loc // 2)
            side = upper if grp == 0 else 1 - upper
            return jnp.where(code >= 0, (e * 2 + side) * capacity + code - e * capacity, -1)

        c1 = place_of(meta[:, 4:5].astype(jnp.int32))
        c2 = place_of(meta[:, 5:6].astype(jnp.int32))
        comb = jnp.where(slot_id == c1, meta[:, 2:3], 0.0) + jnp.where(slot_id == c2, meta[:, 3:4], 0.0)
        moe = dot(comb.astype(BF16), z)
        out_ref[grp] = (hidden_ref[grp].astype(F32) + moe).astype(BF16)

    @pl.when(pl.program_id(0) == 0)
    def _():
        aux_ref[0, 0] = jnp.sum(msg_ref[:, 0:8, :]) * (experts / n_groups)


FIX = 8
LOCAL = 48
PACK = 104
EXTRA = 32
TEAM = 4
POOL = 80
WINDOW = 64


def twice(value):
    return jnp.concatenate([value, value], axis=1)


def packed_front_kernel(
    tokens_ref, pad_ref, draw_ref, choices_ref, norm_attn_ref, wq_ref, wk_ref, wv_ref, wo_ref, norm_moe_ref, wgate_ref,
    hidden_ref, meta_ref, pack_s, starts_ref, fix_ref, msg_ref,
    q_s, k_s, v_s, ctx_s, s_s, p_s, wg_s, b_s, slot_s, count_s, aux_s, flag_s, code_s, goal_s,
    local_s, fix_s, msg_s, fix_send, fix_recv, msg_send, msg_recv, own_sem,
    *, heads, head_dim, capacity,
):
    step = pl.program_id(0)
    steps = pl.num_programs(0)
    quad = step // 2
    quads = steps // 2
    me = lax.axis_index("ep")
    seq = tokens_ref.shape[1]
    d_model = tokens_ref.shape[2]
    experts = wgate_ref.shape[1]
    e_loc = experts // N_DEV

    def remote(src, dst, send_sem, recv_sem, dev, mask, own):
        if mask == 0:
            pltpu.make_async_copy(src, dst, own_sem.at[own]).start()
        else:
            pltpu.make_async_remote_copy(
                src_ref=src, dst_ref=dst, send_sem=send_sem, recv_sem=recv_sem,
                device_id=(dev,), device_id_type=MESH).start()

    def send_quad(which):
        for place, mask in SENDS:
            dev = partner(me, mask)
            row = pl.multiple_of(place * quads * FIX + which * FIX, FIX)
            remote(fix_s.at[which, dev], fix_ref.at[:, pl.ds(row, FIX), :], fix_send, fix_recv, dev, mask, 0)

    @pl.when(step == 0)
    def _():
        greet(me)
        split_gate(wgate_ref, wg_s)
        aux_s[...] = jnp.zeros_like(aux_s)
        flag_s[...] = jnp.zeros_like(flag_s)
        code_s[...] = jnp.zeros_like(code_s)
        goal_s[...] = jnp.zeros_like(goal_s)
        count_s[...] = jnp.zeros_like(count_s)

    @pl.when(step == 2)
    def _():
        pl.semaphore_wait(pltpu.get_barrier_semaphore(), N_DEV - 1)

    @pl.when((step > 0) & (lax.rem(step, 2) == 0))
    def _():
        send_quad(quad - 1)

    b, gate_probs = attend(
        step, tokens_ref, pad_ref, norm_attn_ref, wq_ref, wk_ref, wv_ref, wo_ref, norm_moe_ref, hidden_ref,
        q_s, k_s, v_s, ctx_s, s_s, p_s, wg_s, heads, head_dim, experts)
    side = lax.rem(step, 2)
    b_s[pl.ds(pl.multiple_of(side * 2 * seq, 2 * seq), 2 * seq), :] = b

    eid = lax.broadcasted_iota(jnp.int32, (experts, seq), 0)
    tri = jnp.where(lax.broadcasted_iota(jnp.int32, (seq, seq), 0) <= lax.broadcasted_iota(jnp.int32, (seq, seq), 1), 1.0, 0.0)
    tri = jnp.concatenate([tri, jnp.ones((seq, 128), F32)], axis=1).astype(BF16)
    row_e = lax.broadcasted_iota(jnp.int32, (experts, experts), 0)
    col_e = lax.broadcasted_iota(jnp.int32, (experts, experts), 1)
    same = row_e // e_loc == col_e // e_loc
    mix = jnp.concatenate([jnp.where(same & (col_e < row_e), 1.0, 0.0), jnp.where(same, 1.0, 0.0)], axis=0).astype(BF16)
    spot = lax.broadcasted_iota(jnp.int32, (experts, 128), 1).astype(F32)
    code0 = (lax.rem(lax.broadcasted_iota(jnp.int32, (experts, 128), 0), e_loc) * EXTRA + 1).astype(F32)
    meta_row = lax.broadcasted_iota(jnp.int32, (8, seq), 0)

    def window_start():
        return jnp.minimum(jnp.floor(count_s[3] * (1.0 / 8)) * 8.0, float(PACK - WINDOW))

    for grp in range(2):
        p = gate_probs[:, grp * seq:(grp + 1) * seq]
        valid = pad_ref[pl.ds(2 * step + grp, 1), :] == 1
        draw = draw_ref[pl.ds(2 * step + grp, 1), :]
        e1 = choices_ref[grp, 0:1, :]
        e2 = choices_ref[grp, 1:2, :]
        hot1 = eid == e1
        hot2 = eid == e2
        p1 = jnp.sum(jnp.where(hot1, p, 0.0), axis=0, keepdims=True)
        p2 = jnp.sum(jnp.where(hot2, p, 0.0), axis=0, keepdims=True)
        g1 = p1 / (p1 + p2)
        g2 = p2 / (p1 + p2)
        want2 = valid & (draw < 2.0 * g2)
        take1 = jnp.where(hot1 & valid, 1.0, 0.0)
        take2 = jnp.where(hot2 & want2, 1.0, 0.0)
        cum = dot(jnp.concatenate([take1, take2], axis=0).astype(BF16), tri)
        cum1 = cum[:experts, :seq]
        cum2 = cum[experts:, :seq]
        count1 = cum[:experts, seq:]
        count2 = cum[experts:, seq:]
        first = jnp.minimum(count1, float(capacity))
        pos1 = jnp.sum((cum1 - 1.0) * take1, axis=0, keepdims=True)
        pos2 = jnp.sum((cum2 - 1.0 + twice(first)) * take2, axis=0, keepdims=True)
        keep1 = valid & (pos1 < capacity)
        keep2 = want2 & (pos2 < capacity)

        share = jnp.where(valid, p, 0.0) * twice(count1 * (1.0 / (seq * seq)))
        share = jnp.sum(share.reshape(experts // 8, 8, seq), axis=0)
        for col in range(seq // 128):
            aux_s[...] += share[:, col * 128:(col + 1) * 128]

        before = count_s[0]
        after = before + jnp.minimum(first + count2, float(capacity))
        new = jnp.maximum(after - FIX, 0.0) - jnp.maximum(before - FIX, 0.0)
        sums = dot(mix, new.astype(BF16))
        packed = count_s[1]
        begin = packed + sums[:experts]
        shift = begin - jnp.maximum(before, float(FIX)) + before
        local = shift - count_s[3]
        window = shift - window_start()
        inside = (spot >= begin) & (spot < begin + new)
        code = jnp.where(inside, code0 + count_s[2] + spot - begin, 0.0)
        code_s[...] += jnp.sum(code.reshape(N_DEV, e_loc, 128), axis=1)
        count_s[0] = after
        count_s[1] = packed + sums[experts:]
        count_s[2] += new

        def places(e, take, pos, keep):
            index = pos + jnp.sum(twice(before) * take, axis=0, keepdims=True)
            in_window = pos + jnp.sum(twice(window) * take, axis=0, keepdims=True)
            in_local = pos + jnp.sum(twice(local) * take, axis=0, keepdims=True)
            e = e.astype(F32)
            dev = jnp.floor(e * (1.0 / e_loc))
            fixed = keep & (index < FIX)
            loose = keep & (index >= FIX)
            at_fix = jnp.where(fixed, e * FIX + index, -1.0)
            at_local = jnp.where(loose, dev * LOCAL + in_local, -1.0)
            at_back = jnp.where(loose, experts * FIX + dev * WINDOW + in_window, at_fix)
            return at_fix, at_local, at_back, jnp.where(keep, e * capacity + pos, -1.0)

        f1, l1, c1, w1 = places(e1, take1, pos1, keep1)
        f2, l2, c2, w2 = places(e2, take2, pos2, keep2)
        meta = jnp.where(meta_row == 0, c1, 0.0)
        meta = jnp.where(meta_row == 1, c2, meta)
        meta = jnp.where(meta_row == 2, g1, meta)
        meta = jnp.where(meta_row == 3, g2, meta)
        meta = jnp.where(meta_row == 4, w1, meta)
        meta = jnp.where(meta_row == 5, w2, meta)
        meta_ref[grp] = meta
        tok = pl.ds(pl.multiple_of(side * 2 * seq + grp * seq, seq), seq)
        slot_s[:, tok] = jnp.where(meta_row == 0, f1, jnp.where(meta_row == 1, f2, jnp.where(meta_row == 2, l1, l2))).astype(jnp.int32)

    @pl.when(side == 1)
    def _():
        def gather(first_row, base, count, skip):
            ids = lax.broadcasted_iota(jnp.int32, (count, 4 * seq - skip), 0) + base
            hit = (ids == slot_s[first_row:first_row + 1, skip:]) | (ids == slot_s[first_row + 1:first_row + 2, skip:])
            return dot(jnp.where(hit, 1.0, 0.0).astype(BF16), b_s[skip:, :]).astype(BF16)

        per_dev = e_loc * FIX
        for base in range(0, N_DEV, 8):
            rows = gather(0, base * per_dev, 8 * per_dev, 0)
            fix_s[quad, base:base + 8] = rows.reshape(8, e_loc, FIX, d_model)
        for base in range(0, N_DEV, 8):
            rows = gather(2, base * LOCAL, 8 * LOCAL, 2 * seq)
            local_s[base:base + 8, pl.ds(pl.multiple_of(quad * LOCAL, LOCAL), LOCAL), :] = rows.reshape(8, LOCAL, d_model)

        def per_device(value):
            return value.reshape(N_DEV, e_loc, 128)[:, 0, :]

        start = per_device(count_s[3])
        filled = per_device(count_s[1]) - start
        at = lax.broadcasted_iota(jnp.int32, (N_DEV, 256), 1).astype(F32) - (quad * LOCAL).astype(F32)
        live = (at >= 0.0) & (at < float(LOCAL)) & (at < twice(filled))
        goal_s[...] = jnp.where(live, twice(start) + at + 1.0, goal_s[...])
        flag_s[...] = jnp.maximum(flag_s[...], jnp.where(filled > LOCAL, 1.0, 0.0))
        starts_ref[pl.ds(quad, 1), :] = window_start().T[0:1, :].astype(jnp.int32)
        count_s[0] = jnp.zeros_like(count_s[0])
        count_s[3] = count_s[1]

    @pl.when(step == steps - 1)
    def _():
        send_quad(quads - 1)
        over = jnp.where((count_s[1] > PACK) | (count_s[2] > EXTRA), 1.0, 0.0)
        over = jnp.max(jnp.max(over.reshape(N_DEV, e_loc, 128), axis=1), axis=0, keepdims=True)
        over = jnp.maximum(over, jnp.max(flag_s[...], axis=0, keepdims=True))
        tally = count_s[2].T[0:1, :] + over * 1024.0
        for dev in range(N_DEV):
            msg_s[dev, 0:8] = aux_s[...]
            lower = lax.broadcasted_iota(jnp.int32, (8, 128), 0)
            msg_s[dev, 8:16] = jnp.where(lower == 0, code_s[dev:dev + 1, :], jnp.where(lower == 1, tally, 0.0))
        for place, mask in SENDS:
            dev = partner(me, mask)
            remote(msg_s.at[dev], msg_ref.at[place], msg_send, msg_recv, dev, mask, 1)

        width = goal_s.shape[1] * 3 // 4
        rows = lax.broadcasted_iota(jnp.int32, (PACK, width), 0).astype(F32) + 1.0
        for dev in range(N_DEV):
            hit = jnp.where(rows == goal_s[dev:dev + 1, 0:width], 1.0, 0.0).astype(BF16)
            pack_s[dev] = dot(hit, local_s[dev]).astype(BF16)

        def settle(ref, sem):
            pltpu.make_async_copy(ref, ref, sem).wait()

        others = pl.ds(0, N_DEV - 1)
        settle(fix_s.at[:, 0], own_sem.at[0])
        settle(msg_s.at[0], own_sem.at[1])
        settle(fix_s.at[:, others], fix_send)
        settle(msg_s.at[others], msg_send)
        settle(fix_ref.at[:, pl.ds(0, (N_DEV - 1) * quads * FIX), :], fix_recv)
        settle(msg_ref.at[others], msg_recv)


def gate_rows(meta, count, base):
    cols = meta.T
    ids = lax.broadcasted_iota(jnp.int32, (cols.shape[0], count), 1) + base
    first = ids == cols[:, 0:1].astype(jnp.int32)
    second = ids == cols[:, 1:2].astype(jnp.int32)
    return jnp.where(first, cols[:, 2:3], jnp.where(second, cols[:, 3:4], 0.0)).astype(BF16)


def combine_fixed(fix_ref, hidden_ref, meta_ref, part_ref):
    experts, rows, d_model = fix_ref.shape
    z = fix_ref[...].reshape(experts * rows, d_model)
    for grp in range(2):
        part_ref[grp] = hidden_ref[grp].astype(F32) + dot(gate_rows(meta_ref[grp], experts * rows, 0), z)


def packed_expert_kernel(
    fix_ref, mine_ref, msg_ref, w_in_ref, w_out_ref, hidden_ref, meta_ref, back_ref, back_pack_ref, part_ref,
    w1_s, w2_s, w_sem, act_s, x_s, z_s, zx_s, code_s, pack_ref, pack_s, in_send, in_recv, fix_send, fix_recv, pack_send, pack_recv, own_sem,
):
    step = pl.program_id(0)
    n_exp = pl.num_programs(0) // 2
    e = lax.rem(step, n_exp)
    me = lax.axis_index("ep")
    rows = fix_ref.shape[1]
    d_model = fix_ref.shape[2]
    ff = w_in_ref.shape[2]
    slot = lax.rem(step, 2)
    per_src = rows // N_DEV
    chunk = 1024

    def mlp(x):
        for f in range(ff // chunk):
            act = dot(x, w1_s[slot, :, pl.ds(f * chunk, chunk)])
            act_s[0:x.shape[0], pl.ds(f * chunk, chunk)] = jnp.maximum(act, 0.0).astype(BF16)
        return dot(act_s[0:x.shape[0], :], w2_s[slot]).astype(BF16)

    def spread(place):
        ids = lax.broadcasted_iota(jnp.int32, (x_s.shape[0] * POOL, PACK), 0).astype(F32) + 1.0
        return jnp.where(ids == code_s[place:place + 1, 0:PACK], 1.0, 0.0).astype(BF16)

    def remote(src, dst, send_sem, recv_sem, mask, own):
        if mask == 0:
            pltpu.make_async_copy(src, dst, own_sem.at[own]).start()
        else:
            pltpu.make_async_remote_copy(
                src_ref=src, dst_ref=dst, send_sem=send_sem, recv_sem=recv_sem,
                device_id=(partner(me, mask),), device_id_type=MESH).start()

    def settle(ref, sem):
        pltpu.make_async_copy(ref, ref, sem).wait()

    others = pl.ds(0, N_DEV - 1)

    def weights(which, at):
        return (
            pltpu.make_async_copy(w_in_ref.at[which], w1_s.at[at], w_sem.at[0, at]),
            pltpu.make_async_copy(w_out_ref.at[which], w2_s.at[at], w_sem.at[1, at]),
        )

    @pl.when(step == 0)
    def _():
        for copy in weights(e, slot):
            copy.start()
        greet(me)
        pl.semaphore_wait(pltpu.get_barrier_semaphore(), N_DEV - 1)
        for place, mask in SENDS:
            remote(mine_ref.at[partner(me, mask)], pack_ref.at[place], in_send, in_recv, mask, 0)

    @pl.when(step < 2 * n_exp - 1)
    def _():
        for copy in weights(lax.rem(step + 1, n_exp), 1 - slot):
            copy.start()

    for copy in weights(e, slot):
        copy.wait()

    @pl.when(step < n_exp)
    def _():
        z_s[e] = mlp(fix_ref[0])
        for place, mask in SENDS:
            remote(z_s.at[e, pl.ds(place * per_src, per_src), :], back_ref.at[me * n_exp + e], fix_send, fix_recv, mask, 1)

    @pl.when(step == n_exp)
    def _():
        settle(pack_ref.at[0], own_sem.at[0])
        settle(pack_ref.at[others], in_recv)
        code = jnp.concatenate([msg_ref[place, 8:9, :] for place in range(N_DEV)], axis=0)
        n_loc = x_s.shape[0]
        hits = [(code > ex * EXTRA) & (code <= (ex + 1) * EXTRA) for ex in range(n_loc)]
        row = lax.broadcasted_iota(jnp.int32, (N_DEV, N_DEV), 0)
        col = lax.broadcasted_iota(jnp.int32, (N_DEV, N_DEV), 1)
        prior = jnp.where((row // TEAM == col // TEAM) & (col < row), 1.0, 0.0).astype(BF16)
        spans = dot(prior, jnp.concatenate([jnp.where(hit, 1.0, 0.0) for hit in hits], axis=1).astype(BF16))
        shared = jnp.zeros_like(code)
        for ex, hit in enumerate(hits):
            begin = jnp.sum(spans[:, ex * 128:(ex + 1) * 128], axis=1, keepdims=True)
            shared = jnp.where(hit, code + begin + float(ex * (POOL - EXTRA)), shared)
        code_s[...] = shared
        for team in range(N_DEV // TEAM):
            x = dot(spread(team * TEAM), pack_ref[team * TEAM])
            for place in range(team * TEAM + 1, (team + 1) * TEAM):
                x = x + dot(spread(place), pack_ref[place])
            x_s[:, pl.ds(team * POOL, POOL), :] = x.astype(BF16).reshape(n_loc, POOL, d_model)

    @pl.when(step >= n_exp)
    def _():
        zx_s[e] = mlp(x_s[e])

    @pl.when(step == 2 * n_exp - 1)
    def _():
        ready = None
        for place, mask in SENDS:
            z = zx_s[:, pl.ds(place // TEAM * POOL, POOL), :].reshape(x_s.shape[0] * POOL, d_model)
            pack_s[place] = lax.dot_general(
                spread(place), z, (((0,), (0,)), ((), ())), preferred_element_type=F32).astype(BF16)
            if ready is not None:
                remote(pack_s.at[ready[0]], back_pack_ref.at[me], pack_send, pack_recv, ready[1], 2)
            ready = (place, mask)
        remote(pack_s.at[ready[0]], back_pack_ref.at[me], pack_send, pack_recv, ready[1], 2)

        settle(z_s.at[:, pl.ds(0, per_src), :], own_sem.at[1])
        settle(back_ref.at[pl.ds(0, (N_DEV - 1) * n_exp)], fix_recv)
        groups, seq, _ = hidden_ref.shape
        experts = back_ref.shape[0]
        pltpu.emit_pipeline(
            combine_fixed,
            grid=(groups // 2,),
            in_specs=[
                pl.BlockSpec((experts, FIX, d_model), lambda i: (0, i // 2, 0)),
                pl.BlockSpec((2, seq, d_model), lambda i: (i, 0, 0)),
                pl.BlockSpec((2, 8, seq), lambda i: (i, 0, 0)),
            ],
            out_specs=[pl.BlockSpec((2, seq, d_model), lambda i: (i, 0, 0))],
        )(back_ref, hidden_ref, meta_ref, part_ref)
        settle(pack_s.at[0], own_sem.at[2])
        settle(mine_ref.at[others], in_send)
        settle(z_s.at[:, pl.ds(0, (N_DEV - 1) * per_src), :], fix_send)
        settle(pack_s.at[others], pack_send)
        settle(back_pack_ref.at[others], pack_recv)


def packed_back_kernel(starts_ref, pack_ref, part_ref, meta_ref, msg_ref, out_ref, aux_ref, window_s, *, n_groups, experts):
    groups, seq, _ = part_ref.shape
    e_loc = experts // N_DEV
    step = pl.program_id(0)
    for dev in range(N_DEV):
        start = pl.multiple_of(starts_ref[step, dev * e_loc], 8)
        window_s[dev * WINDOW:(dev + 1) * WINDOW, :] = pack_ref[dev, pl.ds(start, WINDOW), :]

    for grp in range(0, groups, 2):
        gates = jnp.concatenate([gate_rows(meta_ref[grp + i], N_DEV * WINDOW, experts * FIX) for i in range(2)], axis=0)
        moe = dot(gates, window_s[...])
        for i in range(2):
            out_ref[grp + i] = (part_ref[grp + i] + moe[i * seq:(i + 1) * seq]).astype(BF16)

    @pl.when(step == 0)
    def _():
        aux_ref[0, 0] = jnp.sum(msg_ref[:, 0:8, :]) * (experts / n_groups)


def solution(mesh):
    def local_step(tokens, pad_mask, second_draw, choices, norm_attn, w_query, w_key, w_value, w_attn_out, norm_moe, w_gate, w_in, w_out):
        groups, seq, d_model = tokens.shape
        _, heads, head_dim = w_query.shape
        experts = w_gate.shape[1]
        ff = w_in.shape[2]
        e_loc = experts // N_DEV
        capacity = (2 * seq + experts - 1) // experts
        hw = heads * head_dim
        rows = 2 * capacity
        steps = groups // 2
        all_rows = N_DEV * steps * rows

        wq, wk, wv = (w.transpose(1, 2, 0).reshape(hw, d_model) for w in (w_query, w_key, w_value))
        wo = w_attn_out.reshape(hw, d_model)

        def whole(shape):
            return pl.BlockSpec(shape, lambda i: (0,) * len(shape), pipeline_mode=pl.Buffered(1))

        anywhere = pl.BlockSpec(memory_space=pl.ANY)
        front_specs = [
            pl.BlockSpec((2, seq, d_model), lambda i: (i, 0, 0)),
            whole((groups, seq)), whole((groups, seq)),
            pl.BlockSpec((2, 2, seq), lambda i: (i, 0, 0)),
            whole((d_model,)), whole((hw, d_model)), whole((hw, d_model)), whole((hw, d_model)), whole((hw, d_model)),
            whole((d_model,)), whole((d_model, experts)),
        ]
        quads = steps // 2
        fix_rows = quads * FIX
        dma = pltpu.SemaphoreType.DMA
        hidden_p, meta_p, mine, starts, fix, msg = pl.pallas_call(
            functools.partial(packed_front_kernel, heads=heads, head_dim=head_dim, capacity=capacity),
            name="packed_front",
            grid=(steps,),
            in_specs=front_specs,
            out_specs=[
                pl.BlockSpec((2, seq, d_model), lambda i: (i, 0, 0)),
                pl.BlockSpec((2, 8, seq), lambda i: (i, 0, 0)),
                pl.BlockSpec((N_DEV, PACK, d_model), lambda i: (0, 0, 0)),
                pl.BlockSpec((8, 128), lambda i: (0, 0)),
                anywhere, anywhere,
            ],
            out_shape=[
                jax.ShapeDtypeStruct((groups, seq, d_model), BF16),
                jax.ShapeDtypeStruct((groups, 8, seq), F32),
                jax.ShapeDtypeStruct((N_DEV, PACK, d_model), BF16),
                jax.ShapeDtypeStruct((8, 128), jnp.int32),
                jax.ShapeDtypeStruct((e_loc, N_DEV * fix_rows, d_model), BF16),
                jax.ShapeDtypeStruct((N_DEV, 16, 128), F32),
            ],
            scratch_shapes=[
                pltpu.VMEM((hw, 2 * seq), BF16),
                pltpu.VMEM((2 * seq, hw), BF16),
                pltpu.VMEM((hw, 2 * seq), BF16),
                pltpu.VMEM((hw, 2 * seq), BF16),
                pltpu.VMEM((2, heads, seq, seq), F32),
                pltpu.VMEM((2, heads, seq, seq), BF16),
                pltpu.VMEM((3 * experts, d_model), BF16),
                pltpu.VMEM((4 * seq, d_model), BF16),
                pltpu.VMEM((8, 4 * seq), jnp.int32),
                pltpu.VMEM((4, experts, 128), F32),
                pltpu.VMEM((8, 128), F32),
                pltpu.VMEM((N_DEV, 128), F32),
                pltpu.VMEM((N_DEV, 128), F32),
                pltpu.VMEM((N_DEV, 256), F32),
                pltpu.VMEM((N_DEV, quads * LOCAL, d_model), BF16),
                pltpu.VMEM((quads, N_DEV, e_loc, FIX, d_model), BF16),
                pltpu.VMEM((N_DEV, 16, 128), F32),
                dma, dma, dma, dma, dma((2,)),
            ],
            compiler_params=pltpu.CompilerParams(
                dimension_semantics=("arbitrary",), collective_id=0, has_side_effects=True, vmem_limit_bytes=VMEM_LIMIT),
        )(tokens, pad_mask, second_draw, choices.transpose(0, 2, 1), norm_attn, wq, wk, wv, wo, norm_moe, w_gate)

        def packed_path():
            back, back_pack, part = pl.pallas_call(
                packed_expert_kernel,
                name="packed_experts",
                grid=(2 * e_loc,),
                in_specs=[
                    pl.BlockSpec((1, N_DEV * fix_rows, d_model), lambda i: (jnp.minimum(i, e_loc - 1), 0, 0)),
                    whole((N_DEV, PACK, d_model)), whole((N_DEV, 16, 128)),
                    anywhere, anywhere, anywhere, anywhere,
                ],
                out_specs=[anywhere, anywhere, anywhere],
                out_shape=[
                    jax.ShapeDtypeStruct((experts, fix_rows, d_model), BF16),
                    jax.ShapeDtypeStruct((N_DEV, PACK, d_model), BF16),
                    jax.ShapeDtypeStruct((groups, seq, d_model), F32),
                ],
                scratch_shapes=[
                    pltpu.VMEM((2, d_model, ff), BF16),
                    pltpu.VMEM((2, ff, d_model), BF16),
                    dma((2, 2)),
                    pltpu.VMEM((N_DEV * fix_rows, ff), BF16),
                    pltpu.VMEM((e_loc, N_DEV // TEAM * POOL, d_model), BF16),
                    pltpu.VMEM((e_loc, N_DEV * fix_rows, d_model), BF16),
                    pltpu.VMEM((e_loc, N_DEV // TEAM * POOL, d_model), BF16),
                    pltpu.VMEM((N_DEV, 128), F32),
                    pltpu.VMEM((N_DEV, PACK, d_model), BF16),
                    pltpu.VMEM((N_DEV, PACK, d_model), BF16),
                    dma, dma, dma, dma, dma, dma, dma((3,)),
                ],
                compiler_params=pltpu.CompilerParams(
                    dimension_semantics=("arbitrary",), collective_id=1, has_side_effects=True, vmem_limit_bytes=VMEM_LIMIT),
            )(fix, mine, msg, w_in, w_out, hidden_p, meta_p)
            return pl.pallas_call(
                functools.partial(packed_back_kernel, n_groups=groups * N_DEV, experts=experts),
                name="packed_back",
                grid_spec=pltpu.PrefetchScalarGridSpec(
                    num_scalar_prefetch=1,
                    grid=(quads,),
                    in_specs=[
                        pl.BlockSpec((N_DEV, PACK, d_model), lambda i, starts: (0, 0, 0), pipeline_mode=pl.Buffered(1)),
                        pl.BlockSpec((4, seq, d_model), lambda i, starts: (i, 0, 0)),
                        pl.BlockSpec((4, 8, seq), lambda i, starts: (i, 0, 0)),
                        pl.BlockSpec((N_DEV, 16, 128), lambda i, starts: (0, 0, 0), pipeline_mode=pl.Buffered(1)),
                    ],
                    out_specs=[
                        pl.BlockSpec((4, seq, d_model), lambda i, starts: (i, 0, 0)),
                        pl.BlockSpec(memory_space=pltpu.SMEM),
                    ],
                    scratch_shapes=[pltpu.VMEM((N_DEV * WINDOW, d_model), BF16)],
                ),
                out_shape=[
                    jax.ShapeDtypeStruct((groups, seq, d_model), BF16),
                    jax.ShapeDtypeStruct((1, 1), F32),
                ],
                compiler_params=pltpu.CompilerParams(dimension_semantics=("arbitrary",), vmem_limit_bytes=VMEM_LIMIT),
            )(starts, back_pack, part, meta_p, msg)

        def full_path():
            recv = pl.pallas_call(
                functools.partial(full_front_kernel, experts=experts, capacity=capacity),
                name="full_front",
                grid=(steps,),
                in_specs=[
                    pl.BlockSpec((2, seq, d_model), lambda i: (i, 0, 0)),
                    pl.BlockSpec((2, 8, seq), lambda i: (i, 0, 0)),
                    whole((d_model,)),
                ],
                out_specs=anywhere,
                out_shape=jax.ShapeDtypeStruct((e_loc, all_rows, d_model), BF16),
                scratch_shapes=[pltpu.VMEM((steps, N_DEV, e_loc, rows, d_model), BF16), dma, dma, dma],
                compiler_params=pltpu.CompilerParams(
                    dimension_semantics=("arbitrary",), collective_id=2, has_side_effects=True, vmem_limit_bytes=VMEM_LIMIT),
            )(hidden_p, meta_p, norm_moe)
            tile = all_rows // 4
            ret = pl.pallas_call(
                functools.partial(expert_kernel, tile=tile),
                name="full_experts",
                grid=(e_loc,),
                in_specs=[
                    pl.BlockSpec((1, all_rows, d_model), lambda i: (i, 0, 0)),
                    pl.BlockSpec((1, d_model, ff), lambda i: (i, 0, 0)),
                    pl.BlockSpec((1, ff, d_model), lambda i: (i, 0, 0)),
                ],
                out_specs=anywhere,
                out_shape=jax.ShapeDtypeStruct((experts, steps * rows, d_model), BF16),
                scratch_shapes=[pltpu.VMEM((tile, ff), BF16), pltpu.VMEM((e_loc, all_rows, d_model), BF16), dma, dma, dma],
                compiler_params=pltpu.CompilerParams(
                    dimension_semantics=("arbitrary",), collective_id=3, has_side_effects=True, vmem_limit_bytes=VMEM_LIMIT),
            )(recv, w_in, w_out)
            return pl.pallas_call(
                functools.partial(back_kernel, n_groups=groups * N_DEV, capacity=capacity),
                name="full_back",
                grid=(steps,),
                in_specs=[
                    pl.BlockSpec((experts, rows, d_model), lambda i: (0, i, 0)),
                    pl.BlockSpec((2, seq, d_model), lambda i: (i, 0, 0)),
                    pl.BlockSpec((2, 8, seq), lambda i: (i, 0, 0)),
                    whole((N_DEV, 16, 128)),
                ],
                out_specs=[
                    pl.BlockSpec((2, seq, d_model), lambda i: (i, 0, 0)),
                    pl.BlockSpec(memory_space=pltpu.SMEM),
                ],
                out_shape=[
                    jax.ShapeDtypeStruct((groups, seq, d_model), BF16),
                    jax.ShapeDtypeStruct((1, 1), F32),
                ],
                compiler_params=pltpu.CompilerParams(dimension_semantics=("arbitrary",), vmem_limit_bytes=VMEM_LIMIT),
            )(ret, hidden_p, meta_p, msg)

        shared = jnp.sum(msg[:, 9, :].reshape(N_DEV // TEAM, TEAM, experts), axis=1)
        spilled = jnp.max(shared) > POOL
        out, aux = lax.cond(spilled, full_path, packed_path)
        return out, aux.reshape(())

    by_group = P("ep")
    replicated = P()
    in_specs = (by_group, by_group, by_group, by_group, replicated, replicated, replicated, replicated, replicated, replicated, replicated, by_group, by_group)
    return jax.shard_map(local_step, mesh=mesh, in_specs=in_specs, out_specs=(by_group, replicated), check_vma=False)
```
